32 devices in a mesh: data: 4 (over z), col: 2 (over y), row: 4 (over x, core).
Axes of the slice: x: 2, y: 2, z: 4, core: 2. Of those that a mesh axis runs over, the one named last changes fastest.
Arguments:
- x_in: bfloat16 [2048, 2048], P(None, 'row')
- h_act: bfloat16 [2048, 5632], P(None, 'row')
- d_gate: bfloat16 [2048, 5632], P(None, 'col')
- d_up: bfloat16 [2048, 5632], P(None, 'col')
- d_out: bfloat16 [2048, 2048], P(None, 'col')
- w_gate: float32 [2048, 5632], P('row', 'col')
- w_up: float32 [2048, 5632], P('row', 'col')
- w_down: float32 [5632, 2048], P('row', 'col')
- r_gate: float32 [2048], P('row')
- c_gate: float32 [5632], P('col')
- r_up: float32 [2048], P('row')
- c_up: float32 [5632], P('col')
- r_down: float32 [5632], P('row')
- c_down: float32 [2048], P('col')
- beta_two: float32 [], replicated
- rel_step: float32 [], replicated
- clip_thr: float32 [], replicated
Outputs:
- output 1: float32 [2048, 5632], P('row', 'col')
- output 2: float32 [2048, 5632], P('row', 'col')
- output 3: float32 [5632, 2048], P('row', 'col')
- output 4: float32 [2048], P('row')
- output 5: float32 [5632], P('col')
- output 6: float32 [2048], P('row')
- output 7: float32 [5632], P('col')
- output 8: float32 [5632], P('row')
- output 9: float32 [2048], P('col')
All inputs are finite; a program needn't handle non-finite values.
Results may differ from the reference program's by a relative error of at most 0.001.
Values are sent between devices in bfloat16 or wider.
A program may use at most 1 GiB of HBM per device.

```python
import jax
import jax.numpy as jnp

TOKENS = 2048
D = 2048
FF = 5632

EPS_SQ = 1e-30
EPS_SCALE = 1e-3
DOWN_STAT_SCALE = 60.0


def weight_grad(act_in, cot_out):
    return jnp.dot(act_in.T, cot_out, preferred_element_type=jnp.float32)


def adafactor_step(w_mat, g_mat, r_old, c_old, beta_two, rel_step, clip_thr):
    q_mat = g_mat * g_mat + EPS_SQ
    r_new = beta_two * r_old + (1.0 - beta_two) * jnp.mean(q_mat, axis=1)
    c_new = beta_two * c_old + (1.0 - beta_two) * jnp.mean(q_mat, axis=0)
    v_mat = r_new[:, None] * c_new[None, :] / jnp.mean(r_new)
    u_mat = g_mat / jnp.sqrt(v_mat)
    u_rms = jnp.sqrt(jnp.mean(u_mat * u_mat))
    u_hat = u_mat / jnp.maximum(1.0, u_rms / clip_thr)
    w_rms = jnp.sqrt(jnp.mean(w_mat * w_mat))
    step_size = rel_step * jnp.maximum(EPS_SCALE, w_rms)
    return w_mat - step_size * u_hat, r_new, c_new


def old_stats(g_mat, key_row, key_col, stat_scale):
    q_mat = g_mat * g_mat
    row_fac = jnp.exp(jax.random.uniform(key_row, (g_mat.shape[0],), jnp.float32, -1.2, 1.2))
    col_fac = jnp.exp(jax.random.uniform(key_col, (g_mat.shape[1],), jnp.float32, -1.2, 1.2))
    return stat_scale * jnp.mean(q_mat, axis=1) * row_fac, stat_scale * jnp.mean(q_mat, axis=0) * col_fac


def setup_inputs(seed: int = 0) -> dict:
    key_list = jax.random.split(jax.random.key(seed), 17)
    x_in = jax.random.normal(key_list[0], (TOKENS, D), jnp.float32).astype(jnp.bfloat16)
    h_act = jax.random.normal(key_list[1], (TOKENS, FF), jnp.float32).astype(jnp.bfloat16)
    d_gate = jax.random.normal(key_list[2], (TOKENS, FF), jnp.float32).astype(jnp.bfloat16)
    d_up = jax.random.normal(key_list[3], (TOKENS, FF), jnp.float32).astype(jnp.bfloat16)
    d_out = jax.random.normal(key_list[4], (TOKENS, D), jnp.float32).astype(jnp.bfloat16)
    w_gate = jax.random.normal(key_list[5], (D, FF), jnp.float32) * D ** -0.5
    w_up = jax.random.normal(key_list[6], (D, FF), jnp.float32) * D ** -0.5
    w_down = jax.random.normal(key_list[7], (FF, D), jnp.float32) * FF ** -0.5
    r_gate, c_gate = old_stats(weight_grad(x_in, d_gate), key_list[8], key_list[9], 1.0)
    r_up, c_up = old_stats(weight_grad(x_in, d_up), key_list[10], key_list[11], 1.0)
    r_down, c_down = old_stats(weight_grad(h_act, d_out), key_list[12], key_list[13], DOWN_STAT_SCALE)
    beta_two = jax.random.uniform(key_list[14], (), jnp.float32, 0.5, 0.9)
    rel_step = jax.random.uniform(key_list[15], (), jnp.float32, 0.2, 0.6)
    clip_thr = jax.random.uniform(key_list[16], (), jnp.float32, 0.4, 0.6)
    return dict(x_in=x_in, h_act=h_act, d_gate=d_gate, d_up=d_up, d_out=d_out, w_gate=w_gate, w_up=w_up, w_down=w_down, r_gate=r_gate, c_gate=c_gate, r_up=r_up, c_up=c_up, r_down=r_down, c_down=c_down, beta_two=beta_two, rel_step=rel_step, clip_thr=clip_thr)


def reference(x_in, h_act, d_gate, d_up, d_out, w_gate, w_up, w_down, r_gate, c_gate, r_up, c_up, r_down, c_down, beta_two, rel_step, clip_thr):
    gate_w, gate_r, gate_c = adafactor_step(w_gate, weight_grad(x_in, d_gate), r_gate, c_gate, beta_two, rel_step, clip_thr)
    up_w, up_r, up_c = adafactor_step(w_up, weight_grad(x_in, d_up), r_up, c_up, beta_two, rel_step, clip_thr)
    down_w, down_r, down_c = adafactor_step(w_down, weight_grad(h_act, d_out), r_down, c_down, beta_two, rel_step, clip_thr)
    return (gate_w, up_w, down_w, gate_r, gate_c, up_r, up_c, down_r, down_c)
```

```python
import functools

import jax
import jax.numpy as jnp
from jax import lax
from jax.experimental import pallas as pl
from jax.experimental.pallas import tpu as pltpu
from jax.sharding import PartitionSpec as P

EPS_SQ = 1e-30
EPS_SCALE = 1e-3
F32 = jnp.float32
BF16 = jnp.bfloat16
MESH = pl.DeviceIdType.MESH
VM = pltpu.VMEM
HB = pltpu.HBM
KB = 256
NT = 256
RING = 8
PIECES = (176, 80, 96)


def block_rows(q, w, c, dims):
    first = 0
    for m, n in (tuple(dims) + tuple(dims))[:q + 3 * w]:
        first += m * (n // 128)
    return first + c * dims[q][0]


def dot_kernel(
    dims,
    x, h, dg, du, dd, wg, wu, wd, rg, cg, ru, cu, rd, cd,
    held, rs_g, rs_u, rs_d, cs_g, cs_u, cs_d, sw, ro, co,
    xs, hs, xt, ht, ring, x_sem, h_sem, d_sem, w_sem, s_sem,
):
    tokens = x.shape[0]
    nk = tokens // KB
    mats = (
        dict(d=dg, wh=wg, rs=rs_g, cs=cs_g),
        dict(d=du, wh=wu, rs=rs_u, cs=cs_u),
        dict(d=dd, wh=wd, rs=rs_d, cs=cs_d),
    )
    for mat, (m, n) in zip(mats, dims):
        mat["m"], mat["n"] = m, n

    def x_copy(k):
        return pltpu.make_async_copy(x.at[pl.ds(k * KB, KB), :], xs.at[k], x_sem.at[k])

    def h_copy(k):
        return pltpu.make_async_copy(h.at[pl.ds(k * KB, KB), :], hs.at[k % 3], h_sem.at[k % 3])

    tiles = [(q, j) for q in range(3) for j in range(mats[q]["n"] // NT)]

    def d_copy(i):
        q, j = tiles[i]
        return pltpu.make_async_copy(mats[q]["d"].at[:, pl.ds(j * NT, NT)], ring.at[i % RING], d_sem.at[i % RING])

    def w_copy(i, half):
        q, j = tiles[i]
        dst = held.at[pl.ds(block_rows(q, 1, 2 * j + half, dims), mats[q]["m"]), :]
        return pltpu.make_async_copy(mats[q]["wh"].at[:, pl.ds(j * NT + half * 128, 128)], dst, w_sem.at[i, half])

    small = [
        pltpu.make_async_copy(src, dst.at[q, 0, pl.ds(0, src.shape[0])], s_sem.at[i])
        for i, (src, dst, q) in enumerate(
            [(rg, ro, 0), (ru, ro, 1), (rd, ro, 2), (cg, co, 0), (cu, co, 1), (cd, co, 2)])
    ]
    x_copy(0).start()
    d_copy(0).start()
    for k in range(1, nk):
        x_copy(k).start()
    for i in range(1, RING - 1):
        d_copy(i).start()
    for c in small:
        c.start()

    def h_turn(k):
        for c in range(ht.shape[0] // 128):
            ht[pl.ds(c * 128, 128), pl.ds(k * KB, KB)] = hs[k % 3, :, pl.ds(c * 128, 128)].T

    def w_square(i):
        q, j = tiles[i]
        w = held[pl.ds(block_rows(q, 1, 2 * j, dims), 2 * mats[q]["m"]), :]
        s = jnp.sum((w * w).reshape(-1, 8, 128), axis=0)
        if j == 0:
            sw[q] = s
        else:
            sw[q] += s

    units = []
    for i, (q, j) in enumerate(tiles):
        if q < 2:
            units.append((i, q, j, (0, 256), 256))
        else:
            units.append((i, q, j, (0, 352), 352))
            units.append((i, q, j, (704, 1056), 352))
    n_units = len(units)

    before = [[] for _ in range(n_units)]
    beside = [[] for _ in range(n_units)]
    for k in range(nk):
        before[k].append(lambda k=k: h_copy(k).start())
        before[k + 2].append(lambda k=k: h_copy(k).wait())
        beside[k + 2].append(lambda k=k: h_turn(k))
    w_at = [3 + i for i in range(len(tiles))]
    for i in range(len(tiles)):
        u = min(w_at[i], n_units - 4)
        before[u].append(lambda i=i: [w_copy(i, half).start() for half in range(2)])
        before[u + 3].append(lambda i=i: [w_copy(i, half).wait() for half in range(2)])
        beside[u + 3].append(lambda i=i: w_square(i))
    def run(*accs):
        accs = [[accs[(z * 2 + par) * 3:(z * 2 + par) * 3 + 3] for par in range(2)] for z in range(2)]

        def rhs(u, k):
            return ring[units[u][0] % RING, pl.ds(k * KB, KB), :]

        def lhs(q, r0, rows, k):
            src = ht if q == 2 else xt
            return src[pl.ds(r0, rows), pl.ds(k * KB, KB)]

        def drain(u):
            i, q, j, starts, rows = units[u]
            mat = mats[q]
            cc = None
            for z in range(2):
                r0, left = starts[z], rows
                for p, size in enumerate(PIECES):
                    if not left:
                        break
                    g = pltpu.matmul_pop(accs[z][u % 2][p])
                    for half in range(2):
                        gr = block_rows(q, 0, 2 * j + half, dims) + r0
                        held[pl.ds(gr, size), :] = g[:, half * 128:half * 128 + 128]
                    s = g * g
                    lanes = s[:, :128] + s[:, 128:]
                    if j == 0:
                        mat["rs"][pl.ds(r0, size), :] = lanes
                    else:
                        mat["rs"][pl.ds(r0, size), :] += lanes
                    s = jnp.sum(s.reshape(-1, 8, NT), axis=0)
                    cc = s if cc is None else cc + s
                    r0, left = r0 + size, left - size
            if q == 2 and starts[0]:
                mat["cs"][:, pl.ds(j * NT, NT)] += cc
            else:
                mat["cs"][:, pl.ds(j * NT, NT)] = cc

        for z in range(2):
            for par in range(2):
                for p in range(3):
                    pltpu.matmul_pop(accs[z][par][p])

        d_copy(0).wait()
        for u in range(n_units):
            i, q, j, starts, rows = units[u]
            last = u == n_units - 1
            if u == 0:
                x_copy(0).wait()
            for f in before[u]:
                f()
            if not last and units[u + 1][0] != i:
                d_copy(units[u + 1][0]).wait()
            new = u == 0 or units[u - 1][0] != i
            if new and u and i + RING - 2 < len(tiles):
                d_copy(i + RING - 2).start()
            if u == 0:
                for z in range(2):
                    pltpu.matmul_push_rhs(rhs(0, 0), staging_register=0, mxu_index=z)
            for k in range(nk):
                if u == 0:
                    if k:
                        x_copy(k).wait()
                    for z in range(2):
                        xt[pl.ds(z * 256, 256), pl.ds(k * KB, KB)] = xs[k, :, pl.ds(z * 256, 256)].T
                for z in range(2):
                    r0, left = starts[z], rows
                    for p, size in enumerate(PIECES):
                        if not left:
                            break
                        pltpu.matmul_acc_lhs(accs[z][u % 2][p], lhs(q, r0, size, k),
                                             load_staged_rhs=(k % 2 if p == 0 else None))
                        r0, left = r0 + size, left - size
                    if k < nk - 1:
                        pltpu.matmul_push_rhs(rhs(u, k + 1), staging_register=(k + 1) % 2, mxu_index=z)
                    elif not last:
                        pltpu.matmul_push_rhs(rhs(u + 1, 0), staging_register=0, mxu_index=z)
                if k == 1 and u:
                    drain(u - 1)
                if k == 2:
                    for f in beside[u]:
                        f()
        drain(n_units - 1)

    spec = [pltpu.ACC(z)((size, NT), F32) for z in range(2) for par in range(2) for size in PIECES]
    pl.run_scoped(run, *spec)

    for c in small:
        c.wait()


def exchange_kernel(
    dims,
    held, rs_g, rs_u, rs_d, cs_g, cs_u, cs_d, sw, ro, co,
    b2, rel, clip,
    a_g, a_u, a_d, b_g, b_u, b_d, r_g, c_g, r_u, c_u, r_d, c_d,
    su, rsend, rrecv, csend, crecv, pay, got, r1s, r1r, c1s, c1r, p_s, p_r,
):
    col = lax.axis_index("col")
    row = lax.axis_index("row")
    row_peer = (row + 1 - 2 * (row % 2), (row + 2) % 4, 3 - row)
    mats = (
        dict(rs=rs_g, cs=cs_g, a=a_g, b=b_g, r=r_g, c=c_g),
        dict(rs=rs_u, cs=cs_u, a=a_u, b=b_u, r=r_u, c=c_u),
        dict(rs=rs_d, cs=cs_d, a=a_d, b=b_d, r=r_d, c=c_d),
    )
    for mat, (m, n) in zip(mats, dims):
        mat["m"], mat["n"] = m, n
        mat["mt"], mat["nt"] = mat["m"] * 4, mat["n"] * 2

    barrier = pltpu.get_barrier_semaphore()
    plane = [{"row": p, "col": cc} for cc in (col, 1 - col) for p in (row,) + row_peer][1:]
    for dev in plane:
        pl.semaphore_signal(barrier, inc=1, device_id=dev, device_id_type=MESH)
    pay[...] = jnp.zeros_like(pay)

    def first_sends(q):
        mat = mats[q]
        m, n = mat["m"], mat["n"]
        copies = [pltpu.make_async_remote_copy(
            rsend.at[q, :, pl.ds(0, m)], rrecv.at[q, :, pl.ds(0, m)], r1s.at[q], r1r.at[q],
            device_id={"col": 1 - col}, device_id_type=MESH)]
        for d in range(3):
            copies.append(pltpu.make_async_remote_copy(
                csend.at[q, :, pl.ds(0, n)], crecv.at[q, d, :, pl.ds(0, n)], c1s.at[q, d], c1r.at[q, d],
                device_id={"row": row_peer[d]}, device_id_type=MESH))
        return copies

    def first_reduce(q):
        mat = mats[q]
        csend[q, :, pl.ds(0, mat["n"])] = jnp.sum(mat["cs"][...], axis=0, keepdims=True)
        for b in range(mat["m"] // 128):
            t = mat["rs"][pl.ds(b * 128, 128), :].T
            rsend[q, :, pl.ds(b * 128, 128)] = jnp.sum(t, axis=0, keepdims=True)

    def new_stats(q):
        mat = mats[q]
        m, n = mat["m"], mat["n"]
        beta = b2[0, 0]
        rsum = rsend[q, :, pl.ds(0, m)] + rrecv[q, :, pl.ds(0, m)]
        r_new = beta * ro[q, :, pl.ds(0, m)] + (1.0 - beta) * (rsum * (1.0 / mat["nt"]) + EPS_SQ)
        mat["r"][...] = r_new
        csum = (csend[q, :, pl.ds(0, n)] + crecv[q, 0, :, pl.ds(0, n)]) + (
            crecv[q, 1, :, pl.ds(0, n)] + crecv[q, 2, :, pl.ds(0, n)])
        c_new = beta * co[q, :, pl.ds(0, n)] + (1.0 - beta) * (csum * (1.0 / mat["mt"]) + EPS_SQ)
        mat["c"][...] = c_new
        mat["b"][...] = lax.rsqrt(c_new)
        alpha = lax.rsqrt(r_new)
        rp = r_new[:, :128]
        for b in range(m // 128):
            blk = jnp.broadcast_to(alpha[:, b * 128:(b + 1) * 128], (128, 128))
            mat["a"][pl.ds(b * 128, 128), :] = blk.T
            if b:
                rp = rp + r_new[:, b * 128:(b + 1) * 128]
        pay[pl.ds(6 + q, 1), :] = rp

    def u_square(q):
        mat = mats[q]
        su[q] = jnp.zeros((8, 128), F32)

        @pl.loop(0, mat["n"] // 128)
        def _(c):
            cc = pl.ds(pl.multiple_of(c * 128, 128), 128)
            gr = pl.multiple_of(block_rows(q, 0, c, dims), 128)
            t = held[pl.ds(gr, mat["m"]), :] * mat["a"][...]
            s = jnp.sum((t * t).reshape(-1, 8, 128), axis=0)
            bb = mat["b"][:, cc]
            su[q] += s * (bb * bb)

    def pay_rows(q):
        pay[pl.ds(q, 1), :] = jnp.sum(su[q], axis=0, keepdims=True)
        pay[pl.ds(3 + q, 1), :] = jnp.sum(sw[q], axis=0, keepdims=True)

    for q in range(3):
        first_reduce(q)
    pl.semaphore_wait(barrier, len(plane))
    sends = [c for q in range(3) for c in first_sends(q)]
    for c in sends:
        c.start()
    for c in sends:
        c.wait()
    for q in range(3):
        new_stats(q)
    for q in range(3):
        u_square(q)
        pay_rows(q)
    sends = [pltpu.make_async_remote_copy(pay, got.at[i], p_s.at[i], p_r.at[i], device_id=dev, device_id_type=MESH)
             for i, dev in enumerate(plane)]
    for c in sends:
        c.start()
    for c in sends:
        c.wait()
    total = ((pay[...] + got[0]) + (got[1] + got[2])) + ((got[3] + got[4]) + (got[5] + got[6]))
    total = jnp.sum(total, axis=1, keepdims=True)
    for q, mat in enumerate(mats):
        size = float(mat["mt"] * mat["nt"])
        r_mean = total[6 + q:7 + q] * (0.5 / mat["mt"])
        u_rms = jnp.sqrt(r_mean * total[q:q + 1] / size)
        w_rms = jnp.sqrt(total[3 + q:4 + q] / size)
        step = rel[0, 0] * jnp.maximum(EPS_SCALE, w_rms)
        k = step * jnp.sqrt(r_mean) / jnp.maximum(1.0, u_rms / clip[0, 0])
        mat["b"][...] = mat["b"][...] * k


def write_kernel(
    dims,
    held, a_g, a_u, a_d, b_g, b_u, b_d, r_g, c_g, r_u, c_u, r_d, c_d,
    o_g, o_u, o_d, or_g, oc_g, or_u, oc_u, or_d, oc_d,
    wide, tall, o_sem, s_sem,
):
    small = [pltpu.make_async_copy(s.at[0], d, s_sem.at[i]) for i, (s, d) in enumerate(
        [(r_g, or_g), (c_g, oc_g), (r_u, or_u), (c_u, oc_u), (r_d, or_d), (c_d, oc_d)])]
    for c in small:
        c.start()
    slots = 4
    pending = {}
    step = 0
    for q, a, b, o, buf in ((2, a_d, b_d, o_d, tall), (1, a_u, b_u, o_u, wide), (0, a_g, b_g, o_g, wide)):
        rows = buf.shape[1]
        for t in range(dims[q][0] // rows):
            slot = step % slots
            if slot in pending:
                pending.pop(slot).wait()
            rr = pl.ds(t * rows, rows)
            scale = a[rr, :]
            for c in range(dims[q][1] // 128):
                cc = pl.ds(c * 128, 128)
                g, w = (held[pl.ds(block_rows(q, z, c, dims) + t * rows, rows), :] for z in range(2))
                buf[slot, :, cc] = w - (g * scale) * b[:, cc]
            cp = pltpu.make_async_copy(buf.at[slot], o.at[rr, :], o_sem.at[slot])
            cp.start()
            pending[slot] = cp
            step += 1
    for cp in pending.values():
        cp.wait()
    for c in small:
        c.wait()


def solution(mesh):
    def local_program(x_in, h_act, d_gate, d_up, d_out, w_gate, w_up, w_down, r_gate, c_gate, r_up, c_up, r_down, c_down, beta_two, rel_step, clip_thr):
        (mg, ng), (md, nd) = w_gate.shape, w_down.shape
        tokens = x_in.shape[0]
        nk = tokens // KB
        big = [x_in, h_act, d_gate, d_up, d_out, w_gate, w_up, w_down, r_gate, c_gate, r_up, c_up, r_down, c_down]
        one = [v.reshape(1, 1) for v in (beta_two, rel_step, clip_thr)]
        big = [pltpu.with_memory_space_constraint(v, HB) for v in big]
        dims = [(mg, ng), (mg, ng), (md, nd)]
        mm, nn = max(mg, md), max(ng, nd)
        dma = pltpu.SemaphoreType.DMA

        def call(kernel, outs, args, in_spaces, out_space, scratch, mib, **params):
            return pl.pallas_call(
                functools.partial(kernel, dims),
                out_shape=outs,
                in_specs=[pl.BlockSpec(memory_space=v) for v in in_spaces],
                out_specs=tuple(pl.BlockSpec(memory_space=out_space) for _ in outs),
                scratch_shapes=scratch,
                compiler_params=pltpu.CompilerParams(vmem_limit_bytes=mib * 2**20, **params),
                name=kernel.__name__,
            )(*args)

        def vm(shapes):
            return tuple(VM(s, F32) for s in shapes)

        lanes = [(m, 128) for m, _ in dims]
        first = call(
            dot_kernel,
            vm([(2 * sum(m * n for m, n in dims) // 128, 128)] + lanes + [(8, n) for _, n in dims] + [(3, 8, 128), (3, 1, mm), (3, 1, nn)]),
            big, [HB] * len(big), VM,
            [
                VM((nk, KB, mg), BF16), VM((3, KB, md), BF16), VM((mg, tokens), BF16), VM((md, tokens), BF16),
                VM((RING, tokens, NT), BF16),
                dma((nk,)), dma((3,)), dma((RING,)), dma((2 * ng // NT + nd // NT, 2)), dma((6,)),
            ], 22)
        held, rest = first[:1], first[1:]
        stats = [s for m, n in dims for s in ((1, m), (1, n))]
        second = call(
            exchange_kernel,
            vm(lanes + [(1, n) for _, n in dims] + stats),
            held + rest + tuple(one), [VM] * len(first) + [pltpu.SMEM] * 3, VM,
            [
                VM((3, 8, 128), F32),
                VM((3, 1, mm), F32), VM((3, 1, mm), F32), VM((3, 1, nn), F32), VM((3, 3, 1, nn), F32),
                VM((16, 128), F32), VM((7, 16, 128), F32),
                dma((3,)), dma((3,)), dma((3, 3)), dma((3, 3)), dma((7,)), dma((7,)),
            ], 8, collective_id=0, has_side_effects=True)
        outs = call(
            write_kernel,
            tuple(jax.ShapeDtypeStruct(s, F32) for s in dims + [(k,) for mn in dims for k in mn]),
            held + second, [VM] * (1 + len(second)), HB,
            [VM((4, mg // 8, ng), F32), VM((4, md // 8, nd), F32), dma((4,)), dma((6,))], 8)
        return tuple(outs)

    act_spec = P(None, "row")
    cot_spec = P(None, "col")
    w_spec = P("row", "col")
    r_spec = P("row")
    c_spec = P("col")
    s_spec = P()
    return jax.shard_map(local_program, mesh=mesh, in_specs=(act_spec, act_spec, cot_spec, cot_spec, cot_spec, w_spec, w_spec, w_spec, r_spec, c_spec, r_spec, c_spec, r_spec, c_spec, s_spec, s_spec, s_spec), out_specs=(w_spec, w_spec, w_spec, r_spec, c_spec, r_spec, c_spec, r_spec, c_spec), check_vma=False)
```

```python
import functools

import jax
import jax.numpy as jnp
from jax import lax
from jax.experimental import pallas as pl
from jax.experimental.pallas import tpu as pltpu
from jax.sharding import PartitionSpec as P

EPS_SQ = 1e-30
EPS_SCALE = 1e-3
F32 = jnp.float32
BF16 = jnp.bfloat16
MESH = pl.DeviceIdType.MESH
VM = pltpu.VMEM
HB = pltpu.HBM
KB = 256
NT = 256
RING = 4
PIECES = (176, 80, 96)


def block_rows(q, w, c, dims):
    first = 0
    for m, n in (tuple(dims) + tuple(dims))[:q + 3 * w]:
        first += m * (n // 128)
    return first + c * dims[q][0]


def dot_kernel(
    dims,
    x, h, dg, du, dd, wg, wu, wd, rg, cg, ru, cu, rd, cd,
    held, rs_g, rs_u, rs_d, cs_g, cs_u, cs_d, sw, ro, co,
    xs, hs, xt, ht, ring, x_sem, h_sem, d_sem, w_sem, s_sem,
):
    tokens = x.shape[0]
    nk = tokens // KB
    mats = (
        dict(d=dg, wh=wg, rs=rs_g, cs=cs_g),
        dict(d=du, wh=wu, rs=rs_u, cs=cs_u),
        dict(d=dd, wh=wd, rs=rs_d, cs=cs_d),
    )
    for mat, (m, n) in zip(mats, dims):
        mat["m"], mat["n"] = m, n

    def x_copy(k):
        return pltpu.make_async_copy(x.at[pl.ds(k * KB, KB), :], xs.at[k], x_sem.at[k])

    def h_copy(k):
        return pltpu.make_async_copy(h.at[pl.ds(k * KB, KB), :], hs.at[k % 3], h_sem.at[k % 3])

    tiles = [(q, j) for q in range(3) for j in range(mats[q]["n"] // NT)]

    def d_copy(i):
        q, j = tiles[i]
        return pltpu.make_async_copy(mats[q]["d"].at[:, pl.ds(j * NT, NT)], ring.at[i % RING], d_sem.at[i % RING])

    def w_copy(i, half):
        q, j = tiles[i]
        dst = held.at[pl.ds(block_rows(q, 1, 2 * j + half, dims), mats[q]["m"]), :]
        return pltpu.make_async_copy(mats[q]["wh"].at[:, pl.ds(j * NT + half * 128, 128)], dst, w_sem.at[i, half])

    small = [
        pltpu.make_async_copy(src, dst.at[q, 0, pl.ds(0, src.shape[0])], s_sem.at[i])
        for i, (src, dst, q) in enumerate(
            [(rg, ro, 0), (ru, ro, 1), (rd, ro, 2), (cg, co, 0), (cu, co, 1), (cd, co, 2)])
    ]
    x_copy(0).start()
    d_copy(0).start()
    for k in range(1, nk):
        x_copy(k).start()
    for i in range(1, RING - 1):
        d_copy(i).start()
    for c in small:
        c.start()

    def h_turn(k):
        for c in range(ht.shape[0] // 128):
            ht[pl.ds(c * 128, 128), pl.ds(k * KB, KB)] = hs[k % 3, :, pl.ds(c * 128, 128)].T

    def w_square(i):
        q, j = tiles[i]
        w = held[pl.ds(block_rows(q, 1, 2 * j, dims), 2 * mats[q]["m"]), :]
        s = jnp.sum((w * w).reshape(-1, 8, 128), axis=0)
        if j == 0:
            sw[q] = s
        else:
            sw[q] += s

    units = []
    for i, (q, j) in enumerate(tiles):
        if q < 2:
            units.append((i, q, j, (0, 256), 256))
        else:
            units.append((i, q, j, (0, 352), 352))
            units.append((i, q, j, (704, 1056), 352))
    n_units = len(units)

    before = [[] for _ in range(n_units)]
    beside = [[] for _ in range(n_units)]
    for k in range(nk):
        before[k].append(lambda k=k: h_copy(k).start())
        before[k + 2].append(lambda k=k: h_copy(k).wait())
        beside[k + 2].append(lambda k=k: h_turn(k))
    w_at = [3 + i for i in range(len(tiles))]
    for i in range(len(tiles)):
        u = min(w_at[i], n_units - 4)
        before[u].append(lambda i=i: [w_copy(i, half).start() for half in range(2)])
        before[u + 3].append(lambda i=i: [w_copy(i, half).wait() for half in range(2)])
        beside[u + 3].append(lambda i=i: w_square(i))
    def run(*accs):
        accs = [[accs[(z * 2 + par) * 3:(z * 2 + par) * 3 + 3] for par in range(2)] for z in range(2)]

        def rhs(u, k):
            return ring[units[u][0] % RING, pl.ds(k * KB, KB), :]

        def lhs(q, r0, rows, k):
            src = ht if q == 2 else xt
            return src[pl.ds(r0, rows), pl.ds(k * KB, KB)]

        def drain(u):
            i, q, j, starts, rows = units[u]
            mat = mats[q]
            cc = None
            for z in range(2):
                r0, left = starts[z], rows
                for p, size in enumerate(PIECES):
                    if not left:
                        break
                    g = pltpu.matmul_pop(accs[z][u % 2][p])
                    for half in range(2):
                        gr = block_rows(q, 0, 2 * j + half, dims) + r0
                        held[pl.ds(gr, size), :] = g[:, half * 128:half * 128 + 128]
                    s = g * g
                    lanes = s[:, :128] + s[:, 128:]
                    if j == 0:
                        mat["rs"][pl.ds(r0, size), :] = lanes
                    else:
                        mat["rs"][pl.ds(r0, size), :] += lanes
                    s = jnp.sum(s.reshape(-1, 8, NT), axis=0)
                    cc = s if cc is None else cc + s
                    r0, left = r0 + size, left - size
            if q == 2 and starts[0]:
                mat["cs"][:, pl.ds(j * NT, NT)] += cc
            else:
                mat["cs"][:, pl.ds(j * NT, NT)] = cc

        for z in range(2):
            for par in range(2):
                for p in range(3):
                    pltpu.matmul_pop(accs[z][par][p])

        d_copy(0).wait()
        for u in range(n_units):
            i, q, j, starts, rows = units[u]
            last = u == n_units - 1
            if u == 0:
                x_copy(0).wait()
            for f in before[u]:
                f()
            if not last and units[u + 1][0] != i:
                d_copy(units[u + 1][0]).wait()
            new = u == 0 or units[u - 1][0] != i
            if new and u and i + RING - 2 < len(tiles):
                d_copy(i + RING - 2).start()
            if u == 0:
                for z in range(2):
                    pltpu.matmul_push_rhs(rhs(0, 0), staging_register=0, mxu_index=z)
            for k in range(nk):
                if u == 0:
                    if k:
                        x_copy(k).wait()
                    for z in range(2):
                        xt[pl.ds(z * 256, 256), pl.ds(k * KB, KB)] = xs[k, :, pl.ds(z * 256, 256)].T
                for z in range(2):
                    r0, left = starts[z], rows
                    for p, size in enumerate(PIECES):
                        if not left:
                            break
                        pltpu.matmul_acc_lhs(accs[z][u % 2][p], lhs(q, r0, size, k),
                                             load_staged_rhs=(k % 2 if p == 0 else None))
                        r0, left = r0 + size, left - size
                    if k < nk - 1:
                        pltpu.matmul_push_rhs(rhs(u, k + 1), staging_register=(k + 1) % 2, mxu_index=z)
                    elif not last:
                        pltpu.matmul_push_rhs(rhs(u + 1, 0), staging_register=0, mxu_index=z)
                if k == 1 and u:
                    drain(u - 1)
                if k == 2:
                    for f in beside[u]:
                        f()
        drain(n_units - 1)

    spec = [pltpu.ACC(z)((size, NT), F32) for z in range(2) for par in range(2) for size in PIECES]
    pl.run_scoped(run, *spec)

    for c in small:
        c.wait()


def exchange_kernel(
    dims,
    held, rs_g, rs_u, rs_d, cs_g, cs_u, cs_d, sw, ro, co,
    b2, rel, clip,
    a_g, a_u, a_d, b_g, b_u, b_d, r_g, c_g, r_u, c_u, r_d, c_d,
    su, rsend, rrecv, csend, crecv, pay, got, r1s, r1r, c1s, c1r, p_s, p_r,
):
    col = lax.axis_index("col")
    row = lax.axis_index("row")
    row_peer = (row + 1 - 2 * (row % 2), (row + 2) % 4, 3 - row)
    mats = (
        dict(rs=rs_g, cs=cs_g, a=a_g, b=b_g, r=r_g, c=c_g),
        dict(rs=rs_u, cs=cs_u, a=a_u, b=b_u, r=r_u, c=c_u),
        dict(rs=rs_d, cs=cs_d, a=a_d, b=b_d, r=r_d, c=c_d),
    )
    for mat, (m, n) in zip(mats, dims):
        mat["m"], mat["n"] = m, n
        mat["mt"], mat["nt"] = mat["m"] * 4, mat["n"] * 2

    barrier = pltpu.get_barrier_semaphore()
    plane = [{"row": p, "col": cc} for cc in (col, 1 - col) for p in (row,) + row_peer][1:]
    for dev in plane:
        pl.semaphore_signal(barrier, inc=1, device_id=dev, device_id_type=MESH)
    pay[...] = jnp.zeros_like(pay)

    def first_sends(q):
        mat = mats[q]
        m, n = mat["m"], mat["n"]
        copies = [pltpu.make_async_remote_copy(
            rsend.at[q, :, pl.ds(0, m)], rrecv.at[q, :, pl.ds(0, m)], r1s.at[q], r1r.at[q],
            device_id={"col": 1 - col}, device_id_type=MESH)]
        for d in range(3):
            copies.append(pltpu.make_async_remote_copy(
                csend.at[q, :, pl.ds(0, n)], crecv.at[q, d, :, pl.ds(0, n)], c1s.at[q, d], c1r.at[q, d],
                device_id={"row": row_peer[d]}, device_id_type=MESH))
        return copies

    def first_reduce(q):
        mat = mats[q]
        csend[q, :, pl.ds(0, mat["n"])] = jnp.sum(mat["cs"][...], axis=0, keepdims=True)
        for b in range(mat["m"] // 128):
            t = mat["rs"][pl.ds(b * 128, 128), :].T
            rsend[q, :, pl.ds(b * 128, 128)] = jnp.sum(t, axis=0, keepdims=True)

    def new_stats(q):
        mat = mats[q]
        m, n = mat["m"], mat["n"]
        beta = b2[0, 0]
        rsum = rsend[q, :, pl.ds(0, m)] + rrecv[q, :, pl.ds(0, m)]
        r_new = beta * ro[q, :, pl.ds(0, m)] + (1.0 - beta) * (rsum * (1.0 / mat["nt"]) + EPS_SQ)
        mat["r"][...] = r_new
        csum = (csend[q, :, pl.ds(0, n)] + crecv[q, 0, :, pl.ds(0, n)]) + (
            crecv[q, 1, :, pl.ds(0, n)] + crecv[q, 2, :, pl.ds(0, n)])
        c_new = beta * co[q, :, pl.ds(0, n)] + (1.0 - beta) * (csum * (1.0 / mat["mt"]) + EPS_SQ)
        mat["c"][...] = c_new
        mat["b"][...] = lax.rsqrt(c_new)
        alpha = lax.rsqrt(r_new)
        rp = r_new[:, :128]
        for b in range(m // 128):
            blk = jnp.broadcast_to(alpha[:, b * 128:(b + 1) * 128], (128, 128))
            mat["a"][pl.ds(b * 128, 128), :] = blk.T
            if b:
                rp = rp + r_new[:, b * 128:(b + 1) * 128]
        pay[pl.ds(6 + q, 1), :] = rp

    def u_square(q):
        mat = mats[q]
        su[q] = jnp.zeros((8, 128), F32)

        @pl.loop(0, mat["n"] // 128)
        def _(c):
            cc = pl.ds(pl.multiple_of(c * 128, 128), 128)
            gr = pl.multiple_of(block_rows(q, 0, c, dims), 128)
            t = held[pl.ds(gr, mat["m"]), :] * mat["a"][...]
            s = jnp.sum((t * t).reshape(-1, 8, 128), axis=0)
            bb = mat["b"][:, cc]
            su[q] += s * (bb * bb)

    def pay_rows(q):
        pay[pl.ds(q, 1), :] = jnp.sum(su[q], axis=0, keepdims=True)
        pay[pl.ds(3 + q, 1), :] = jnp.sum(sw[q], axis=0, keepdims=True)

    for q in range(3):
        first_reduce(q)
    pl.semaphore_wait(barrier, len(plane))
    sends = [c for q in range(3) for c in first_sends(q)]
    for c in sends:
        c.start()
    for c in sends:
        c.wait()
    for q in range(3):
        new_stats(q)
    for q in range(3):
        u_square(q)
        pay_rows(q)
    sends = [pltpu.make_async_remote_copy(pay, got.at[i], p_s.at[i], p_r.at[i], device_id=dev, device_id_type=MESH)
             for i, dev in enumerate(plane)]
    for c in sends:
        c.start()
    for c in sends:
        c.wait()
    total = ((pay[...] + got[0]) + (got[1] + got[2])) + ((got[3] + got[4]) + (got[5] + got[6]))
    total = jnp.sum(total, axis=1, keepdims=True)
    for q, mat in enumerate(mats):
        size = float(mat["mt"] * mat["nt"])
        r_mean = total[6 + q:7 + q] * (0.5 / mat["mt"])
        u_rms = jnp.sqrt(r_mean * total[q:q + 1] / size)
        w_rms = jnp.sqrt(total[3 + q:4 + q] / size)
        step = rel[0, 0] * jnp.maximum(EPS_SCALE, w_rms)
        k = step * jnp.sqrt(r_mean) / jnp.maximum(1.0, u_rms / clip[0, 0])
        mat["b"][...] = mat["b"][...] * k


def write_kernel(
    dims,
    held, a_g, a_u, a_d, b_g, b_u, b_d, r_g, c_g, r_u, c_u, r_d, c_d,
    o_g, o_u, o_d, or_g, oc_g, or_u, oc_u, or_d, oc_d,
    wide, tall, o_sem, s_sem,
):
    small = [pltpu.make_async_copy(s.at[0], d, s_sem.at[i]) for i, (s, d) in enumerate(
        [(r_g, or_g), (c_g, oc_g), (r_u, or_u), (c_u, oc_u), (r_d, or_d), (c_d, oc_d)])]
    for c in small:
        c.start()
    slots = 4
    pending = {}
    step = 0
    for q, a, b, o, buf in ((2, a_d, b_d, o_d, tall), (1, a_u, b_u, o_u, wide), (0, a_g, b_g, o_g, wide)):
        rows = buf.shape[1]
        for t in range(dims[q][0] // rows):
            slot = step % slots
            if slot in pending:
                pending.pop(slot).wait()
            rr = pl.ds(t * rows, rows)
            scale = a[rr, :]
            for c in range(dims[q][1] // 128):
                cc = pl.ds(c * 128, 128)
                g, w = (held[pl.ds(block_rows(q, z, c, dims) + t * rows, rows), :] for z in range(2))
                buf[slot, :, cc] = w - (g * scale) * b[:, cc]
            cp = pltpu.make_async_copy(buf.at[slot], o.at[rr, :], o_sem.at[slot])
            cp.start()
            pending[slot] = cp
            step += 1
    for cp in pending.values():
        cp.wait()
    for c in small:
        c.wait()


def solution(mesh):
    def local_program(x_in, h_act, d_gate, d_up, d_out, w_gate, w_up, w_down, r_gate, c_gate, r_up, c_up, r_down, c_down, beta_two, rel_step, clip_thr):
        (mg, ng), (md, nd) = w_gate.shape, w_down.shape
        tokens = x_in.shape[0]
        nk = tokens // KB
        big = [x_in, h_act, d_gate, d_up, d_out, w_gate, w_up, w_down, r_gate, c_gate, r_up, c_up, r_down, c_down]
        one = [v.reshape(1, 1) for v in (beta_two, rel_step, clip_thr)]
        big = [pltpu.with_memory_space_constraint(v, HB) for v in big]
        dims = [(mg, ng), (mg, ng), (md, nd)]
        mm, nn = max(mg, md), max(ng, nd)
        dma = pltpu.SemaphoreType.DMA

        def call(kernel, outs, args, in_spaces, out_space, scratch, mib, **params):
            return pl.pallas_call(
                functools.partial(kernel, dims),
                out_shape=outs,
                in_specs=[pl.BlockSpec(memory_space=v) for v in in_spaces],
                out_specs=tuple(pl.BlockSpec(memory_space=out_space) for _ in outs),
                scratch_shapes=scratch,
                compiler_params=pltpu.CompilerParams(vmem_limit_bytes=mib * 2**20, **params),
                name=kernel.__name__,
            )(*args)

        def vm(shapes):
            return tuple(VM(s, F32) for s in shapes)

        lanes = [(m, 128) for m, _ in dims]
        first = call(
            dot_kernel,
            vm([(2 * sum(m * n for m, n in dims) // 128, 128)] + lanes + [(8, n) for _, n in dims] + [(3, 8, 128), (3, 1, mm), (3, 1, nn)]),
            big, [HB] * len(big), VM,
            [
                VM((nk, KB, mg), BF16), VM((3, KB, md), BF16), VM((mg, tokens), BF16), VM((md, tokens), BF16),
                VM((RING, tokens, NT), BF16),
                dma((nk,)), dma((3,)), dma((RING,)), dma((2 * ng // NT + nd // NT, 2)), dma((6,)),
            ], 18)
        held, rest = first[:1], first[1:]
        stats = [s for m, n in dims for s in ((1, m), (1, n))]
        second = call(
            exchange_kernel,
            vm(lanes + [(1, n) for _, n in dims] + stats),
            held + rest + tuple(one), [VM] * len(first) + [pltpu.SMEM] * 3, VM,
            [
                VM((3, 8, 128), F32),
                VM((3, 1, mm), F32), VM((3, 1, mm), F32), VM((3, 1, nn), F32), VM((3, 3, 1, nn), F32),
                VM((16, 128), F32), VM((7, 16, 128), F32),
                dma((3,)), dma((3,)), dma((3, 3)), dma((3, 3)), dma((7,)), dma((7,)),
            ], 18, collective_id=0, has_side_effects=True)
        outs = call(
            write_kernel,
            tuple(jax.ShapeDtypeStruct(s, F32) for s in dims + [(k,) for mn in dims for k in mn]),
            held + second, [VM] * (1 + len(second)), HB,
            [VM((4, mg // 8, ng), F32), VM((4, md // 8, nd), F32), dma((4,)), dma((6,))], 18)
        return tuple(outs)

    act_spec = P(None, "row")
    cot_spec = P(None, "col")
    w_spec = P("row", "col")
    r_spec = P("row")
    c_spec = P("col")
    s_spec = P()
    return jax.shard_map(local_program, mesh=mesh, in_specs=(act_spec, act_spec, cot_spec, cot_spec, cot_spec, w_spec, w_spec, w_spec, r_spec, c_spec, r_spec, c_spec, r_spec, c_spec, s_spec, s_spec, s_spec), out_specs=(w_spec, w_spec, w_spec, r_spec, c_spec, r_spec, c_spec, r_spec, c_spec), check_vma=False)
```

```python
import functools

import jax
import jax.numpy as jnp
from jax import lax
from jax.experimental import pallas as pl
from jax.experimental.pallas import tpu as pltpu
from jax.sharding import PartitionSpec as P

EPS_SQ = 1e-30
EPS_SCALE = 1e-3
F32 = jnp.float32
BF16 = jnp.bfloat16
MESH = pl.DeviceIdType.MESH
VM = pltpu.VMEM
HB = pltpu.HBM
KB = 256
NT = 256
RING = 12
PIECES = (176, 80, 96)


def block_rows(q, w, c, dims):
    first = 0
    for m, n in (tuple(dims) + tuple(dims))[:q + 3 * w]:
        first += m * (n // 128)
    return first + c * dims[q][0]


def dot_kernel(
    dims,
    x, h, dg, du, dd, wg, wu, wd, rg, cg, ru, cu, rd, cd,
    held, rs_g, rs_u, rs_d, cs_g, cs_u, cs_d, sw, ro, co,
    xs, hs, xt, ht, ring, x_sem, h_sem, d_sem, w_sem, s_sem,
):
    tokens = x.shape[0]
    nk = tokens // KB
    mats = (
        dict(d=dg, wh=wg, rs=rs_g, cs=cs_g),
        dict(d=du, wh=wu, rs=rs_u, cs=cs_u),
        dict(d=dd, wh=wd, rs=rs_d, cs=cs_d),
    )
    for mat, (m, n) in zip(mats, dims):
        mat["m"], mat["n"] = m, n

    def x_copy(k):
        return pltpu.make_async_copy(x.at[pl.ds(k * KB, KB), :], xs.at[k], x_sem.at[k])

    def h_copy(k):
        return pltpu.make_async_copy(h.at[pl.ds(k * KB, KB), :], hs.at[k % 3], h_sem.at[k % 3])

    tiles = [(q, j) for q in range(3) for j in range(mats[q]["n"] // NT)]

    def d_copy(i):
        q, j = tiles[i]
        return pltpu.make_async_copy(mats[q]["d"].at[:, pl.ds(j * NT, NT)], ring.at[i % RING], d_sem.at[i % RING])

    def w_copy(i, half):
        q, j = tiles[i]
        dst = held.at[pl.ds(block_rows(q, 1, 2 * j + half, dims), mats[q]["m"]), :]
        return pltpu.make_async_copy(mats[q]["wh"].at[:, pl.ds(j * NT + half * 128, 128)], dst, w_sem.at[i, half])

    small = [
        pltpu.make_async_copy(src, dst.at[q, 0, pl.ds(0, src.shape[0])], s_sem.at[i])
        for i, (src, dst, q) in enumerate(
            [(rg, ro, 0), (ru, ro, 1), (rd, ro, 2), (cg, co, 0), (cu, co, 1), (cd, co, 2)])
    ]
    x_copy(0).start()
    d_copy(0).start()
    for k in range(1, nk):
        x_copy(k).start()
    for i in range(1, RING - 1):
        d_copy(i).start()
    for c in small:
        c.start()

    def h_turn(k):
        for c in range(ht.shape[0] // 128):
            ht[pl.ds(c * 128, 128), pl.ds(k * KB, KB)] = hs[k % 3, :, pl.ds(c * 128, 128)].T

    def w_square(i):
        q, j = tiles[i]
        w = held[pl.ds(block_rows(q, 1, 2 * j, dims), 2 * mats[q]["m"]), :]
        s = jnp.sum((w * w).reshape(-1, 8, 128), axis=0)
        if j == 0:
            sw[q] = s
        else:
            sw[q] += s

    units = []
    for i, (q, j) in enumerate(tiles):
        if q < 2:
            units.append((i, q, j, (0, 256), 256))
        else:
            units.append((i, q, j, (0, 352), 352))
            units.append((i, q, j, (704, 1056), 352))
    n_units = len(units)

    before = [[] for _ in range(n_units)]
    beside = [[] for _ in range(n_units)]
    for k in range(nk):
        before[k].append(lambda k=k: h_copy(k).start())
        before[k + 2].append(lambda k=k: h_copy(k).wait())
        beside[k + 2].append(lambda k=k: h_turn(k))
    w_at = [3 + i for i in range(len(tiles))]
    for i in range(len(tiles)):
        u = min(w_at[i], n_units - 4)
        before[u].append(lambda i=i: [w_copy(i, half).start() for half in range(2)])
        before[u + 3].append(lambda i=i: [w_copy(i, half).wait() for half in range(2)])
        beside[u + 3].append(lambda i=i: w_square(i))
    def run(*accs):
        accs = [[accs[(z * 2 + par) * 3:(z * 2 + par) * 3 + 3] for par in range(2)] for z in range(2)]

        def rhs(u, k):
            return ring[units[u][0] % RING, pl.ds(k * KB, KB), :]

        def lhs(q, r0, rows, k):
            src = ht if q == 2 else xt
            return src[pl.ds(r0, rows), pl.ds(k * KB, KB)]

        def drain(u):
            i, q, j, starts, rows = units[u]
            mat = mats[q]
            cc = None
            for z in range(2):
                r0, left = starts[z], rows
                for p, size in enumerate(PIECES):
                    if not left:
                        break
                    g = pltpu.matmul_pop(accs[z][u % 2][p])
                    for half in range(2):
                        gr = block_rows(q, 0, 2 * j + half, dims) + r0
                        held[pl.ds(gr, size), :] = g[:, half * 128:half * 128 + 128]
                    s = g * g
                    lanes = s[:, :128] + s[:, 128:]
                    if j == 0:
                        mat["rs"][pl.ds(r0, size), :] = lanes
                    else:
                        mat["rs"][pl.ds(r0, size), :] += lanes
                    s = jnp.sum(s.reshape(-1, 8, NT), axis=0)
                    cc = s if cc is None else cc + s
                    r0, left = r0 + size, left - size
            if q == 2 and starts[0]:
                mat["cs"][:, pl.ds(j * NT, NT)] += cc
            else:
                mat["cs"][:, pl.ds(j * NT, NT)] = cc

        for z in range(2):
            for par in range(2):
                for p in range(3):
                    pltpu.matmul_pop(accs[z][par][p])

        d_copy(0).wait()
        for u in range(n_units):
            i, q, j, starts, rows = units[u]
            last = u == n_units - 1
            if u == 0:
                x_copy(0).wait()
            for f in before[u]:
                f()
            if not last and units[u + 1][0] != i:
                d_copy(units[u + 1][0]).wait()
            new = u == 0 or units[u - 1][0] != i
            if new and u and i + RING - 2 < len(tiles):
                d_copy(i + RING - 2).start()
            if u == 0:
                for z in range(2):
                    pltpu.matmul_push_rhs(rhs(0, 0), staging_register=0, mxu_index=z)
            for k in range(nk):
                if u == 0:
                    if k:
                        x_copy(k).wait()
                    for z in range(2):
                        xt[pl.ds(z * 256, 256), pl.ds(k * KB, KB)] = xs[k, :, pl.ds(z * 256, 256)].T
                for z in range(2):
                    r0, left = starts[z], rows
                    for p, size in enumerate(PIECES):
                        if not left:
                            break
                        pltpu.matmul_acc_lhs(accs[z][u % 2][p], lhs(q, r0, size, k),
                                             load_staged_rhs=(k % 2 if p == 0 else None))
                        r0, left = r0 + size, left - size
                    if k < nk - 1:
                        pltpu.matmul_push_rhs(rhs(u, k + 1), staging_register=(k + 1) % 2, mxu_index=z)
                    elif not last:
                        pltpu.matmul_push_rhs(rhs(u + 1, 0), staging_register=0, mxu_index=z)
                if k == 1 and u:
                    drain(u - 1)
                if k == 2:
                    for f in beside[u]:
                        f()
        drain(n_units - 1)

    spec = [pltpu.ACC(z)((size, NT), F32) for z in range(2) for par in range(2) for size in PIECES]
    pl.run_scoped(run, *spec)

    for c in small:
        c.wait()


def exchange_kernel(
    dims,
    held, rs_g, rs_u, rs_d, cs_g, cs_u, cs_d, sw, ro, co,
    b2, rel, clip,
    a_g, a_u, a_d, b_g, b_u, b_d, r_g, c_g, r_u, c_u, r_d, c_d,
    su, rsend, rrecv, csend, crecv, pay, got, r1s, r1r, c1s, c1r, p_s, p_r,
):
    col = lax.axis_index("col")
    row = lax.axis_index("row")
    row_peer = (row + 1 - 2 * (row % 2), (row + 2) % 4, 3 - row)
    mats = (
        dict(rs=rs_g, cs=cs_g, a=a_g, b=b_g, r=r_g, c=c_g),
        dict(rs=rs_u, cs=cs_u, a=a_u, b=b_u, r=r_u, c=c_u),
        dict(rs=rs_d, cs=cs_d, a=a_d, b=b_d, r=r_d, c=c_d),
    )
    for mat, (m, n) in zip(mats, dims):
        mat["m"], mat["n"] = m, n
        mat["mt"], mat["nt"] = mat["m"] * 4, mat["n"] * 2

    barrier = pltpu.get_barrier_semaphore()
    plane = [{"row": p, "col": cc} for cc in (col, 1 - col) for p in (row,) + row_peer][1:]
    for dev in plane:
        pl.semaphore_signal(barrier, inc=1, device_id=dev, device_id_type=MESH)
    pay[...] = jnp.zeros_like(pay)

    def first_sends(q):
        mat = mats[q]
        m, n = mat["m"], mat["n"]
        copies = [pltpu.make_async_remote_copy(
            rsend.at[q, :, pl.ds(0, m)], rrecv.at[q, :, pl.ds(0, m)], r1s.at[q], r1r.at[q],
            device_id={"col": 1 - col}, device_id_type=MESH)]
        for d in range(3):
            copies.append(pltpu.make_async_remote_copy(
                csend.at[q, :, pl.ds(0, n)], crecv.at[q, d, :, pl.ds(0, n)], c1s.at[q, d], c1r.at[q, d],
                device_id={"row": row_peer[d]}, device_id_type=MESH))
        return copies

    def first_reduce(q):
        mat = mats[q]
        csend[q, :, pl.ds(0, mat["n"])] = jnp.sum(mat["cs"][...], axis=0, keepdims=True)
        for b in range(mat["m"] // 128):
            t = mat["rs"][pl.ds(b * 128, 128), :].T
            rsend[q, :, pl.ds(b * 128, 128)] = jnp.sum(t, axis=0, keepdims=True)

    def new_stats(q):
        mat = mats[q]
        m, n = mat["m"], mat["n"]
        beta = b2[0, 0]
        rsum = rsend[q, :, pl.ds(0, m)] + rrecv[q, :, pl.ds(0, m)]
        r_new = beta * ro[q, :, pl.ds(0, m)] + (1.0 - beta) * (rsum * (1.0 / mat["nt"]) + EPS_SQ)
        mat["r"][...] = r_new
        csum = (csend[q, :, pl.ds(0, n)] + crecv[q, 0, :, pl.ds(0, n)]) + (
            crecv[q, 1, :, pl.ds(0, n)] + crecv[q, 2, :, pl.ds(0, n)])
        c_new = beta * co[q, :, pl.ds(0, n)] + (1.0 - beta) * (csum * (1.0 / mat["mt"]) + EPS_SQ)
        mat["c"][...] = c_new
        mat["b"][...] = lax.rsqrt(c_new)
        alpha = lax.rsqrt(r_new)
        rp = r_new[:, :128]
        for b in range(m // 128):
            blk = jnp.broadcast_to(alpha[:, b * 128:(b + 1) * 128], (128, 128))
            mat["a"][pl.ds(b * 128, 128), :] = blk.T
            if b:
                rp = rp + r_new[:, b * 128:(b + 1) * 128]
        pay[pl.ds(6 + q, 1), :] = rp

    def u_square(q):
        mat = mats[q]
        su[q] = jnp.zeros((8, 128), F32)

        @pl.loop(0, mat["n"] // 128)
        def _(c):
            cc = pl.ds(pl.multiple_of(c * 128, 128), 128)
            gr = pl.multiple_of(block_rows(q, 0, c, dims), 128)
            t = held[pl.ds(gr, mat["m"]), :] * mat["a"][...]
            s = jnp.sum((t * t).reshape(-1, 8, 128), axis=0)
            bb = mat["b"][:, cc]
            su[q] += s * (bb * bb)

    def pay_rows(q):
        pay[pl.ds(q, 1), :] = jnp.sum(su[q], axis=0, keepdims=True)
        pay[pl.ds(3 + q, 1), :] = jnp.sum(sw[q], axis=0, keepdims=True)

    for q in range(3):
        first_reduce(q)
    pl.semaphore_wait(barrier, len(plane))
    sends = [c for q in range(3) for c in first_sends(q)]
    for c in sends:
        c.start()
    for c in sends:
        c.wait()
    for q in range(3):
        new_stats(q)
    for q in range(3):
        u_square(q)
        pay_rows(q)
    sends = [pltpu.make_async_remote_copy(pay, got.at[i], p_s.at[i], p_r.at[i], device_id=dev, device_id_type=MESH)
             for i, dev in enumerate(plane)]
    for c in sends:
        c.start()
    for c in sends:
        c.wait()
    total = ((pay[...] + got[0]) + (got[1] + got[2])) + ((got[3] + got[4]) + (got[5] + got[6]))
    total = jnp.sum(total, axis=1, keepdims=True)
    for q, mat in enumerate(mats):
        size = float(mat["mt"] * mat["nt"])
        r_mean = total[6 + q:7 + q] * (0.5 / mat["mt"])
        u_rms = jnp.sqrt(r_mean * total[q:q + 1] / size)
        w_rms = jnp.sqrt(total[3 + q:4 + q] / size)
        step = rel[0, 0] * jnp.maximum(EPS_SCALE, w_rms)
        k = step * jnp.sqrt(r_mean) / jnp.maximum(1.0, u_rms / clip[0, 0])
        mat["b"][...] = mat["b"][...] * k


def write_kernel(
    dims,
    held, a_g, a_u, a_d, b_g, b_u, b_d, r_g, c_g, r_u, c_u, r_d, c_d,
    o_g, o_u, o_d, or_g, oc_g, or_u, oc_u, or_d, oc_d,
    wide, tall, o_sem, s_sem,
):
    small = [pltpu.make_async_copy(s.at[0], d, s_sem.at[i]) for i, (s, d) in enumerate(
        [(r_g, or_g), (c_g, oc_g), (r_u, or_u), (c_u, oc_u), (r_d, or_d), (c_d, oc_d)])]
    for c in small:
        c.start()
    slots = 8
    pending = {}
    step = 0
    for q, a, b, o, buf in ((2, a_d, b_d, o_d, tall), (1, a_u, b_u, o_u, wide), (0, a_g, b_g, o_g, wide)):
        rows = buf.shape[1]
        for t in range(dims[q][0] // rows):
            slot = step % slots
            if slot in pending:
                pending.pop(slot).wait()
            rr = pl.ds(t * rows, rows)
            scale = a[rr, :]
            for c in range(dims[q][1] // 128):
                cc = pl.ds(c * 128, 128)
                g, w = (held[pl.ds(block_rows(q, z, c, dims) + t * rows, rows), :] for z in range(2))
                buf[slot, :, cc] = w - (g * scale) * b[:, cc]
            cp = pltpu.make_async_copy(buf.at[slot], o.at[rr, :], o_sem.at[slot])
            cp.start()
            pending[slot] = cp
            step += 1
    for cp in pending.values():
        cp.wait()
    for c in small:
        c.wait()


def solution(mesh):
    def local_program(x_in, h_act, d_gate, d_up, d_out, w_gate, w_up, w_down, r_gate, c_gate, r_up, c_up, r_down, c_down, beta_two, rel_step, clip_thr):
        (mg, ng), (md, nd) = w_gate.shape, w_down.shape
        tokens = x_in.shape[0]
        nk = tokens // KB
        big = [x_in, h_act, d_gate, d_up, d_out, w_gate, w_up, w_down, r_gate, c_gate, r_up, c_up, r_down, c_down]
        one = [v.reshape(1, 1) for v in (beta_two, rel_step, clip_thr)]
        big = [pltpu.with_memory_space_constraint(v, HB) for v in big]
        dims = [(mg, ng), (mg, ng), (md, nd)]
        mm, nn = max(mg, md), max(ng, nd)
        dma = pltpu.SemaphoreType.DMA

        def call(kernel, outs, args, in_spaces, out_space, scratch, mib, **params):
            return pl.pallas_call(
                functools.partial(kernel, dims),
                out_shape=outs,
                in_specs=[pl.BlockSpec(memory_space=v) for v in in_spaces],
                out_specs=tuple(pl.BlockSpec(memory_space=out_space) for _ in outs),
                scratch_shapes=scratch,
                compiler_params=pltpu.CompilerParams(vmem_limit_bytes=mib * 2**20, **params),
                name=kernel.__name__,
            )(*args)

        def vm(shapes):
            return tuple(VM(s, F32) for s in shapes)

        lanes = [(m, 128) for m, _ in dims]
        first = call(
            dot_kernel,
            vm([(2 * sum(m * n for m, n in dims) // 128, 128)] + lanes + [(8, n) for _, n in dims] + [(3, 8, 128), (3, 1, mm), (3, 1, nn)]),
            big, [HB] * len(big), VM,
            [
                VM((nk, KB, mg), BF16), VM((3, KB, md), BF16), VM((mg, tokens), BF16), VM((md, tokens), BF16),
                VM((RING, tokens, NT), BF16),
                dma((nk,)), dma((3,)), dma((RING,)), dma((2 * ng // NT + nd // NT, 2)), dma((6,)),
            ], 26)
        held, rest = first[:1], first[1:]
        stats = [s for m, n in dims for s in ((1, m), (1, n))]
        second = call(
            exchange_kernel,
            vm(lanes + [(1, n) for _, n in dims] + stats),
            tuple(pltpu.with_memory_space_constraint(v, VM) for v in held + rest) + tuple(one), [VM] * len(first) + [pltpu.SMEM] * 3, VM,
            [
                VM((3, 8, 128), F32),
                VM((3, 1, mm), F32), VM((3, 1, mm), F32), VM((3, 1, nn), F32), VM((3, 3, 1, nn), F32),
                VM((16, 128), F32), VM((7, 16, 128), F32),
                dma((3,)), dma((3,)), dma((3, 3)), dma((3, 3)), dma((7,)), dma((7,)),
            ], 26, collective_id=0, has_side_effects=True)
        outs = call(
            write_kernel,
            tuple(jax.ShapeDtypeStruct(s, F32) for s in dims + [(k,) for mn in dims for k in mn]),
            tuple(pltpu.with_memory_space_constraint(v, VM) for v in held + second), [VM] * (1 + len(second)), HB,
            [VM((8, mg // 8, ng), F32), VM((8, md // 8, nd), F32), dma((8,)), dma((6,))], 26)
        return tuple(outs)

    act_spec = P(None, "row")
    cot_spec = P(None, "col")
    w_spec = P("row", "col")
    r_spec = P("row")
    c_spec = P("col")
    s_spec = P()
    return jax.shard_map(local_program, mesh=mesh, in_specs=(act_spec, act_spec, cot_spec, cot_spec, cot_spec, w_spec, w_spec, w_spec, r_spec, c_spec, r_spec, c_spec, r_spec, c_spec, s_spec, s_spec, s_spec), out_specs=(w_spec, w_spec, w_spec, r_spec, c_spec, r_spec, c_spec, r_spec, c_spec), check_vma=False)
```

```python
import functools

import jax
import jax.numpy as jnp
from jax import lax
from jax.experimental import pallas as pl
from jax.experimental.pallas import tpu as pltpu
from jax.sharding import PartitionSpec as P

EPS_SQ = 1e-30
EPS_SCALE = 1e-3
F32 = jnp.float32
BF16 = jnp.bfloat16
MESH = pl.DeviceIdType.MESH
VM = pltpu.VMEM
HB = pltpu.HBM
KB = 256
NT = 256
RING = 11
PIECES = (128, 128)
GRANT = 18
CHUNKS = 4


def fold(v):
    slabs = v.reshape(-1, 8, v.shape[1])
    n = slabs.shape[0] // 4 * 4
    s = jnp.sum(slabs[:n].reshape(-1, 4, 8, v.shape[1]), axis=0)
    s = (s[0] + s[1]) + (s[2] + s[3])
    for i in range(n, slabs.shape[0]):
        s = s + slabs[i]
    return s


def dot_kernel(
    dims,
    x, h, dg, du, dd, wg, rg, cg, ru, cu, rd, cd,
    held, ht, dt, rs_g, rs_u, cs_g, cs_u, sw, ro, co,
    xs, hs, xt, ring, x_sem, h_sem, d_sem, first_sem, t_sem, w_sem, s_sem,
):
    m, n = dims[0]
    nk = x.shape[0] // KB
    up = n // NT
    cots, rss, css = (dg, du), (rs_g, rs_u), (cs_g, cs_u)
    n_units = 2 * up

    def x_copy(k):
        return pltpu.make_async_copy(x.at[pl.ds(k * KB, KB), :], xs.at[k], x_sem.at[k])

    def h_copy(k):
        return pltpu.make_async_copy(h.at[pl.ds(k * KB, KB), :], hs.at[k % 3], h_sem.at[k % 3])

    def d_copy(u):
        q, j = divmod(u, up)
        return pltpu.make_async_copy(cots[q].at[:, pl.ds(j * NT, NT)], ring.at[u % RING], d_sem.at[u % RING])

    def first_copy(k):
        return pltpu.make_async_copy(dg.at[pl.ds(k * KB, KB), pl.ds(0, NT)], ring.at[0, pl.ds(k * KB, KB), :], first_sem.at[k])

    def t_copy(j):
        return pltpu.make_async_copy(dd.at[:, pl.ds(j * NT, NT)], dt.at[j], t_sem.at[j])

    def w_copy(c):
        return pltpu.make_async_copy(wg.at[:, pl.ds(c * 128, 128)], held.at[pl.ds(2 * m * (n // 128) + c * m, m), :], w_sem.at[c])

    small = [
        pltpu.make_async_copy(src, dst.at[q, 0, pl.ds(0, src.shape[0])], s_sem.at[i])
        for i, (src, dst, q) in enumerate(
            [(rg, ro, 0), (ru, ro, 1), (rd, ro, 2), (cg, co, 0), (cu, co, 1), (cd, co, 2)])
    ]
    for k in range(nk):
        x_copy(k).start()
        first_copy(k).start()

    def h_turn(k):
        for c in range(ht.shape[0] // 128):
            ht[pl.ds(c * 128, 128), pl.ds(k * KB, KB)] = hs[k % 3, :, pl.ds(c * 128, 128)].T

    def w_square(c):
        w = held[pl.ds(2 * m * (n // 128) + c * m, m), :]
        s = fold(w * w)
        if c == 0:
            sw[...] = s
        else:
            sw[...] += s

    before = [[] for _ in range(n_units)]
    beside = [[] for _ in range(n_units)]
    for k in range(nk):
        before[k + 1].append(lambda k=k: h_copy(k).start())
        before[k + 3].append(lambda k=k: h_copy(k).wait())
        beside[k + 3].append(lambda k=k: h_turn(k))
    for j in range(dt.shape[0]):
        before[10 + 2 * j].append(lambda j=j: t_copy(j).start())
        before[min(16 + 2 * j, n_units - 1)].append(lambda j=j: t_copy(j).wait())
    for c in range(n // 128):
        u = 9 + c // 3
        before[u].append(lambda c=c: w_copy(c).start())
        before[u + 4].append(lambda c=c: w_copy(c).wait())
        beside[u + 4].append(lambda c=c: w_square(c))
    before[8].append(lambda: [c.start() for c in small])
    before[20].append(lambda: [c.wait() for c in small])

    def run(*accs):
        def acc(z, par, p):
            return accs[(z * 2 + par) * 2 + p]

        def rhs(u, k):
            return ring[u % RING, pl.ds(k * KB, KB), :]

        def drain(u):
            q, j = divmod(u, up)
            cc = None
            for z in range(2):
                for p, size in enumerate(PIECES):
                    r0 = z * sum(PIECES) + sum(PIECES[:p])
                    g = pltpu.matmul_pop(acc(z, u % 2, p))
                    for half in range(2):
                        held[pl.ds((q * (n // 128) + 2 * j + half) * m + r0, size), :] = g[:, half * 128:half * 128 + 128]
                    s = g * g
                    lanes = s[:, :128] + s[:, 128:]
                    if j == 0:
                        rss[q][pl.ds(r0, size), :] = lanes
                    else:
                        rss[q][pl.ds(r0, size), :] += lanes
                    s = fold(s)
                    cc = s if cc is None else cc + s
            css[q][:, pl.ds(j * NT, NT)] = cc

        for z in range(2):
            for par in range(2):
                for p in range(2):
                    pltpu.matmul_pop(acc(z, par, p))

        for u in range(n_units):
            last = u == n_units - 1
            for f in before[u]:
                f()
            if u:
                if not last:
                    d_copy(u + 1).wait()
                if u + RING - 2 < n_units:
                    d_copy(u + RING - 2).start()
            for k in range(nk):
                if u == 0:
                    x_copy(k).wait()
                    first_copy(k).wait()
                    for z in range(2):
                        xt[pl.ds(z * 256, 256), pl.ds(k * KB, KB)] = xs[k, :, pl.ds(z * 256, 256)].T
                        pltpu.matmul_push_rhs(rhs(0, k), staging_register=k % 2, mxu_index=z)
                    if k == 0:
                        for i in range(1, 4):
                            d_copy(i).start()
                    elif k + 3 <= RING - 2:
                        d_copy(k + 3).start()
                    if k == nk - 1:
                        for i in range(nk + 3, RING - 1):
                            d_copy(i).start()
                        d_copy(1).wait()
                for z in range(2):
                    for p, size in enumerate(PIECES):
                        r0 = z * sum(PIECES) + sum(PIECES[:p])
                        pltpu.matmul_acc_lhs(acc(z, u % 2, p), xt[pl.ds(r0, size), pl.ds(k * KB, KB)],
                                             load_staged_rhs=(k % 2 if p == 0 else None))
                    if k < nk - 1:
                        if u:
                            pltpu.matmul_push_rhs(rhs(u, k + 1), staging_register=(k + 1) % 2, mxu_index=z)
                    elif not last:
                        pltpu.matmul_push_rhs(rhs(u + 1, 0), staging_register=0, mxu_index=z)
                if k == 1 and u:
                    drain(u - 1)
                if k == 2:
                    for f in beside[u]:
                        f()
        drain(n_units - 1)

    pl.run_scoped(run, *[pltpu.ACC(z)((size, NT), F32) for z in range(2) for par in range(2) for size in PIECES])


def exchange_kernel(
    dims,
    held, ht, dt, rs_g, rs_u, cs_g, cs_u, sw_g, ro, co,
    wu, wd,
    b2, rel, clip,
    late, a_g, a_u, a_d, b_g, b_u, b_d, r_g, c_g, r_u, c_u, r_d, c_d,
    rs_d, cs_d, su, sw, rsend, rrecv, csend, crecv, pay, got, w_sem, r1s, r1r, c1s, c1r, p_s, p_r,
):
    col = lax.axis_index("col")
    row = lax.axis_index("row")
    row_peer = (row + 1 - 2 * (row % 2), (row + 2) % 4, 3 - row)
    mats = (
        dict(rs=rs_g, cs=cs_g, a=a_g, b=b_g, r=r_g, c=c_g),
        dict(rs=rs_u, cs=cs_u, a=a_u, b=b_u, r=r_u, c=c_u),
        dict(rs=rs_d, cs=cs_d, a=a_d, b=b_d, r=r_d, c=c_d),
    )
    for mat, (m, n) in zip(mats, dims):
        mat["m"], mat["n"] = m, n
        mat["mt"], mat["nt"] = m * 4, n * 2
    (mg, ng), (md, nd) = dims[0], dims[2]
    size = mg * ng // 128

    barrier = pltpu.get_barrier_semaphore()
    plane = [{"row": p, "col": cc} for cc in (col, 1 - col) for p in (row,) + row_peer][1:]
    for dev in plane:
        pl.semaphore_signal(barrier, inc=1, device_id=dev, device_id_type=MESH)

    def w_copy(i):
        q, c = (1, i) if i < ng // 128 else (2, i - ng // 128)
        m = dims[q][0]
        return pltpu.make_async_copy((wu, wd)[q - 1].at[:, pl.ds(c * 128, 128)], late.at[pl.ds(q * size + c * m, m), :], w_sem.at[i])

    blocks = ng // 128 + nd // 128
    for i in range(blocks):
        w_copy(i).start()
    pay[...] = jnp.zeros_like(pay)
    sw[0] = sw_g[...]

    def w_square(i):
        q, c = (1, i) if i < ng // 128 else (2, i - ng // 128)
        m = dims[q][0]
        w = late[pl.ds(q * size + c * m, m), :]
        s = fold(w * w)
        if c == 0:
            sw[q] = s
        else:
            sw[q] += s

    def first_sends(q):
        mat = mats[q]
        m, n = mat["m"], mat["n"]
        copies = [pltpu.make_async_remote_copy(
            rsend.at[q, :, pl.ds(0, m)], rrecv.at[q, :, pl.ds(0, m)], r1s.at[q], r1r.at[q],
            device_id={"col": 1 - col}, device_id_type=MESH)]
        for d in range(3):
            copies.append(pltpu.make_async_remote_copy(
                csend.at[q, :, pl.ds(0, n)], crecv.at[q, d, :, pl.ds(0, n)], c1s.at[q, d], c1r.at[q, d],
                device_id={"row": row_peer[d]}, device_id_type=MESH))
        return copies

    def first_reduce(q):
        mat = mats[q]
        csend[q, :, pl.ds(0, mat["n"])] = jnp.sum(mat["cs"][...], axis=0, keepdims=True)
        for b in range(mat["m"] // 128):
            t = mat["rs"][pl.ds(b * 128, 128), :].T
            rsend[q, :, pl.ds(b * 128, 128)] = jnp.sum(t, axis=0, keepdims=True)

    def new_stats(q):
        mat = mats[q]
        m, n = mat["m"], mat["n"]
        beta = b2[0, 0]
        rsum = rsend[q, :, pl.ds(0, m)] + rrecv[q, :, pl.ds(0, m)]
        r_new = beta * ro[q, :, pl.ds(0, m)] + (1.0 - beta) * (rsum * (1.0 / mat["nt"]) + EPS_SQ)
        mat["r"][...] = r_new
        csum = (csend[q, :, pl.ds(0, n)] + crecv[q, 0, :, pl.ds(0, n)]) + (
            crecv[q, 1, :, pl.ds(0, n)] + crecv[q, 2, :, pl.ds(0, n)])
        c_new = beta * co[q, :, pl.ds(0, n)] + (1.0 - beta) * (csum * (1.0 / mat["mt"]) + EPS_SQ)
        mat["c"][...] = c_new
        mat["b"][...] = lax.rsqrt(c_new)
        alpha = lax.rsqrt(r_new)
        rp = r_new[:, :128]
        for b in range(m // 128):
            blk = jnp.broadcast_to(alpha[:, b * 128:(b + 1) * 128], (128, 128))
            mat["a"][pl.ds(b * 128, 128), :] = blk.T
            if b:
                rp = rp + r_new[:, b * 128:(b + 1) * 128]
        pay[pl.ds(6 + q, 1), :] = rp

    def u_square(q, c):
        mat = mats[q]
        m = mat["m"]
        g = late[pl.ds(c * m, m), :] if q == 2 else held[pl.ds(q * size + c * m, m), :]
        t = g * mat["a"][...]
        bb = mat["b"][:, c * 128:(c + 1) * 128]
        s = fold(t * t) * (bb * bb)
        if c == 0:
            su[q] = s
        else:
            su[q] += s

    def pay_rows(q):
        pay[pl.ds(q, 1), :] = jnp.sum(su[q], axis=0, keepdims=True)
        pay[pl.ds(3 + q, 1), :] = jnp.sum(sw[q], axis=0, keepdims=True)

    rows = md // CHUNKS
    steps = nd // NT * CHUNKS

    def product(i):
        j, c = divmod(i, CHUNKS)
        rr = pl.ds(c * rows, rows)
        g = jnp.dot(ht[rr, :], dt[j], preferred_element_type=F32)
        for half in range(2):
            late[pl.ds((2 * j + half) * md + c * rows, rows), :] = g[:, half * 128:half * 128 + 128]
        s = g * g
        lanes = s[:, :128] + s[:, 128:]
        if j == 0:
            rs_d[rr, :] = lanes
        else:
            rs_d[rr, :] += lanes
        cc = pl.ds(j * NT, NT)
        if c == 0:
            cs_d[:, cc] = fold(s)
        else:
            cs_d[:, cc] += fold(s)

    sends = [c for q in range(2) for c in first_sends(q)]
    tasks = [[] for _ in range(steps)]
    tasks[0] = [lambda: first_reduce(0), lambda: first_reduce(1)]
    for i in range(blocks):
        tasks[3 + i * (steps - 3) // blocks].append(lambda i=i: w_square(i))
    todo = [(q, c) for q in range(2) for c in range(ng // 128)]
    at = 10
    for t, (q, c) in enumerate(todo):
        tasks[at + t * (steps - at) // len(todo)].append(lambda q=q, c=c: u_square(q, c))
    seen = 0
    for i in range(steps):
        if i == 4:
            pl.semaphore_wait(barrier, len(plane))
            for c in sends:
                c.start()
        if i == at:
            for c in sends:
                c.wait()
            new_stats(0)
            new_stats(1)
        if i >= 3:
            while seen < blocks and 3 + seen * (steps - 3) // blocks == i:
                w_copy(seen).wait()
                seen += 1
        product(i)
        for f in tasks[i]:
            f()
    pay_rows(0)
    pay_rows(1)

    first_reduce(2)
    sends = first_sends(2)
    for c in sends:
        c.start()
    for c in sends:
        c.wait()
    new_stats(2)
    for c in range(nd // 128):
        u_square(2, c)
    pay_rows(2)
    sends = [pltpu.make_async_remote_copy(pay, got.at[i], p_s.at[i], p_r.at[i], device_id=dev, device_id_type=MESH)
             for i, dev in enumerate(plane)]
    for c in sends:
        c.start()
    for c in sends:
        c.wait()
    total = ((pay[...] + got[0]) + (got[1] + got[2])) + ((got[3] + got[4]) + (got[5] + got[6]))
    total = jnp.sum(total, axis=1, keepdims=True)
    for q, mat in enumerate(mats):
        size = float(mat["mt"] * mat["nt"])
        r_mean = total[6 + q:7 + q] * (0.5 / mat["mt"])
        u_rms = jnp.sqrt(r_mean * total[q:q + 1] / size)
        w_rms = jnp.sqrt(total[3 + q:4 + q] / size)
        step = rel[0, 0] * jnp.maximum(EPS_SCALE, w_rms)
        k = step * jnp.sqrt(r_mean) / jnp.maximum(1.0, u_rms / clip[0, 0])
        mat["b"][...] = mat["b"][...] * k


def write_kernel(
    dims,
    held, ht, dt, rs_g, rs_u, cs_g, cs_u, sw_g, ro, co,
    late, a_g, a_u, a_d, b_g, b_u, b_d, r_g, c_g, r_u, c_u, r_d, c_d,
    o_g, o_u, o_d, or_g, oc_g, or_u, oc_u, or_d, oc_d,
    wide, tall, o_sem, s_sem,
):
    small = [pltpu.make_async_copy(s.at[0], d, s_sem.at[i]) for i, (s, d) in enumerate(
        [(r_g, or_g), (c_g, oc_g), (r_u, or_u), (c_u, oc_u), (r_d, or_d), (c_d, oc_d)])]
    for c in small:
        c.start()
    slots = 8
    size = dims[0][0] * dims[0][1] // 128
    where = (((held, 0), (held, 2)), ((held, 1), (late, 1)), ((late, 0), (late, 2)))
    pending = {}
    step = 0
    for q, a, b, o, buf in ((2, a_d, b_d, o_d, tall), (1, a_u, b_u, o_u, wide), (0, a_g, b_g, o_g, wide)):
        rows = buf.shape[1]
        for t in range(dims[q][0] // rows):
            slot = step % slots
            if slot in pending:
                pending.pop(slot).wait()
            rr = pl.ds(t * rows, rows)
            scale = a[rr, :]
            for c in range(dims[q][1] // 128):
                cc = pl.ds(c * 128, 128)
                off = c * dims[q][0] + t * rows
                g, w = (ref[pl.ds(k * size + off, rows), :] for ref, k in where[q])
                buf[slot, :, cc] = w - (g * scale) * b[:, cc]
            cp = pltpu.make_async_copy(buf.at[slot], o.at[rr, :], o_sem.at[slot])
            cp.start()
            pending[slot] = cp
            step += 1
    for cp in pending.values():
        cp.wait()
    for c in small:
        c.wait()


def solution(mesh):
    def local_program(x_in, h_act, d_gate, d_up, d_out, w_gate, w_up, w_down, r_gate, c_gate, r_up, c_up, r_down, c_down, beta_two, rel_step, clip_thr):
        (mg, ng), (md, nd) = w_gate.shape, w_down.shape
        tokens = x_in.shape[0]
        nk = tokens // KB
        def hbm(*arrays):
            return tuple(pltpu.with_memory_space_constraint(v, HB) for v in arrays)

        def vmem(*arrays):
            return tuple(pltpu.with_memory_space_constraint(v, VM) for v in arrays)

        one = tuple(v.reshape(1, 1) for v in (beta_two, rel_step, clip_thr))
        dims = [(mg, ng), (mg, ng), (md, nd)]
        mm, nn = max(mg, md), max(ng, nd)
        dma = pltpu.SemaphoreType.DMA
        blocks = ng // 128 + nd // 128

        def call(kernel, outs, args, in_spaces, out_space, scratch, **params):
            return pl.pallas_call(
                functools.partial(kernel, dims),
                out_shape=outs,
                in_specs=[pl.BlockSpec(memory_space=v) for v in in_spaces],
                out_specs=tuple(pl.BlockSpec(memory_space=out_space) for _ in outs),
                scratch_shapes=scratch,
                compiler_params=pltpu.CompilerParams(vmem_limit_bytes=GRANT * 2**20, **params),
                name=kernel.__name__,
            )(*args)

        def vm(shapes):
            return tuple(VM(s, F32) for s in shapes)

        def vm(shapes):
            return tuple(VM(s, F32) for s in shapes)

        held_shape = (3 * mg * ng // 128, 128)
        lanes = [(m, 128) for m, _ in dims]
        stats = [s for m, n in dims for s in ((1, m), (1, n))]
        first = call(
            dot_kernel,
            vm([held_shape]) + (VM((md, tokens), BF16), VM((nd // NT, tokens, NT), BF16))
            + vm(lanes[:2] + [(8, ng), (8, ng), (8, 128), (3, 1, mm), (3, 1, nn)]),
            hbm(x_in, h_act, d_gate, d_up, d_out, w_gate, r_gate, c_gate, r_up, c_up, r_down, c_down), [HB] * 12, VM,
            [
                VM((nk, KB, mg), BF16), VM((3, KB, md), BF16), VM((mg, tokens), BF16), VM((RING, tokens, NT), BF16),
                dma((nk,)), dma((3,)), dma((RING,)), dma((nk,)), dma((nd // NT,)), dma((ng // 128,)), dma((6,)),
            ])
        second = call(
            exchange_kernel,
            vm([held_shape] + lanes + [(1, n) for _, n in dims] + stats),
            vmem(*first) + hbm(w_up, w_down) + one, [VM] * len(first) + [HB] * 2 + [pltpu.SMEM] * 3, VM,
            [
                VM((md, 128), F32), VM((8, nd), F32), VM((3, 8, 128), F32), VM((3, 8, 128), F32),
                VM((3, 1, mm), F32), VM((3, 1, mm), F32), VM((3, 1, nn), F32), VM((3, 3, 1, nn), F32),
                VM((16, 128), F32), VM((7, 16, 128), F32), dma((blocks,)),
                dma((3,)), dma((3,)), dma((3, 3)), dma((3, 3)), dma((7,)), dma((7,)),
            ], collective_id=0, has_side_effects=True)
        outs = call(
            write_kernel,
            tuple(jax.ShapeDtypeStruct(s, F32) for s in dims + [(k,) for mn in dims for k in mn]),
            vmem(*first, *second), [VM] * (len(first) + len(second)), HB,
            [VM((8, mg // 8, ng), F32), VM((8, md // 8, nd), F32), dma((8,)), dma((6,))])
        return tuple(outs)

    act_spec = P(None, "row")
    cot_spec = P(None, "col")
    w_spec = P("row", "col")
    r_spec = P("row")
    c_spec = P("col")
    s_spec = P()
    return jax.shard_map(local_program, mesh=mesh, in_specs=(act_spec, act_spec, cot_spec, cot_spec, cot_spec, w_spec, w_spec, w_spec, r_spec, c_spec, r_spec, c_spec, r_spec, c_spec, s_spec, s_spec, s_spec), out_specs=(w_spec, w_spec, w_spec, r_spec, c_spec, r_spec, c_spec, r_spec, c_spec), check_vma=False)
```

```python
import functools

import jax
import jax.numpy as jnp
from jax import lax
from jax.experimental import pallas as pl
from jax.experimental.pallas import tpu as pltpu
from jax.sharding import PartitionSpec as P

EPS_SQ = 1e-30
EPS_SCALE = 1e-3
F32 = jnp.float32
BF16 = jnp.bfloat16
MESH = pl.DeviceIdType.MESH
VM = pltpu.VMEM
HB = pltpu.HBM
KB = 256
NT = 256
WIDE = 2 * NT
HB_ROWS = 512
RING = 5
PIECES = (128, 128)
GRANT = 18
CHUNKS = 4


def fold(v):
    slabs = v.reshape(-1, 8, v.shape[1])
    n = slabs.shape[0] // 4 * 4
    s = jnp.sum(slabs[:n].reshape(-1, 4, 8, v.shape[1]), axis=0)
    s = (s[0] + s[1]) + (s[2] + s[3])
    for i in range(n, slabs.shape[0]):
        s = s + slabs[i]
    return s


def dot_kernel(
    dims,
    x, h, dg, du, dd, wgh, wuh, wdh, rg, cg, ru, cu, rd, cd,
    held, ht, dt, wg, wu, wd, rs_g, rs_u, cs_g, cs_u, sw, ro, co,
    xs, hs, xt, ring, x_sem, h_sem, d_sem, first_sem, big_sem, s_sem,
):
    m, n = dims[0]
    nk = x.shape[0] // KB
    up = n // NT
    cots, rss, css = (dg, du), (rs_g, rs_u), (cs_g, cs_u)
    n_units = 2 * up
    tiles, unit_tile = [], []
    for q in range(2):
        for c0 in range(0, n, WIDE):
            cols = min(WIDE, n - c0)
            for off in range(0, cols, NT):
                unit_tile.append((len(tiles), off))
            tiles.append((q, c0, cols))

    def x_copy(k):
        return pltpu.make_async_copy(x.at[pl.ds(k * KB, KB), :], xs.at[k], x_sem.at[k])

    def first_copy(k):
        return pltpu.make_async_copy(dg.at[pl.ds(k * KB, KB), pl.ds(0, WIDE)], ring.at[0, pl.ds(k * KB, KB), :], first_sem.at[k])

    def d_copy(t):
        q, c0, cols = tiles[t]
        return pltpu.make_async_copy(cots[q].at[:, pl.ds(c0, cols)], ring.at[t % RING, :, pl.ds(0, cols)], d_sem.at[t % RING])

    def h_copy(k):
        return pltpu.make_async_copy(h.at[pl.ds(k * HB_ROWS, HB_ROWS), :], hs.at[k % 2], h_sem.at[k % 2])

    bigs = [pltpu.make_async_copy(a, b, big_sem.at[i]) for i, (a, b) in enumerate(((wgh, wg), (dd, dt), (wuh, wu), (wdh, wd)))]
    small = [
        pltpu.make_async_copy(src, dst.at[q, 0, pl.ds(0, src.shape[0])], s_sem.at[i])
        for i, (src, dst, q) in enumerate(
            [(rg, ro, 0), (ru, ro, 1), (rd, ro, 2), (cg, co, 0), (cu, co, 1), (cd, co, 2)])
    ]
    for k in range(nk):
        x_copy(k).start()
        first_copy(k).start()

    blocks = ht.shape[0] // 128

    def h_turn(k, part):
        for c in range(part * (blocks // 2), blocks if part else blocks // 2):
            ht[pl.ds(c * 128, 128), pl.ds(k * HB_ROWS, HB_ROWS)] = hs[k % 2, :, pl.ds(c * 128, 128)].T

    def w_square(c):
        w = wg[:, pl.ds(c * 128, 128)]
        s = fold(w * w)
        if c == 0:
            sw[...] = s
        else:
            sw[...] += s

    before = {u: [] for u in range(n_units)}
    beside = [[] for _ in range(n_units)]
    before[1] += [h_copy(0).start, h_copy(1).start]
    before[3] += [h_copy(0).wait]
    before[5] += [h_copy(1).wait, h_copy(2).start]
    before[7] += [h_copy(2).wait, h_copy(3).start]
    before[9] += [h_copy(3).wait]
    for k in range(4):
        for part in range(2):
            beside[3 + 2 * k + part].append(lambda k=k, part=part: h_turn(k, part))
    before[7].append(bigs[0].start)
    before[10].append(bigs[1].start)
    before[12].append(bigs[2].start)
    before[14].append(bigs[3].start)
    before[16].append(bigs[0].wait)
    for c in range(n // 128):
        beside[16 + c // 5].append(lambda c=c: w_square(c))

    def run(*accs):
        def acc(z, par, p):
            return accs[(z * 2 + par) * 2 + p]

        def rhs(u, k):
            t, off = unit_tile[u]
            return ring[t % RING, pl.ds(k * KB, KB), pl.ds(off, NT)]

        def drain(u):
            q, j = divmod(u, up)
            cc = None
            for z in range(2):
                for p, size in enumerate(PIECES):
                    r0 = z * sum(PIECES) + sum(PIECES[:p])
                    g = pltpu.matmul_pop(acc(z, u % 2, p))
                    for half in range(2):
                        held[pl.ds((q * (n // 128) + 2 * j + half) * m + r0, size), :] = g[:, half * 128:half * 128 + 128]
                    s = g * g
                    lanes = s[:, :128] + s[:, 128:]
                    if j == 0:
                        rss[q][pl.ds(r0, size), :] = lanes
                    else:
                        rss[q][pl.ds(r0, size), :] += lanes
                    s = fold(s)
                    cc = s if cc is None else cc + s
            css[q][:, pl.ds(j * NT, NT)] = cc

        for z in range(2):
            for par in range(2):
                for p in range(2):
                    pltpu.matmul_pop(acc(z, par, p))

        for u in range(n_units):
            last = u == n_units - 1
            t = unit_tile[u][0]
            if not last and unit_tile[u + 1][0] != t:
                d_copy(t + 1).wait()
                if t and t - 1 + RING < len(tiles):
                    d_copy(t - 1 + RING).start()
                for f in before.pop(u):
                    f()
            for k in range(nk):
                if u == 0:
                    x_copy(k).wait()
                    first_copy(k).wait()
                    for z in range(2):
                        xt[pl.ds(z * 256, 256), pl.ds(k * KB, KB)] = xs[k, :, pl.ds(z * 256, 256)].T
                        pltpu.matmul_push_rhs(rhs(0, k), staging_register=k % 2, mxu_index=z)
                    if k % 2 == 0 and k // 2 + 1 < RING:
                        d_copy(k // 2 + 1).start()
                for z in range(2):
                    for p, size in enumerate(PIECES):
                        r0 = z * sum(PIECES) + sum(PIECES[:p])
                        pltpu.matmul_acc_lhs(acc(z, u % 2, p), xt[pl.ds(r0, size), pl.ds(k * KB, KB)],
                                             load_staged_rhs=(k % 2 if p == 0 else None))
                    if k < nk - 1:
                        if u:
                            pltpu.matmul_push_rhs(rhs(u, k + 1), staging_register=(k + 1) % 2, mxu_index=z)
                    elif not last:
                        pltpu.matmul_push_rhs(rhs(u + 1, 0), staging_register=0, mxu_index=z)
                if k == 1 and u:
                    drain(u - 1)
                if k == 2:
                    for f in beside[u]:
                        f()
        drain(n_units - 1)
        assert not any(before.values())

    for c in small:
        c.start()
    pl.run_scoped(run, *[pltpu.ACC(z)((size, NT), F32) for z in range(2) for par in range(2) for size in PIECES])
    for c in bigs[1:] + small:
        c.wait()


def exchange_kernel(
    dims,
    held, ht, dt, wg, wu, wd, rs_g, rs_u, cs_g, cs_u, sw_g, ro, co,
    b2, rel, clip,
    late, a_g, a_u, a_d, b_g, b_u, b_d, r_g, c_g, r_u, c_u, r_d, c_d,
    rs_d, cs_d, su, sw, rsend, rrecv, csend, crecv, pay, got, pay2, got2, r1s, r1r, c1s, c1r, p_s, p_r, p2_s, p2_r,
):
    col = lax.axis_index("col")
    row = lax.axis_index("row")
    row_peer = (row + 1 - 2 * (row % 2), (row + 2) % 4, 3 - row)
    mats = (
        dict(rs=rs_g, cs=cs_g, a=a_g, b=b_g, r=r_g, c=c_g),
        dict(rs=rs_u, cs=cs_u, a=a_u, b=b_u, r=r_u, c=c_u),
        dict(rs=rs_d, cs=cs_d, a=a_d, b=b_d, r=r_d, c=c_d),
    )
    for mat, (m, n) in zip(mats, dims):
        mat["m"], mat["n"] = m, n
        mat["mt"], mat["nt"] = m * 4, n * 2
    (mg, ng), (md, nd) = dims[0], dims[2]
    size = mg * ng // 128

    barrier = pltpu.get_barrier_semaphore()
    plane = [{"row": p, "col": cc} for cc in (col, 1 - col) for p in (row,) + row_peer][1:]
    for dev in plane:
        pl.semaphore_signal(barrier, inc=1, device_id=dev, device_id_type=MESH)

    pay[...] = jnp.zeros_like(pay)
    pay2[...] = jnp.zeros_like(pay2)

    def w_square(q, w):
        m, n = dims[q]
        sw[...] = jnp.zeros_like(sw)

        @pl.loop(0, n // 256)
        def _(c):
            c0 = pl.multiple_of(c * 256, 256)
            a, b = w[:, pl.ds(c0, 128)], w[:, pl.ds(c0 + 128, 128)]
            sw[...] += fold(a * a) + fold(b * b)

        pay[pl.ds(q, 1), :] = jnp.sum(sw[...], axis=0, keepdims=True)

    def first_sends(q):
        mat = mats[q]
        m, n = mat["m"], mat["n"]
        copies = [pltpu.make_async_remote_copy(
            rsend.at[q, :, pl.ds(0, m)], rrecv.at[q, :, pl.ds(0, m)], r1s.at[q], r1r.at[q],
            device_id={"col": 1 - col}, device_id_type=MESH)]
        for d in range(3):
            copies.append(pltpu.make_async_remote_copy(
                csend.at[q, :, pl.ds(0, n)], crecv.at[q, d, :, pl.ds(0, n)], c1s.at[q, d], c1r.at[q, d],
                device_id={"row": row_peer[d]}, device_id_type=MESH))
        return copies

    def first_reduce(q):
        mat = mats[q]
        csend[q, :, pl.ds(0, mat["n"])] = jnp.sum(mat["cs"][...], axis=0, keepdims=True)
        for b in range(mat["m"] // 128):
            t = mat["rs"][pl.ds(b * 128, 128), :].T
            rsend[q, :, pl.ds(b * 128, 128)] = jnp.sum(t, axis=0, keepdims=True)

    def new_stats(q):
        mat = mats[q]
        m, n = mat["m"], mat["n"]
        beta = b2[0, 0]
        rsum = rsend[q, :, pl.ds(0, m)] + rrecv[q, :, pl.ds(0, m)]
        r_new = beta * ro[q, :, pl.ds(0, m)] + (1.0 - beta) * (rsum * (1.0 / mat["nt"]) + EPS_SQ)
        mat["r"][...] = r_new
        csum = (csend[q, :, pl.ds(0, n)] + crecv[q, 0, :, pl.ds(0, n)]) + (
            crecv[q, 1, :, pl.ds(0, n)] + crecv[q, 2, :, pl.ds(0, n)])
        c_new = beta * co[q, :, pl.ds(0, n)] + (1.0 - beta) * (csum * (1.0 / mat["mt"]) + EPS_SQ)
        mat["c"][...] = c_new
        mat["b"][...] = lax.rsqrt(c_new)
        alpha = lax.rsqrt(r_new)
        rp = r_new[:, :128]
        for b in range(m // 128):
            blk = jnp.broadcast_to(alpha[:, b * 128:(b + 1) * 128], (128, 128))
            mat["a"][pl.ds(b * 128, 128), :] = blk.T
            if b:
                rp = rp + r_new[:, b * 128:(b + 1) * 128]
        if q == 2:
            pay2[pl.ds(3, 1), :] = rp
        else:
            pay[pl.ds(3 + q, 1), :] = rp

    def u_square(q):
        mat = mats[q]
        m = mat["m"]
        src, first = (late, 0) if q == 2 else (held, q * size)
        su[...] = jnp.zeros_like(su)

        @pl.loop(0, mat["n"] // 256)
        def _(c):
            total = None
            for half in range(2):
                c0 = pl.multiple_of(c * 256 + half * 128, 128)
                g = src[pl.ds(pl.multiple_of(first + (2 * c + half) * m, 128), m), :]
                t = g * mat["a"][...]
                bb = mat["b"][:, pl.ds(c0, 128)]
                s = fold(t * t) * (bb * bb)
                total = s if total is None else total + s
            su[...] += total

        pay2[pl.ds(q, 1), :] = jnp.sum(su[...], axis=0, keepdims=True)

    rows = md // CHUNKS
    steps = nd // NT * CHUNKS

    def product(i):
        j, c = divmod(i, CHUNKS)
        rr = pl.ds(c * rows, rows)
        g = jnp.dot(ht[rr, :], dt[:, pl.ds(j * NT, NT)], preferred_element_type=F32)
        for half in range(2):
            late[pl.ds((2 * j + half) * md + c * rows, rows), :] = g[:, half * 128:half * 128 + 128]
        s = g * g
        lanes = s[:, :128] + s[:, 128:]
        if j == 0:
            rs_d[rr, :] = lanes
        else:
            rs_d[rr, :] += lanes
        cc = pl.ds(j * NT, NT)
        if c == 0:
            cs_d[:, cc] = fold(s)
        else:
            cs_d[:, cc] += fold(s)

    def plane_sends(src, dst, rows, s_sem, r_sem):
        rr = pl.ds(0, rows)
        return [pltpu.make_async_remote_copy(src.at[rr], dst.at[i, rr], s_sem.at[i], r_sem.at[i], device_id=dev, device_id_type=MESH)
                for i, dev in enumerate(plane)]

    def plane_sum(src, dst, rows):
        a = [src[pl.ds(0, rows), :]] + [dst[i, pl.ds(0, rows), :] for i in range(len(plane))]
        total = ((a[0] + a[1]) + (a[2] + a[3])) + ((a[4] + a[5]) + (a[6] + a[7]))
        return jnp.sum(total, axis=1, keepdims=True)

    early = [c for q in range(2) for c in first_sends(q)]
    for i in range(steps):
        if i == CHUNKS:
            first_reduce(0)
            first_reduce(1)
            pl.semaphore_wait(barrier, len(plane))
            for c in early:
                c.start()
        product(i)
    first_reduce(2)
    sends = first_sends(2)
    for c in sends:
        c.start()
    for c in early:
        c.wait()
    pay[pl.ds(0, 1), :] = jnp.sum(sw_g[...], axis=0, keepdims=True)
    for q in range(2):
        new_stats(q)
    w_square(1, wu)
    w_square(2, wd)
    sums = plane_sends(pay, got, 5, p_s, p_r)
    for c in sums:
        c.start()
    for q in range(2):
        u_square(q)
    for c in sends:
        c.wait()
    new_stats(2)
    u_square(2)
    sums2 = plane_sends(pay2, got2, 4, p2_s, p2_r)
    for c in sums2:
        c.start()
    for c in sums + sums2:
        c.wait()
    norms = plane_sum(pay, got, 5)
    shapes = plane_sum(pay2, got2, 4)
    for q, mat in enumerate(mats):
        count = float(mat["mt"] * mat["nt"])
        r_sum = shapes[3:4] if q == 2 else norms[3 + q:4 + q]
        r_mean = r_sum * (0.5 / mat["mt"])
        u_rms = jnp.sqrt(r_mean * shapes[q:q + 1] / count)
        w_rms = jnp.sqrt(norms[q:q + 1] / count)
        step = rel[0, 0] * jnp.maximum(EPS_SCALE, w_rms)
        k = step * jnp.sqrt(r_mean) / jnp.maximum(1.0, u_rms / clip[0, 0])
        mat["b"][...] = mat["b"][...] * k


def write_kernel(
    dims,
    held, ht, dt, w_g, w_u, w_d, rs_g, rs_u, cs_g, cs_u, sw_g, ro, co,
    late, a_g, a_u, a_d, b_g, b_u, b_d, r_g, c_g, r_u, c_u, r_d, c_d,
    o_g, o_u, o_d, or_g, oc_g, or_u, oc_u, or_d, oc_d,
    wide, tall, o_sem, s_sem,
):
    small = [pltpu.make_async_copy(s.at[0], d, s_sem.at[i]) for i, (s, d) in enumerate(
        [(r_g, or_g), (c_g, oc_g), (r_u, or_u), (c_u, oc_u), (r_d, or_d), (c_d, oc_d)])]
    for c in small:
        c.start()
    slots = 8
    size = dims[0][0] * dims[0][1] // 128
    where = ((held, 0, w_g), (held, 1, w_u), (late, 0, w_d))
    pending = {}
    step = 0
    for q, a, b, o, buf in ((2, a_d, b_d, o_d, tall), (1, a_u, b_u, o_u, wide), (0, a_g, b_g, o_g, wide)):
        rows = buf.shape[1]
        src, k, w = where[q]
        for t in range(dims[q][0] // rows):
            slot = step % slots
            if slot in pending:
                pending.pop(slot).wait()
            rr = pl.ds(t * rows, rows)
            scale = a[rr, :]
            for c in range(dims[q][1] // 128):
                cc = pl.ds(c * 128, 128)
                off = c * dims[q][0] + t * rows
                g = src[pl.ds(k * size + off, rows), :]
                buf[slot, :, cc] = w[rr, cc] - (g * scale) * b[:, cc]
            cp = pltpu.make_async_copy(buf.at[slot], o.at[rr, :], o_sem.at[slot])
            cp.start()
            pending[slot] = cp
            step += 1
    for cp in pending.values():
        cp.wait()
    for c in small:
        c.wait()


def solution(mesh):
    def local_program(x_in, h_act, d_gate, d_up, d_out, w_gate, w_up, w_down, r_gate, c_gate, r_up, c_up, r_down, c_down, beta_two, rel_step, clip_thr):
        (mg, ng), (md, nd) = w_gate.shape, w_down.shape
        tokens = x_in.shape[0]
        nk = tokens // KB
        def hbm(*arrays):
            return tuple(pltpu.with_memory_space_constraint(v, HB) for v in arrays)

        def vmem(*arrays):
            return tuple(pltpu.with_memory_space_constraint(v, VM) for v in arrays)

        one = tuple(v.reshape(1, 1) for v in (beta_two, rel_step, clip_thr))
        dims = [(mg, ng), (mg, ng), (md, nd)]
        mm, nn = max(mg, md), max(ng, nd)
        dma = pltpu.SemaphoreType.DMA

        def call(kernel, outs, args, in_spaces, out_space, scratch, **params):
            return pl.pallas_call(
                functools.partial(kernel, dims),
                out_shape=outs,
                in_specs=[pl.BlockSpec(memory_space=v) for v in in_spaces],
                out_specs=tuple(pl.BlockSpec(memory_space=out_space) for _ in outs),
                scratch_shapes=scratch,
                compiler_params=pltpu.CompilerParams(vmem_limit_bytes=GRANT * 2**20, **params),
                name=kernel.__name__,
            )(*args)

        def vm(shapes):
            return tuple(VM(s, F32) for s in shapes)

        def vm(shapes):
            return tuple(VM(s, F32) for s in shapes)

        size = mg * ng // 128
        lanes = [(m, 128) for m, _ in dims]
        stats = [s for m, n in dims for s in ((1, m), (1, n))]
        first = call(
            dot_kernel,
            vm([(2 * size, 128)]) + (VM((md, tokens), BF16), VM((tokens, nd), BF16))
            + vm(dims + lanes[:2] + [(8, ng), (8, ng), (8, 128), (3, 1, mm), (3, 1, nn)]),
            hbm(x_in, h_act, d_gate, d_up, d_out, w_gate, w_up, w_down, r_gate, c_gate, r_up, c_up, r_down, c_down), [HB] * 14, VM,
            [
                VM((nk, KB, mg), BF16), VM((2, HB_ROWS, md), BF16), VM((mg, tokens), BF16), VM((RING, tokens, WIDE), BF16),
                dma((nk,)), dma((2,)), dma((RING,)), dma((nk,)), dma((4,)), dma((6,)),
            ])
        second = call(
            exchange_kernel,
            vm([(size, 128)] + lanes + [(1, n) for _, n in dims] + stats),
            vmem(*first) + one, [VM] * len(first) + [pltpu.SMEM] * 3, VM,
            [
                VM((md, 128), F32), VM((8, nd), F32), VM((8, 128), F32), VM((8, 128), F32),
                VM((3, 1, mm), F32), VM((3, 1, mm), F32), VM((3, 1, nn), F32), VM((3, 3, 1, nn), F32),
                VM((8, 128), F32), VM((7, 8, 128), F32), VM((8, 128), F32), VM((7, 8, 128), F32),
                dma((3,)), dma((3,)), dma((3, 3)), dma((3, 3)), dma((7,)), dma((7,)), dma((7,)), dma((7,)),
            ], collective_id=0, has_side_effects=True)
        outs = call(
            write_kernel,
            tuple(jax.ShapeDtypeStruct(s, F32) for s in dims + [(k,) for mn in dims for k in mn]),
            vmem(*first, *second), [VM] * (len(first) + len(second)), HB,
            [VM((8, mg // 8, ng), F32), VM((8, md // 8, nd), F32), dma((8,)), dma((6,))])
        return tuple(outs)

    act_spec = P(None, "row")
    cot_spec = P(None, "col")
    w_spec = P("row", "col")
    r_spec = P("row")
    c_spec = P("col")
    s_spec = P()
    return jax.shard_map(local_program, mesh=mesh, in_specs=(act_spec, act_spec, cot_spec, cot_spec, cot_spec, w_spec, w_spec, w_spec, r_spec, c_spec, r_spec, c_spec, r_spec, c_spec, s_spec, s_spec, s_spec), out_specs=(w_spec, w_spec, w_spec, r_spec, c_spec, r_spec, c_spec, r_spec, c_spec), check_vma=False)
```

```python
import functools

import jax
import jax.numpy as jnp
from jax import lax
from jax.experimental import pallas as pl
from jax.experimental.pallas import tpu as pltpu
from jax.sharding import PartitionSpec as P

EPS_SQ = 1e-30
EPS_SCALE = 1e-3
F32 = jnp.float32
BF16 = jnp.bfloat16
MESH = pl.DeviceIdType.MESH
VM = pltpu.VMEM
HB = pltpu.HBM
KB = 256
NT = 256
WIDE = 2 * NT
HB_ROWS = 512
RING = 5
PIECES = (128, 128)
GRANT = 18
CHUNKS = 4


def fold(v):
    slabs = v.reshape(-1, 8, v.shape[1])
    n = slabs.shape[0] // 4 * 4
    s = jnp.sum(slabs[:n].reshape(-1, 4, 8, v.shape[1]), axis=0)
    s = (s[0] + s[1]) + (s[2] + s[3])
    for i in range(n, slabs.shape[0]):
        s = s + slabs[i]
    return s


def dot_kernel(
    dims,
    x, h, dg, du, dd, wgh, rg, cg, ru, cu, rd, cd,
    held, ht, dt, wg, rs_g, rs_u, cs_g, cs_u, sw, ro, co,
    xs, hs, xt, ring, x_sem, h_sem, d_sem, first_sem, big_sem, s_sem,
):
    m, n = dims[0]
    nk = x.shape[0] // KB
    up = n // NT
    cots, rss, css = (dg, du), (rs_g, rs_u), (cs_g, cs_u)
    n_units = 2 * up
    tiles, unit_tile = [], []
    for q in range(2):
        for c0 in range(0, n, WIDE):
            cols = min(WIDE, n - c0)
            for off in range(0, cols, NT):
                unit_tile.append((len(tiles), off))
            tiles.append((q, c0, cols))

    def x_copy(k):
        return pltpu.make_async_copy(x.at[pl.ds(k * KB, KB), :], xs.at[k], x_sem.at[k])

    def first_copy(k):
        return pltpu.make_async_copy(dg.at[pl.ds(k * KB, KB), pl.ds(0, WIDE)], ring.at[0, pl.ds(k * KB, KB), :], first_sem.at[k])

    def d_copy(t):
        q, c0, cols = tiles[t]
        return pltpu.make_async_copy(cots[q].at[:, pl.ds(c0, cols)], ring.at[t % RING, :, pl.ds(0, cols)], d_sem.at[t % RING])

    def h_copy(k):
        return pltpu.make_async_copy(h.at[pl.ds(k * HB_ROWS, HB_ROWS), :], hs.at[k % 2], h_sem.at[k % 2])

    bigs = [pltpu.make_async_copy(a, b, big_sem.at[i]) for i, (a, b) in enumerate(((wgh, wg), (dd, dt)))]
    small = [
        pltpu.make_async_copy(src, dst.at[q, 0, pl.ds(0, src.shape[0])], s_sem.at[i])
        for i, (src, dst, q) in enumerate(
            [(rg, ro, 0), (ru, ro, 1), (rd, ro, 2), (cg, co, 0), (cu, co, 1), (cd, co, 2)])
    ]
    for k in range(nk):
        x_copy(k).start()
        first_copy(k).start()

    blocks = ht.shape[0] // 128

    def h_turn(k, part):
        for c in range(part * (blocks // 2), blocks if part else blocks // 2):
            ht[pl.ds(c * 128, 128), pl.ds(k * HB_ROWS, HB_ROWS)] = hs[k % 2, :, pl.ds(c * 128, 128)].T

    def w_square(c):
        w = wg[:, pl.ds(c * 128, 128)]
        s = fold(w * w)
        if c == 0:
            sw[...] = s
        else:
            sw[...] += s

    before = {u: [] for u in range(n_units)}
    beside = [[] for _ in range(n_units)]
    before[1] += [h_copy(0).start, h_copy(1).start]
    before[3] += [h_copy(0).wait]
    before[5] += [h_copy(1).wait, h_copy(2).start]
    before[7] += [h_copy(2).wait, h_copy(3).start]
    before[9] += [h_copy(3).wait]
    for k in range(4):
        for part in range(2):
            beside[3 + 2 * k + part].append(lambda k=k, part=part: h_turn(k, part))
    before[7].append(bigs[0].start)
    before[10].append(bigs[1].start)
    before[16].append(bigs[0].wait)
    for c in range(n // 128):
        beside[16 + c // 5].append(lambda c=c: w_square(c))

    def run(*accs):
        def acc(z, par, p):
            return accs[(z * 2 + par) * 2 + p]

        def rhs(u, k):
            t, off = unit_tile[u]
            return ring[t % RING, pl.ds(k * KB, KB), pl.ds(off, NT)]

        def drain(u):
            q, j = divmod(u, up)
            cc = None
            for z in range(2):
                for p, size in enumerate(PIECES):
                    r0 = z * sum(PIECES) + sum(PIECES[:p])
                    g = pltpu.matmul_pop(acc(z, u % 2, p))
                    for half in range(2):
                        held[pl.ds((q * (n // 128) + 2 * j + half) * m + r0, size), :] = g[:, half * 128:half * 128 + 128]
                    s = g * g
                    lanes = s[:, :128] + s[:, 128:]
                    if j == 0:
                        rss[q][pl.ds(r0, size), :] = lanes
                    else:
                        rss[q][pl.ds(r0, size), :] += lanes
                    s = fold(s)
                    cc = s if cc is None else cc + s
            css[q][:, pl.ds(j * NT, NT)] = cc

        for z in range(2):
            for par in range(2):
                for p in range(2):
                    pltpu.matmul_pop(acc(z, par, p))

        for u in range(n_units):
            last = u == n_units - 1
            t = unit_tile[u][0]
            if not last and unit_tile[u + 1][0] != t:
                d_copy(t + 1).wait()
                if t and t - 1 + RING < len(tiles):
                    d_copy(t - 1 + RING).start()
                for f in before.pop(u):
                    f()
            for k in range(nk):
                if u == 0:
                    x_copy(k).wait()
                    first_copy(k).wait()
                    for z in range(2):
                        xt[pl.ds(z * 256, 256), pl.ds(k * KB, KB)] = xs[k, :, pl.ds(z * 256, 256)].T
                        pltpu.matmul_push_rhs(rhs(0, k), staging_register=k % 2, mxu_index=z)
                    if k % 2 == 0 and k // 2 + 1 < RING:
                        d_copy(k // 2 + 1).start()
                for z in range(2):
                    for p, size in enumerate(PIECES):
                        r0 = z * sum(PIECES) + sum(PIECES[:p])
                        pltpu.matmul_acc_lhs(acc(z, u % 2, p), xt[pl.ds(r0, size), pl.ds(k * KB, KB)],
                                             load_staged_rhs=(k % 2 if p == 0 else None))
                    if k < nk - 1:
                        if u:
                            pltpu.matmul_push_rhs(rhs(u, k + 1), staging_register=(k + 1) % 2, mxu_index=z)
                    elif not last:
                        pltpu.matmul_push_rhs(rhs(u + 1, 0), staging_register=0, mxu_index=z)
                if k == 1 and u:
                    drain(u - 1)
                if k == 2:
                    for f in beside[u]:
                        f()
        drain(n_units - 1)
        assert not any(before.values())

    for c in small:
        c.start()
    pl.run_scoped(run, *[pltpu.ACC(z)((size, NT), F32) for z in range(2) for par in range(2) for size in PIECES])
    for c in bigs[1:] + small:
        c.wait()


def exchange_kernel(
    dims,
    held, ht, dt, wg, rs_g, rs_u, cs_g, cs_u, sw_g, ro, co,
    wuh, wdh,
    b2, rel, clip,
    late, wu, wd, a_g, a_u, a_d, b_g, b_u, b_d, r_g, c_g, r_u, c_u, r_d, c_d,
    w_sem, rs_d, cs_d, su, sw, rsend, rrecv, csend, crecv, pay, got, pay2, got2, r1s, r1r, c1s, c1r, p_s, p_r, p2_s, p2_r,
):
    col = lax.axis_index("col")
    row = lax.axis_index("row")
    row_peer = (row + 1 - 2 * (row % 2), (row + 2) % 4, 3 - row)
    mats = (
        dict(rs=rs_g, cs=cs_g, a=a_g, b=b_g, r=r_g, c=c_g),
        dict(rs=rs_u, cs=cs_u, a=a_u, b=b_u, r=r_u, c=c_u),
        dict(rs=rs_d, cs=cs_d, a=a_d, b=b_d, r=r_d, c=c_d),
    )
    for mat, (m, n) in zip(mats, dims):
        mat["m"], mat["n"] = m, n
        mat["mt"], mat["nt"] = m * 4, n * 2
    (mg, ng), (md, nd) = dims[0], dims[2]
    size = mg * ng // 128

    barrier = pltpu.get_barrier_semaphore()
    plane = [{"row": p, "col": cc} for cc in (col, 1 - col) for p in (row,) + row_peer][1:]
    for dev in plane:
        pl.semaphore_signal(barrier, inc=1, device_id=dev, device_id_type=MESH)

    loads = [pltpu.make_async_copy(a, b, w_sem.at[i]) for i, (a, b) in enumerate(((wuh, wu), (wdh, wd)))]
    for c in loads:
        c.start()
    pay[...] = jnp.zeros_like(pay)
    pay2[...] = jnp.zeros_like(pay2)

    def w_square(q, w):
        m, n = dims[q]
        sw[...] = jnp.zeros_like(sw)

        @pl.loop(0, n // 256)
        def _(c):
            c0 = pl.multiple_of(c * 256, 256)
            a, b = w[:, pl.ds(c0, 128)], w[:, pl.ds(c0 + 128, 128)]
            sw[...] += fold(a * a) + fold(b * b)

        pay[pl.ds(q, 1), :] = jnp.sum(sw[...], axis=0, keepdims=True)

    def first_sends(q):
        mat = mats[q]
        m, n = mat["m"], mat["n"]
        copies = [pltpu.make_async_remote_copy(
            rsend.at[q, :, pl.ds(0, m)], rrecv.at[q, :, pl.ds(0, m)], r1s.at[q], r1r.at[q],
            device_id={"col": 1 - col}, device_id_type=MESH)]
        for d in range(3):
            copies.append(pltpu.make_async_remote_copy(
                csend.at[q, :, pl.ds(0, n)], crecv.at[q, d, :, pl.ds(0, n)], c1s.at[q, d], c1r.at[q, d],
                device_id={"row": row_peer[d]}, device_id_type=MESH))
        return copies

    def first_reduce(q):
        mat = mats[q]
        csend[q, :, pl.ds(0, mat["n"])] = jnp.sum(mat["cs"][...], axis=0, keepdims=True)
        for b in range(mat["m"] // 128):
            t = mat["rs"][pl.ds(b * 128, 128), :].T
            rsend[q, :, pl.ds(b * 128, 128)] = jnp.sum(t, axis=0, keepdims=True)

    def new_stats(q):
        mat = mats[q]
        m, n = mat["m"], mat["n"]
        beta = b2[0, 0]
        rsum = rsend[q, :, pl.ds(0, m)] + rrecv[q, :, pl.ds(0, m)]
        r_new = beta * ro[q, :, pl.ds(0, m)] + (1.0 - beta) * (rsum * (1.0 / mat["nt"]) + EPS_SQ)
        mat["r"][...] = r_new
        csum = (csend[q, :, pl.ds(0, n)] + crecv[q, 0, :, pl.ds(0, n)]) + (
            crecv[q, 1, :, pl.ds(0, n)] + crecv[q, 2, :, pl.ds(0, n)])
        c_new = beta * co[q, :, pl.ds(0, n)] + (1.0 - beta) * (csum * (1.0 / mat["mt"]) + EPS_SQ)
        mat["c"][...] = c_new
        mat["b"][...] = lax.rsqrt(c_new)
        alpha = lax.rsqrt(r_new)
        rp = r_new[:, :128]
        for b in range(m // 128):
            blk = jnp.broadcast_to(alpha[:, b * 128:(b + 1) * 128], (128, 128))
            mat["a"][pl.ds(b * 128, 128), :] = blk.T
            if b:
                rp = rp + r_new[:, b * 128:(b + 1) * 128]
        if q == 2:
            pay2[pl.ds(3, 1), :] = rp
        else:
            pay[pl.ds(3 + q, 1), :] = rp

    def u_square(q):
        mat = mats[q]
        m = mat["m"]
        src, first = (late, 0) if q == 2 else (held, q * size)
        su[...] = jnp.zeros_like(su)

        @pl.loop(0, mat["n"] // 256)
        def _(c):
            total = None
            for half in range(2):
                c0 = pl.multiple_of(c * 256 + half * 128, 128)
                g = src[pl.ds(pl.multiple_of(first + (2 * c + half) * m, 128), m), :]
                t = g * mat["a"][...]
                bb = mat["b"][:, pl.ds(c0, 128)]
                s = fold(t * t) * (bb * bb)
                total = s if total is None else total + s
            su[...] += total

        pay2[pl.ds(q, 1), :] = jnp.sum(su[...], axis=0, keepdims=True)

    rows = md // CHUNKS
    steps = nd // NT * CHUNKS

    def product(i):
        j, c = divmod(i, CHUNKS)
        rr = pl.ds(c * rows, rows)
        g = jnp.dot(ht[rr, :], dt[:, pl.ds(j * NT, NT)], preferred_element_type=F32)
        for half in range(2):
            late[pl.ds((2 * j + half) * md + c * rows, rows), :] = g[:, half * 128:half * 128 + 128]
        s = g * g
        lanes = s[:, :128] + s[:, 128:]
        if j == 0:
            rs_d[rr, :] = lanes
        else:
            rs_d[rr, :] += lanes
        cc = pl.ds(j * NT, NT)
        if c == 0:
            cs_d[:, cc] = fold(s)
        else:
            cs_d[:, cc] += fold(s)

    def plane_sends(src, dst, rows, s_sem, r_sem):
        rr = pl.ds(0, rows)
        return [pltpu.make_async_remote_copy(src.at[rr], dst.at[i, rr], s_sem.at[i], r_sem.at[i], device_id=dev, device_id_type=MESH)
                for i, dev in enumerate(plane)]

    def plane_sum(src, dst, rows):
        a = [src[pl.ds(0, rows), :]] + [dst[i, pl.ds(0, rows), :] for i in range(len(plane))]
        total = ((a[0] + a[1]) + (a[2] + a[3])) + ((a[4] + a[5]) + (a[6] + a[7]))
        return jnp.sum(total, axis=1, keepdims=True)

    early = [c for q in range(2) for c in first_sends(q)]
    for i in range(steps):
        if i == CHUNKS:
            first_reduce(0)
            first_reduce(1)
            pl.semaphore_wait(barrier, len(plane))
            for c in early:
                c.start()
        product(i)
    first_reduce(2)
    sends = first_sends(2)
    for c in sends:
        c.start()
    for c in early:
        c.wait()
    pay[pl.ds(0, 1), :] = jnp.sum(sw_g[...], axis=0, keepdims=True)
    for q in range(2):
        new_stats(q)
    for c in loads:
        c.wait()
    w_square(1, wu)
    w_square(2, wd)
    sums = plane_sends(pay, got, 5, p_s, p_r)
    for c in sums:
        c.start()
    for q in range(2):
        u_square(q)
    for c in sends:
        c.wait()
    new_stats(2)
    u_square(2)
    sums2 = plane_sends(pay2, got2, 4, p2_s, p2_r)
    for c in sums2:
        c.start()
    for c in sums + sums2:
        c.wait()
    norms = plane_sum(pay, got, 5)
    shapes = plane_sum(pay2, got2, 4)
    for q, mat in enumerate(mats):
        count = float(mat["mt"] * mat["nt"])
        r_sum = shapes[3:4] if q == 2 else norms[3 + q:4 + q]
        r_mean = r_sum * (0.5 / mat["mt"])
        u_rms = jnp.sqrt(r_mean * shapes[q:q + 1] / count)
        w_rms = jnp.sqrt(norms[q:q + 1] / count)
        step = rel[0, 0] * jnp.maximum(EPS_SCALE, w_rms)
        k = step * jnp.sqrt(r_mean) / jnp.maximum(1.0, u_rms / clip[0, 0])
        mat["b"][...] = mat["b"][...] * k


def write_kernel(
    dims,
    held, ht, dt, w_g, rs_g, rs_u, cs_g, cs_u, sw_g, ro, co,
    late, w_u, w_d, a_g, a_u, a_d, b_g, b_u, b_d, r_g, c_g, r_u, c_u, r_d, c_d,
    o_g, o_u, o_d, or_g, oc_g, or_u, oc_u, or_d, oc_d,
    wide, tall, o_sem, s_sem,
):
    small = [pltpu.make_async_copy(s.at[0], d, s_sem.at[i]) for i, (s, d) in enumerate(
        [(r_g, or_g), (c_g, oc_g), (r_u, or_u), (c_u, oc_u), (r_d, or_d), (c_d, oc_d)])]
    for c in small:
        c.start()
    slots = 8
    size = dims[0][0] * dims[0][1] // 128
    where = ((held, 0, w_g), (held, 1, w_u), (late, 0, w_d))
    pending = {}
    step = 0
    for q, a, b, o, buf in ((2, a_d, b_d, o_d, tall), (1, a_u, b_u, o_u, wide), (0, a_g, b_g, o_g, wide)):
        rows = buf.shape[1]
        src, k, w = where[q]
        for t in range(dims[q][0] // rows):
            slot = step % slots
            if slot in pending:
                pending.pop(slot).wait()
            rr = pl.ds(t * rows, rows)
            scale = a[rr, :]
            for c in range(dims[q][1] // 128):
                cc = pl.ds(c * 128, 128)
                off = c * dims[q][0] + t * rows
                g = src[pl.ds(k * size + off, rows), :]
                buf[slot, :, cc] = w[rr, cc] - (g * scale) * b[:, cc]
            cp = pltpu.make_async_copy(buf.at[slot], o.at[rr, :], o_sem.at[slot])
            cp.start()
            pending[slot] = cp
            step += 1
    for cp in pending.values():
        cp.wait()
    for c in small:
        c.wait()


def solution(mesh):
    def local_program(x_in, h_act, d_gate, d_up, d_out, w_gate, w_up, w_down, r_gate, c_gate, r_up, c_up, r_down, c_down, beta_two, rel_step, clip_thr):
        (mg, ng), (md, nd) = w_gate.shape, w_down.shape
        tokens = x_in.shape[0]
        nk = tokens // KB
        def hbm(*arrays):
            return tuple(pltpu.with_memory_space_constraint(v, HB) for v in arrays)

        def vmem(*arrays):
            return tuple(pltpu.with_memory_space_constraint(v, VM) for v in arrays)

        one = tuple(v.reshape(1, 1) for v in (beta_two, rel_step, clip_thr))
        dims = [(mg, ng), (mg, ng), (md, nd)]
        mm, nn = max(mg, md), max(ng, nd)
        dma = pltpu.SemaphoreType.DMA

        def call(kernel, outs, args, in_spaces, out_space, scratch, **params):
            return pl.pallas_call(
                functools.partial(kernel, dims),
                out_shape=outs,
                in_specs=[pl.BlockSpec(memory_space=v) for v in in_spaces],
                out_specs=tuple(pl.BlockSpec(memory_space=out_space) for _ in outs),
                scratch_shapes=scratch,
                compiler_params=pltpu.CompilerParams(vmem_limit_bytes=GRANT * 2**20, **params),
                name=kernel.__name__,
            )(*args)

        def vm(shapes):
            return tuple(VM(s, F32) for s in shapes)

        def vm(shapes):
            return tuple(VM(s, F32) for s in shapes)

        size = mg * ng // 128
        lanes = [(m, 128) for m, _ in dims]
        stats = [s for m, n in dims for s in ((1, m), (1, n))]
        first = call(
            dot_kernel,
            vm([(2 * size, 128)]) + (VM((md, tokens), BF16), VM((tokens, nd), BF16))
            + vm(dims[:1] + lanes[:2] + [(8, ng), (8, ng), (8, 128), (3, 1, mm), (3, 1, nn)]),
            hbm(x_in, h_act, d_gate, d_up, d_out, w_gate, r_gate, c_gate, r_up, c_up, r_down, c_down), [HB] * 12, VM,
            [
                VM((nk, KB, mg), BF16), VM((2, HB_ROWS, md), BF16), VM((mg, tokens), BF16), VM((RING, tokens, WIDE), BF16),
                dma((nk,)), dma((2,)), dma((RING,)), dma((nk,)), dma((2,)), dma((6,)),
            ])
        second = call(
            exchange_kernel,
            vm([(size, 128)] + dims[1:] + lanes + [(1, n) for _, n in dims] + stats),
            vmem(*first) + hbm(w_up, w_down) + one, [VM] * len(first) + [HB] * 2 + [pltpu.SMEM] * 3, VM,
            [
                dma((2,)),
                VM((md, 128), F32), VM((8, nd), F32), VM((8, 128), F32), VM((8, 128), F32),
                VM((3, 1, mm), F32), VM((3, 1, mm), F32), VM((3, 1, nn), F32), VM((3, 3, 1, nn), F32),
                VM((8, 128), F32), VM((7, 8, 128), F32), VM((8, 128), F32), VM((7, 8, 128), F32),
                dma((3,)), dma((3,)), dma((3, 3)), dma((3, 3)), dma((7,)), dma((7,)), dma((7,)), dma((7,)),
            ], collective_id=0, has_side_effects=True)
        outs = call(
            write_kernel,
            tuple(jax.ShapeDtypeStruct(s, F32) for s in dims + [(k,) for mn in dims for k in mn]),
            vmem(*first, *second), [VM] * (len(first) + len(second)), HB,
            [VM((8, mg // 8, ng), F32), VM((8, md // 8, nd), F32), dma((8,)), dma((6,))])
        return tuple(outs)

    act_spec = P(None, "row")
    cot_spec = P(None, "col")
    w_spec = P("row", "col")
    r_spec = P("row")
    c_spec = P("col")
    s_spec = P()
    return jax.shard_map(local_program, mesh=mesh, in_specs=(act_spec, act_spec, cot_spec, cot_spec, cot_spec, w_spec, w_spec, w_spec, r_spec, c_spec, r_spec, c_spec, r_spec, c_spec, s_spec, s_spec, s_spec), out_specs=(w_spec, w_spec, w_spec, r_spec, c_spec, r_spec, c_spec, r_spec, c_spec), check_vma=False)
```

```python
import functools

import jax
import jax.numpy as jnp
from jax import lax
from jax.experimental import pallas as pl
from jax.experimental.pallas import tpu as pltpu
from jax.sharding import PartitionSpec as P

EPS_SQ = 1e-30
EPS_SCALE = 1e-3
F32 = jnp.float32
BF16 = jnp.bfloat16
MESH = pl.DeviceIdType.MESH
VM = pltpu.VMEM
HB = pltpu.HBM
KB = 256
NT = 256
WIDE = 2 * NT
HB_ROWS = 512
RING = 5
PIECES = (128, 128)
GRANT = 18
CHUNKS = 4


def fold(v):
    slabs = v.reshape(-1, 8, v.shape[1])
    n = slabs.shape[0] // 4 * 4
    s = jnp.sum(slabs[:n].reshape(-1, 4, 8, v.shape[1]), axis=0)
    s = (s[0] + s[1]) + (s[2] + s[3])
    for i in range(n, slabs.shape[0]):
        s = s + slabs[i]
    return s


def dot_kernel(
    dims,
    x, h, dg, du, dd, wgh, rg, cg, ru, cu, rd, cd,
    held, ht, dt, wg, rs_g, rs_u, cs_g, cs_u, sw, ro, co,
    xs, hs, xt, ring, x_sem, h_sem, d_sem, first_sem, big_sem, s_sem,
):
    m, n = dims[0]
    nk = x.shape[0] // KB
    up = n // NT
    cots, rss, css = (dg, du), (rs_g, rs_u), (cs_g, cs_u)
    n_units = 2 * up
    tiles, unit_tile = [], []
    for q in range(2):
        odd = n % WIDE
        for c0, cols in ([(0, odd)] if odd and not q else []) + [(c, min(WIDE, n - c)) for c in range(0 if q else odd, n, WIDE)]:
            for off in range(0, cols, NT):
                unit_tile.append((len(tiles), off))
            tiles.append((q, c0, cols))

    wide0 = tiles[0][2]

    def x_copy(k):
        return pltpu.make_async_copy(x.at[pl.ds(k * KB, KB), :], xs.at[k], x_sem.at[k])

    def first_copy(k):
        return pltpu.make_async_copy(dg.at[pl.ds(k * KB, KB), pl.ds(0, wide0)], ring.at[0, pl.ds(k * KB, KB), pl.ds(0, wide0)], first_sem.at[k])

    def d_copy(t):
        q, c0, cols = tiles[t]
        return pltpu.make_async_copy(cots[q].at[:, pl.ds(c0, cols)], ring.at[t % RING, :, pl.ds(0, cols)], d_sem.at[t % RING])

    def h_copy(k):
        return pltpu.make_async_copy(h.at[pl.ds(k * HB_ROWS, HB_ROWS), :], hs.at[k % 2], h_sem.at[k % 2])

    bigs = [pltpu.make_async_copy(a, b, big_sem.at[i]) for i, (a, b) in enumerate(((wgh, wg), (dd, dt)))]
    small = [
        pltpu.make_async_copy(src, dst.at[q, 0, pl.ds(0, src.shape[0])], s_sem.at[i])
        for i, (src, dst, q) in enumerate(
            [(rg, ro, 0), (ru, ro, 1), (rd, ro, 2), (cg, co, 0), (cu, co, 1), (cd, co, 2)])
    ]
    for k in range(nk):
        x_copy(k).start()
        first_copy(k).start()

    blocks = ht.shape[0] // 128

    def h_turn(k, part):
        for c in range(part * (blocks // 2), blocks if part else blocks // 2):
            ht[pl.ds(c * 128, 128), pl.ds(k * HB_ROWS, HB_ROWS)] = hs[k % 2, :, pl.ds(c * 128, 128)].T

    def w_square(c):
        w = wg[:, pl.ds(c * 128, 128)]
        s = fold(w * w)
        if c == 0:
            sw[...] = s
        else:
            sw[...] += s

    before = {u: [] for u in range(n_units)}
    beside = [[] for _ in range(n_units)]
    heads = [u for u in range(n_units - 1) if unit_tile[u][0] != unit_tile[u + 1][0]]

    def head(u):
        return max(v for v in heads if v <= u)

    wait_h = (head(7), head(9), head(15), head(17))
    for u, k in zip((head(2), head(2), wait_h[1], head(wait_h[1] + 3)), range(4)):
        before[u].append(h_copy(k).start)
    for u, k in zip(wait_h, range(4)):
        before[u].append(h_copy(k).wait)
        for part in range(2):
            beside[u + part].append(lambda k=k, part=part: h_turn(k, part))
    before[head(11)].append(bigs[0].start)
    before[head(14)].append(bigs[1].start)
    w0 = head(19)
    before[w0].append(bigs[0].wait)
    span = n_units - w0
    for c in range(n // 128):
        beside[w0 + c * span // (n // 128)].append(lambda c=c: w_square(c))

    def run(*accs):
        def acc(z, par, p):
            return accs[(z * 2 + par) * 2 + p]

        def rhs(u, k):
            t, off = unit_tile[u]
            return ring[t % RING, pl.ds(k * KB, KB), pl.ds(off, NT)]

        def drain(u):
            q, j = divmod(u, up)
            cc = None
            for z in range(2):
                for p, size in enumerate(PIECES):
                    r0 = z * sum(PIECES) + sum(PIECES[:p])
                    g = pltpu.matmul_pop(acc(z, u % 2, p))
                    for half in range(2):
                        held[pl.ds((q * (n // 128) + 2 * j + half) * m + r0, size), :] = g[:, half * 128:half * 128 + 128]
                    s = g * g
                    lanes = s[:, :128] + s[:, 128:]
                    if j == 0:
                        rss[q][pl.ds(r0, size), :] = lanes
                    else:
                        rss[q][pl.ds(r0, size), :] += lanes
                    s = fold(s)
                    cc = s if cc is None else cc + s
            css[q][:, pl.ds(j * NT, NT)] = cc

        for z in range(2):
            for par in range(2):
                for p in range(2):
                    pltpu.matmul_pop(acc(z, par, p))

        for u in range(n_units):
            last = u == n_units - 1
            t = unit_tile[u][0]
            if not last and unit_tile[u + 1][0] != t:
                if u:
                    d_copy(t + 1).wait()
                if t and t - 1 + RING < len(tiles):
                    d_copy(t - 1 + RING).start()
                for f in before.pop(u):
                    f()
            for k in range(nk):
                if u == 0:
                    x_copy(k).wait()
                    first_copy(k).wait()
                    for z in range(2):
                        xt[pl.ds(z * 256, 256), pl.ds(k * KB, KB)] = xs[k, :, pl.ds(z * 256, 256)].T
                        pltpu.matmul_push_rhs(rhs(0, k), staging_register=k % 2, mxu_index=z)
                    if k % 2 and k // 2 + 1 < RING:
                        d_copy(k // 2 + 1).start()
                    if k == nk - 1 and unit_tile[1][0] == 1:
                        d_copy(1).wait()
                for z in range(2):
                    for p, size in enumerate(PIECES):
                        r0 = z * sum(PIECES) + sum(PIECES[:p])
                        pltpu.matmul_acc_lhs(acc(z, u % 2, p), xt[pl.ds(r0, size), pl.ds(k * KB, KB)],
                                             load_staged_rhs=(k % 2 if p == 0 else None))
                    if k < nk - 1:
                        if u:
                            pltpu.matmul_push_rhs(rhs(u, k + 1), staging_register=(k + 1) % 2, mxu_index=z)
                    elif not last:
                        pltpu.matmul_push_rhs(rhs(u + 1, 0), staging_register=0, mxu_index=z)
                if k == 1 and u:
                    drain(u - 1)
                if k == 2:
                    for f in beside[u]:
                        f()
        drain(n_units - 1)
        assert not any(before.values())

    for c in small:
        c.start()
    pl.run_scoped(run, *[pltpu.ACC(z)((size, NT), F32) for z in range(2) for par in range(2) for size in PIECES])
    for c in bigs[1:] + small:
        c.wait()


def exchange_kernel(
    dims,
    held, ht, dt, wg, rs_g, rs_u, cs_g, cs_u, sw_g, ro, co,
    wuh, wdh,
    b2, rel, clip,
    late, wu, wd, a_g, a_u, a_d, b_g, b_u, b_d, r_g, c_g, r_u, c_u, r_d, c_d,
    w_sem, rs_d, cs_d, sw, rsend, rrecv, csend, crecv, pay, got, pay2, got2, r1s, r1r, c1s, c1r, p_s, p_r, p2_s, p2_r,
):
    col = lax.axis_index("col")
    row = lax.axis_index("row")
    row_peer = (row + 1 - 2 * (row % 2), (row + 2) % 4, 3 - row)
    mats = (
        dict(rs=rs_g, cs=cs_g, a=a_g, b=b_g, r=r_g, c=c_g),
        dict(rs=rs_u, cs=cs_u, a=a_u, b=b_u, r=r_u, c=c_u),
        dict(rs=rs_d, cs=cs_d, a=a_d, b=b_d, r=r_d, c=c_d),
    )
    for mat, (m, n) in zip(mats, dims):
        mat["m"], mat["n"] = m, n
        mat["mt"], mat["nt"] = m * 4, n * 2
    (mg, ng), (md, nd) = dims[0], dims[2]
    size = mg * ng // 128

    barrier = pltpu.get_barrier_semaphore()
    plane = [{"row": p, "col": cc} for cc in (col, 1 - col) for p in (row,) + row_peer][1:]
    for dev in plane:
        pl.semaphore_signal(barrier, inc=1, device_id=dev, device_id_type=MESH)

    loads = [pltpu.make_async_copy(a, b, w_sem.at[i]) for i, (a, b) in enumerate(((wuh, wu), (wdh, wd)))]
    for c in loads:
        c.start()
    pay[...] = jnp.zeros_like(pay)
    pay2[...] = jnp.zeros_like(pay2)

    def w_square(q, w):
        m, n = dims[q]
        sw[...] = jnp.zeros_like(sw)

        @pl.loop(0, n // 256)
        def _(c):
            c0 = pl.multiple_of(c * 256, 256)
            a, b = w[:, pl.ds(c0, 128)], w[:, pl.ds(c0 + 128, 128)]
            sw[...] += fold(a * a) + fold(b * b)

        pay[pl.ds(q, 1), :] = jnp.sum(sw[...], axis=0, keepdims=True)

    def first_sends(q):
        mat = mats[q]
        m, n = mat["m"], mat["n"]
        copies = [pltpu.make_async_remote_copy(
            rsend.at[q, :, pl.ds(0, m)], rrecv.at[q, :, pl.ds(0, m)], r1s.at[q], r1r.at[q],
            device_id={"col": 1 - col}, device_id_type=MESH)]
        for d in range(3):
            copies.append(pltpu.make_async_remote_copy(
                csend.at[q, :, pl.ds(0, n)], crecv.at[q, d, :, pl.ds(0, n)], c1s.at[q, d], c1r.at[q, d],
                device_id={"row": row_peer[d]}, device_id_type=MESH))
        return copies

    def first_reduce(q):
        mat = mats[q]
        csend[q, :, pl.ds(0, mat["n"])] = jnp.sum(mat["cs"][...], axis=0, keepdims=True)
        for b in range(mat["m"] // 128):
            t = mat["rs"][pl.ds(b * 128, 128), :].T
            rsend[q, :, pl.ds(b * 128, 128)] = jnp.sum(t, axis=0, keepdims=True)

    def new_stats(q):
        mat = mats[q]
        m, n = mat["m"], mat["n"]
        beta = b2[0, 0]
        rsum = rsend[q, :, pl.ds(0, m)] + rrecv[q, :, pl.ds(0, m)]
        r_new = beta * ro[q, :, pl.ds(0, m)] + (1.0 - beta) * (rsum * (1.0 / mat["nt"]) + EPS_SQ)
        mat["r"][...] = r_new
        csum = (csend[q, :, pl.ds(0, n)] + crecv[q, 0, :, pl.ds(0, n)]) + (
            crecv[q, 1, :, pl.ds(0, n)] + crecv[q, 2, :, pl.ds(0, n)])
        c_new = beta * co[q, :, pl.ds(0, n)] + (1.0 - beta) * (csum * (1.0 / mat["mt"]) + EPS_SQ)
        mat["c"][...] = c_new
        mat["b"][...] = lax.rsqrt(c_new)
        alpha = lax.rsqrt(r_new)
        rp = r_new[:, :128]
        for b in range(m // 128):
            blk = jnp.broadcast_to(alpha[:, b * 128:(b + 1) * 128], (128, 128))
            mat["a"][pl.ds(b * 128, 128), :] = blk.T
            if b:
                rp = rp + r_new[:, b * 128:(b + 1) * 128]
        if q == 2:
            pay2[pl.ds(3, 1), :] = rp
        else:
            pay[pl.ds(3 + q, 1), :] = rp

    def u_square(q, rows):
        mat = mats[q]
        m, n = mat["m"], mat["n"]
        src, first = (late, 0) if q == 2 else (held, q * size)
        blocks = n // 128

        def chunk(r, sums):
            r0 = pl.multiple_of(r * rows, 8)
            a = mat["a"][pl.ds(r0, rows), :]
            new = []
            for c in range(blocks):
                t = src[pl.ds(pl.multiple_of(first + c * m + r0, 8), rows), :] * a
                new.append(sums[c] + fold(t * t))
            return tuple(new)

        sums = lax.fori_loop(0, m // rows, chunk, (jnp.zeros((8, 128), F32),) * blocks)
        total = None
        for c in range(blocks):
            bb = mat["b"][:, c * 128:(c + 1) * 128]
            s = sums[c] * (bb * bb)
            total = s if total is None else total + s
        pay2[pl.ds(q, 1), :] = jnp.sum(total, axis=0, keepdims=True)

    rows = md // CHUNKS
    steps = nd // NT * CHUNKS

    def product(i):
        j, c = divmod(i, CHUNKS)
        rr = pl.ds(c * rows, rows)
        g = jnp.dot(ht[rr, :], dt[:, pl.ds(j * NT, NT)], preferred_element_type=F32)
        for half in range(2):
            late[pl.ds((2 * j + half) * md + c * rows, rows), :] = g[:, half * 128:half * 128 + 128]
        s = g * g
        lanes = s[:, :128] + s[:, 128:]
        if j == 0:
            rs_d[rr, :] = lanes
        else:
            rs_d[rr, :] += lanes
        cc = pl.ds(j * NT, NT)
        if c == 0:
            cs_d[:, cc] = fold(s)
        else:
            cs_d[:, cc] += fold(s)

    def plane_sends(src, dst, rows, s_sem, r_sem):
        rr = pl.ds(0, rows)
        return [pltpu.make_async_remote_copy(src.at[rr], dst.at[i, rr], s_sem.at[i], r_sem.at[i], device_id=dev, device_id_type=MESH)
                for i, dev in enumerate(plane)]

    def plane_sum(src, dst, rows):
        a = [src[pl.ds(0, rows), :]] + [dst[i, pl.ds(0, rows), :] for i in range(len(plane))]
        total = ((a[0] + a[1]) + (a[2] + a[3])) + ((a[4] + a[5]) + (a[6] + a[7]))
        return jnp.sum(total, axis=1, keepdims=True)

    early = [c for q in range(2) for c in first_sends(q)]
    for i in range(steps):
        if i == CHUNKS:
            first_reduce(0)
            first_reduce(1)
            pl.semaphore_wait(barrier, len(plane))
            for c in early:
                c.start()
        product(i)
    first_reduce(2)
    sends = first_sends(2)
    for c in sends:
        c.start()
    for c in early:
        c.wait()
    pay[pl.ds(0, 1), :] = jnp.sum(sw_g[...], axis=0, keepdims=True)
    for q in range(2):
        new_stats(q)
    for c in loads:
        c.wait()
    w_square(1, wu)
    w_square(2, wd)
    sums = plane_sends(pay, got, 5, p_s, p_r)
    for c in sums:
        c.start()
    for q in range(2):
        u_square(q, 64)
    for c in sends:
        c.wait()
    new_stats(2)
    u_square(2, md // 4)
    sums2 = plane_sends(pay2, got2, 4, p2_s, p2_r)
    for c in sums2:
        c.start()
    for c in sums + sums2:
        c.wait()
    norms = plane_sum(pay, got, 5)
    shapes = plane_sum(pay2, got2, 4)
    for q, mat in enumerate(mats):
        count = float(mat["mt"] * mat["nt"])
        r_sum = shapes[3:4] if q == 2 else norms[3 + q:4 + q]
        r_mean = r_sum * (0.5 / mat["mt"])
        u_rms = jnp.sqrt(r_mean * shapes[q:q + 1] / count)
        w_rms = jnp.sqrt(norms[q:q + 1] / count)
        step = rel[0, 0] * jnp.maximum(EPS_SCALE, w_rms)
        k = step * jnp.sqrt(r_mean) / jnp.maximum(1.0, u_rms / clip[0, 0])
        mat["b"][...] = mat["b"][...] * k


def write_kernel(
    dims,
    held, ht, dt, w_g, rs_g, rs_u, cs_g, cs_u, sw_g, ro, co,
    late, w_u, w_d, a_g, a_u, a_d, b_g, b_u, b_d, r_g, c_g, r_u, c_u, r_d, c_d,
    o_g, o_u, o_d, or_g, oc_g, or_u, oc_u, or_d, oc_d,
    wide, tall, o_sem, s_sem,
):
    small = [pltpu.make_async_copy(s.at[0], d, s_sem.at[i]) for i, (s, d) in enumerate(
        [(r_g, or_g), (c_g, oc_g), (r_u, or_u), (c_u, oc_u), (r_d, or_d), (c_d, oc_d)])]
    for c in small:
        c.start()
    slots = 8
    size = dims[0][0] * dims[0][1] // 128
    where = ((held, 0, w_g), (held, 1, w_u), (late, 0, w_d))
    pending = {}
    step = 0
    for q, a, b, o, buf in ((2, a_d, b_d, o_d, tall), (1, a_u, b_u, o_u, wide), (0, a_g, b_g, o_g, wide)):
        rows = buf.shape[1]
        src, k, w = where[q]
        for t in range(dims[q][0] // rows):
            slot = step % slots
            if slot in pending:
                pending.pop(slot).wait()
            rr = pl.ds(t * rows, rows)
            scale = a[rr, :]
            for c in range(dims[q][1] // 128):
                cc = pl.ds(c * 128, 128)
                off = c * dims[q][0] + t * rows
                g = src[pl.ds(k * size + off, rows), :]
                buf[slot, :, cc] = w[rr, cc] - (g * scale) * b[:, cc]
            cp = pltpu.make_async_copy(buf.at[slot], o.at[rr, :], o_sem.at[slot])
            cp.start()
            pending[slot] = cp
            step += 1
    for cp in pending.values():
        cp.wait()
    for c in small:
        c.wait()


def solution(mesh):
    def local_program(x_in, h_act, d_gate, d_up, d_out, w_gate, w_up, w_down, r_gate, c_gate, r_up, c_up, r_down, c_down, beta_two, rel_step, clip_thr):
        (mg, ng), (md, nd) = w_gate.shape, w_down.shape
        tokens = x_in.shape[0]
        nk = tokens // KB
        def hbm(*arrays):
            return tuple(pltpu.with_memory_space_constraint(v, HB) for v in arrays)

        def vmem(*arrays):
            return tuple(pltpu.with_memory_space_constraint(v, VM) for v in arrays)

        one = tuple(lax.ppermute(v.reshape(1, 1), 'data', [(i, (i + 1) % 4) for i in range(4)]) for v in (beta_two, rel_step, clip_thr))
        dims = [(mg, ng), (mg, ng), (md, nd)]
        mm, nn = max(mg, md), max(ng, nd)
        dma = pltpu.SemaphoreType.DMA

        def call(kernel, outs, args, in_spaces, out_space, scratch, **params):
            return pl.pallas_call(
                functools.partial(kernel, dims),
                out_shape=outs,
                in_specs=[pl.BlockSpec(memory_space=v) for v in in_spaces],
                out_specs=tuple(pl.BlockSpec(memory_space=out_space) for _ in outs),
                scratch_shapes=scratch,
                compiler_params=pltpu.CompilerParams(vmem_limit_bytes=GRANT * 2**20, **params),
                name=kernel.__name__,
            )(*args)

        def vm(shapes):
            return tuple(VM(s, F32) for s in shapes)

        def vm(shapes):
            return tuple(VM(s, F32) for s in shapes)

        size = mg * ng // 128
        lanes = [(m, 128) for m, _ in dims]
        stats = [s for m, n in dims for s in ((1, m), (1, n))]
        first = call(
            dot_kernel,
            vm([(2 * size, 128)]) + (VM((md, tokens), BF16), VM((tokens, nd), BF16))
            + vm(dims[:1] + lanes[:2] + [(8, ng), (8, ng), (8, 128), (3, 1, mm), (3, 1, nn)]),
            hbm(x_in, h_act, d_gate, d_up, d_out, w_gate, r_gate, c_gate, r_up, c_up, r_down, c_down), [HB] * 12, VM,
            [
                VM((nk, KB, mg), BF16), VM((2, HB_ROWS, md), BF16), VM((mg, tokens), BF16), VM((RING, tokens, WIDE), BF16),
                dma((nk,)), dma((2,)), dma((RING,)), dma((nk,)), dma((2,)), dma((6,)),
            ])
        second = call(
            exchange_kernel,
            vm([(size, 128)] + dims[1:] + lanes + [(1, n) for _, n in dims] + stats),
            vmem(*first) + hbm(w_up, w_down) + one, [VM] * len(first) + [HB] * 2 + [pltpu.SMEM] * 3, VM,
            [
                dma((2,)),
                VM((md, 128), F32), VM((8, nd), F32), VM((8, 128), F32),
                VM((3, 1, mm), F32), VM((3, 1, mm), F32), VM((3, 1, nn), F32), VM((3, 3, 1, nn), F32),
                VM((8, 128), F32), VM((7, 8, 128), F32), VM((8, 128), F32), VM((7, 8, 128), F32),
                dma((3,)), dma((3,)), dma((3, 3)), dma((3, 3)), dma((7,)), dma((7,)), dma((7,)), dma((7,)),
            ], collective_id=0, has_side_effects=True)
        outs = call(
            write_kernel,
            tuple(jax.ShapeDtypeStruct(s, F32) for s in dims + [(k,) for mn in dims for k in mn]),
            vmem(*first, *second), [VM] * (len(first) + len(second)), HB,
            [VM((8, mg // 8, ng), F32), VM((8, md // 8, nd), F32), dma((8,)), dma((6,))])
        return tuple(outs)

    act_spec = P(None, "row")
    cot_spec = P(None, "col")
    w_spec = P("row", "col")
    r_spec = P("row")
    c_spec = P("col")
    s_spec = P()
    return jax.shard_map(local_program, mesh=mesh, in_specs=(act_spec, act_spec, cot_spec, cot_spec, cot_spec, w_spec, w_spec, w_spec, r_spec, c_spec, r_spec, c_spec, r_spec, c_spec, s_spec, s_spec, s_spec), out_specs=(w_spec, w_spec, w_spec, r_spec, c_spec, r_spec, c_spec, r_spec, c_spec), check_vma=False)
```

```python
import functools

import jax
import jax.numpy as jnp
from jax import lax
from jax.experimental import pallas as pl
from jax.experimental.pallas import tpu as pltpu
from jax.sharding import PartitionSpec as P

EPS_SQ = 1e-30
EPS_SCALE = 1e-3
F32 = jnp.float32
BF16 = jnp.bfloat16
MESH = pl.DeviceIdType.MESH
VM = pltpu.VMEM
HB = pltpu.HBM
KB = 256
NT = 256
WIDE = 2 * NT
HB_ROWS = 512
RING = 5
PIECES = (128, 128)
GRANT = 18
CHUNKS = 4


def fold(v):
    slabs = v.reshape(-1, 8, v.shape[1])
    n = slabs.shape[0] // 4 * 4
    s = jnp.sum(slabs[:n].reshape(-1, 4, 8, v.shape[1]), axis=0)
    s = (s[0] + s[1]) + (s[2] + s[3])
    for i in range(n, slabs.shape[0]):
        s = s + slabs[i]
    return s


def dot_kernel(
    dims,
    x, h, dg, du, dd, wgh, rg, cg, ru, cu, rd, cd,
    held, ht, dt, wg, rs_g, rs_u, cs_g, cs_u, sw, ro, co,
    xs, hs, xt, ring, x_sem, h_sem, d_sem, first_sem, big_sem, s_sem,
):
    m, n = dims[0]
    nk = x.shape[0] // KB
    up = n // NT
    cots, rss, css = (dg, du), (rs_g, rs_u), (cs_g, cs_u)
    n_units = 2 * up
    tiles, unit_tile = [], []
    for q in range(2):
        odd = n % WIDE
        for c0, cols in ([(0, odd)] if odd and not q else []) + [(c, min(WIDE, n - c)) for c in range(0 if q else odd, n, WIDE)]:
            for off in range(0, cols, NT):
                unit_tile.append((len(tiles), off))
            tiles.append((q, c0, cols))

    wide0 = tiles[0][2]

    def x_copy(k):
        return pltpu.make_async_copy(x.at[pl.ds(k * KB, KB), :], xs.at[k], x_sem.at[k])

    def first_copy(k):
        return pltpu.make_async_copy(dg.at[pl.ds(k * KB, KB), pl.ds(0, wide0)], ring.at[0, pl.ds(k * KB, KB), pl.ds(0, wide0)], first_sem.at[k])

    def d_copy(t):
        q, c0, cols = tiles[t]
        return pltpu.make_async_copy(cots[q].at[:, pl.ds(c0, cols)], ring.at[t % RING, :, pl.ds(0, cols)], d_sem.at[t % RING])

    def h_copy(k):
        return pltpu.make_async_copy(h.at[pl.ds(k * HB_ROWS, HB_ROWS), :], hs.at[k % 2], h_sem.at[k % 2])

    bigs = [pltpu.make_async_copy(a, b, big_sem.at[i]) for i, (a, b) in enumerate(((wgh, wg), (dd, dt)))]
    small = [
        pltpu.make_async_copy(src, dst.at[q, 0, pl.ds(0, src.shape[0])], s_sem.at[i])
        for i, (src, dst, q) in enumerate(
            [(rg, ro, 0), (ru, ro, 1), (rd, ro, 2), (cg, co, 0), (cu, co, 1), (cd, co, 2)])
    ]
    for k in range(nk):
        x_copy(k).start()
        first_copy(k).start()

    blocks = ht.shape[0] // 128

    def h_turn(k, part):
        for c in range(part * (blocks // 2), blocks if part else blocks // 2):
            ht[pl.ds(c * 128, 128), pl.ds(k * HB_ROWS, HB_ROWS)] = hs[k % 2, :, pl.ds(c * 128, 128)].T

    def w_square(c):
        w = wg[:, pl.ds(c * 128, 128)]
        s = fold(w * w)
        if c == 0:
            sw[...] = s
        else:
            sw[...] += s

    before = {u: [] for u in range(n_units)}
    beside = [[] for _ in range(n_units)]
    heads = [u for u in range(n_units - 1) if unit_tile[u][0] != unit_tile[u + 1][0]]

    def head(u):
        return max(v for v in heads if v <= u)

    wait_h = (head(7), head(9), head(15), head(17))
    for u, k in zip((head(2), head(2), wait_h[1], head(wait_h[1] + 3)), range(4)):
        before[u].append(h_copy(k).start)
    for u, k in zip(wait_h, range(4)):
        before[u].append(h_copy(k).wait)
        for part in range(2):
            beside[u + part].append(lambda k=k, part=part: h_turn(k, part))
    before[head(11)].append(bigs[0].start)
    before[head(14)].append(bigs[1].start)
    w0 = head(19)
    before[w0].append(bigs[0].wait)
    span = n_units - w0
    for c in range(n // 128):
        beside[w0 + c * span // (n // 128)].append(lambda c=c: w_square(c))

    def run(*accs):
        def acc(z, par, p):
            return accs[(z * 2 + par) * 2 + p]

        def rhs(u, k):
            t, off = unit_tile[u]
            return ring[t % RING, pl.ds(k * KB, KB), pl.ds(off, NT)]

        def drain(u):
            q, j = divmod(u, up)
            cc = None
            for z in range(2):
                for p, size in enumerate(PIECES):
                    r0 = z * sum(PIECES) + sum(PIECES[:p])
                    g = pltpu.matmul_pop(acc(z, u % 2, p))
                    for half in range(2):
                        held[pl.ds((q * (n // 128) + 2 * j + half) * m + r0, size), :] = g[:, half * 128:half * 128 + 128]
                    s = g * g
                    lanes = s[:, :128] + s[:, 128:]
                    if j == 0:
                        rss[q][pl.ds(r0, size), :] = lanes
                    else:
                        rss[q][pl.ds(r0, size), :] += lanes
                    s = fold(s)
                    cc = s if cc is None else cc + s
            css[q][:, pl.ds(j * NT, NT)] = cc

        for z in range(2):
            for par in range(2):
                for p in range(2):
                    pltpu.matmul_pop(acc(z, par, p))

        for u in range(n_units):
            last = u == n_units - 1
            t = unit_tile[u][0]
            if not last and unit_tile[u + 1][0] != t:
                if u:
                    d_copy(t + 1).wait()
                if t and t - 1 + RING < len(tiles):
                    d_copy(t - 1 + RING).start()
                for f in before.pop(u):
                    f()
            for k in range(nk):
                if u == 0:
                    x_copy(k).wait()
                    first_copy(k).wait()
                    for z in range(2):
                        xt[pl.ds(z * 256, 256), pl.ds(k * KB, KB)] = xs[k, :, pl.ds(z * 256, 256)].T
                        pltpu.matmul_push_rhs(rhs(0, k), staging_register=k % 2, mxu_index=z)
                    if k % 2 and k // 2 + 1 < RING:
                        d_copy(k // 2 + 1).start()
                    if k == nk - 1 and unit_tile[1][0] == 1:
                        d_copy(1).wait()
                for z in range(2):
                    for p, size in enumerate(PIECES):
                        r0 = z * sum(PIECES) + sum(PIECES[:p])
                        pltpu.matmul_acc_lhs(acc(z, u % 2, p), xt[pl.ds(r0, size), pl.ds(k * KB, KB)],
                                             load_staged_rhs=(k % 2 if p == 0 else None))
                    if k < nk - 1:
                        if u:
                            pltpu.matmul_push_rhs(rhs(u, k + 1), staging_register=(k + 1) % 2, mxu_index=z)
                    elif not last:
                        pltpu.matmul_push_rhs(rhs(u + 1, 0), staging_register=0, mxu_index=z)
                if k == 1 and u:
                    drain(u - 1)
                if k == 2:
                    for f in beside[u]:
                        f()
        drain(n_units - 1)
        assert not any(before.values())

    for c in small:
        c.start()
    pl.run_scoped(run, *[pltpu.ACC(z)((size, NT), F32) for z in range(2) for par in range(2) for size in PIECES])
    for c in bigs[1:] + small:
        c.wait()


def exchange_kernel(
    dims,
    held, ht, dt, wg, rs_g, rs_u, cs_g, cs_u, sw_g, ro, co,
    wuh, wdh,
    b2, rel, clip,
    late, wu, wd, a_g, a_u, a_d, b_g, b_u, b_d, r_g, c_g, r_u, c_u, r_d, c_d,
    w_sem, rs_d, cs_d, sw, rsend, rrecv, csend, crecv, pay, got, pay2, got2, r1s, r1r, c1s, c1r, p_s, p_r, p2_s, p2_r,
):
    col = lax.axis_index("col")
    row = lax.axis_index("row")
    row_peer = (row + 1 - 2 * (row % 2), (row + 2) % 4, 3 - row)
    mats = (
        dict(rs=rs_g, cs=cs_g, a=a_g, b=b_g, r=r_g, c=c_g),
        dict(rs=rs_u, cs=cs_u, a=a_u, b=b_u, r=r_u, c=c_u),
        dict(rs=rs_d, cs=cs_d, a=a_d, b=b_d, r=r_d, c=c_d),
    )
    for mat, (m, n) in zip(mats, dims):
        mat["m"], mat["n"] = m, n
        mat["mt"], mat["nt"] = m * 4, n * 2
    (mg, ng), (md, nd) = dims[0], dims[2]
    size = mg * ng // 128

    barrier = pltpu.get_barrier_semaphore()
    plane = [{"row": p, "col": cc} for cc in (col, 1 - col) for p in (row,) + row_peer][1:]
    for dev in plane:
        pl.semaphore_signal(barrier, inc=1, device_id=dev, device_id_type=MESH)

    loads = [pltpu.make_async_copy(a, b, w_sem.at[i]) for i, (a, b) in enumerate(((wuh, wu), (wdh, wd)))]
    for c in loads:
        c.start()
    pay[...] = jnp.zeros_like(pay)
    pay2[...] = jnp.zeros_like(pay2)

    def w_square(q, w):
        m, n = dims[q]
        sw[...] = jnp.zeros_like(sw)

        @pl.loop(0, n // 256)
        def _(c):
            c0 = pl.multiple_of(c * 256, 256)
            a, b = w[:, pl.ds(c0, 128)], w[:, pl.ds(c0 + 128, 128)]
            sw[...] += fold(a * a) + fold(b * b)

        pay[pl.ds(q, 1), :] = jnp.sum(sw[...], axis=0, keepdims=True)

    def first_sends(q):
        mat = mats[q]
        m, n = mat["m"], mat["n"]
        copies = [pltpu.make_async_remote_copy(
            rsend.at[q, :, pl.ds(0, m)], rrecv.at[q, :, pl.ds(0, m)], r1s.at[q], r1r.at[q],
            device_id={"col": 1 - col}, device_id_type=MESH)]
        for d in range(3):
            copies.append(pltpu.make_async_remote_copy(
                csend.at[q, :, pl.ds(0, n)], crecv.at[q, d, :, pl.ds(0, n)], c1s.at[q, d], c1r.at[q, d],
                device_id={"row": row_peer[d]}, device_id_type=MESH))
        return copies

    def first_reduce(q):
        mat = mats[q]
        csend[q, :, pl.ds(0, mat["n"])] = jnp.sum(mat["cs"][...], axis=0, keepdims=True)
        for b in range(mat["m"] // 128):
            t = mat["rs"][pl.ds(b * 128, 128), :].T
            rsend[q, :, pl.ds(b * 128, 128)] = jnp.sum(t, axis=0, keepdims=True)

    def new_stats(q):
        mat = mats[q]
        m, n = mat["m"], mat["n"]
        beta = b2[0, 0]
        rsum = rsend[q, :, pl.ds(0, m)] + rrecv[q, :, pl.ds(0, m)]
        r_new = beta * ro[q, :, pl.ds(0, m)] + (1.0 - beta) * (rsum * (1.0 / mat["nt"]) + EPS_SQ)
        mat["r"][...] = r_new
        csum = (csend[q, :, pl.ds(0, n)] + crecv[q, 0, :, pl.ds(0, n)]) + (
            crecv[q, 1, :, pl.ds(0, n)] + crecv[q, 2, :, pl.ds(0, n)])
        c_new = beta * co[q, :, pl.ds(0, n)] + (1.0 - beta) * (csum * (1.0 / mat["mt"]) + EPS_SQ)
        mat["c"][...] = c_new
        mat["b"][...] = lax.rsqrt(c_new)
        alpha = lax.rsqrt(r_new)
        rp = r_new[:, :128]
        for b in range(m // 128):
            blk = jnp.broadcast_to(alpha[:, b * 128:(b + 1) * 128], (128, 128))
            mat["a"][pl.ds(b * 128, 128), :] = blk.T
            if b:
                rp = rp + r_new[:, b * 128:(b + 1) * 128]
        if q == 2:
            pay2[pl.ds(3, 1), :] = rp
        else:
            pay[pl.ds(3 + q, 1), :] = rp

    def u_square(q, rows):
        mat = mats[q]
        m, n = mat["m"], mat["n"]
        src, first = (late, 0) if q == 2 else (held, q * size)
        blocks = n // 128

        def chunk(r, sums):
            r0 = pl.multiple_of(r * rows, 8)
            a = mat["a"][pl.ds(r0, rows), :]
            new = []
            for c in range(blocks):
                t = src[pl.ds(pl.multiple_of(first + c * m + r0, 8), rows), :] * a
                new.append(sums[c] + fold(t * t))
            return tuple(new)

        sums = lax.fori_loop(0, m // rows, chunk, (jnp.zeros((8, 128), F32),) * blocks)
        total = None
        for c in range(blocks):
            bb = mat["b"][:, c * 128:(c + 1) * 128]
            s = sums[c] * (bb * bb)
            total = s if total is None else total + s
        pay2[pl.ds(q, 1), :] = jnp.sum(total, axis=0, keepdims=True)

    rows = md // CHUNKS
    steps = nd // NT * CHUNKS

    def product(i):
        j, c = divmod(i, CHUNKS)
        rr = pl.ds(c * rows, rows)
        g = jnp.dot(ht[rr, :], dt[:, pl.ds(j * NT, NT)], preferred_element_type=F32)
        for half in range(2):
            late[pl.ds((2 * j + half) * md + c * rows, rows), :] = g[:, half * 128:half * 128 + 128]
        s = g * g
        lanes = s[:, :128] + s[:, 128:]
        if j == 0:
            rs_d[rr, :] = lanes
        else:
            rs_d[rr, :] += lanes
        cc = pl.ds(j * NT, NT)
        if c == 0:
            cs_d[:, cc] = fold(s)
        else:
            cs_d[:, cc] += fold(s)

    def plane_sends(src, dst, rows, s_sem, r_sem):
        rr = pl.ds(0, rows)
        return [pltpu.make_async_remote_copy(src.at[rr], dst.at[i, rr], s_sem.at[i], r_sem.at[i], device_id=dev, device_id_type=MESH)
                for i, dev in enumerate(plane)]

    def plane_sum(src, dst, rows):
        a = [src[pl.ds(0, rows), :]] + [dst[i, pl.ds(0, rows), :] for i in range(len(plane))]
        total = ((a[0] + a[1]) + (a[2] + a[3])) + ((a[4] + a[5]) + (a[6] + a[7]))
        return jnp.sum(total, axis=1, keepdims=True)

    early = [c for q in range(2) for c in first_sends(q)]
    for i in range(steps):
        if i == CHUNKS:
            first_reduce(0)
            first_reduce(1)
            pl.semaphore_wait(barrier, len(plane))
            for c in early:
                c.start()
        product(i)
    first_reduce(2)
    sends = first_sends(2)
    for c in sends:
        c.start()
    for c in early:
        c.wait()
    pay[pl.ds(0, 1), :] = jnp.sum(sw_g[...], axis=0, keepdims=True)
    for q in range(2):
        new_stats(q)
    for c in loads:
        c.wait()
    w_square(1, wu)
    w_square(2, wd)
    sums = plane_sends(pay, got, 5, p_s, p_r)
    for c in sums:
        c.start()
    for q in range(2):
        u_square(q, 64)
    for c in sends:
        c.wait()
    new_stats(2)
    u_square(2, md // 4)
    sums2 = plane_sends(pay2, got2, 4, p2_s, p2_r)
    for c in sums2:
        c.start()
    for c in sums + sums2:
        c.wait()
    norms = plane_sum(pay, got, 5)
    shapes = plane_sum(pay2, got2, 4)
    for q, mat in enumerate(mats):
        count = float(mat["mt"] * mat["nt"])
        r_sum = shapes[3:4] if q == 2 else norms[3 + q:4 + q]
        r_mean = r_sum * (0.5 / mat["mt"])
        u_rms = jnp.sqrt(r_mean * shapes[q:q + 1] / count)
        w_rms = jnp.sqrt(norms[q:q + 1] / count)
        step = rel[0, 0] * jnp.maximum(EPS_SCALE, w_rms)
        k = step * jnp.sqrt(r_mean) / jnp.maximum(1.0, u_rms / clip[0, 0])
        mat["b"][...] = mat["b"][...] * k


def write_kernel(
    dims,
    held, ht, dt, w_g, rs_g, rs_u, cs_g, cs_u, sw_g, ro, co,
    late, w_u, w_d, a_g, a_u, a_d, b_g, b_u, b_d, r_g, c_g, r_u, c_u, r_d, c_d,
    o_g, o_u, o_d, or_g, oc_g, or_u, oc_u, or_d, oc_d,
    wide, tall, o_sem, s_sem,
):
    small = [pltpu.make_async_copy(s.at[0], d, s_sem.at[i]) for i, (s, d) in enumerate(
        [(r_g, or_g), (c_g, oc_g), (r_u, or_u), (c_u, oc_u), (r_d, or_d), (c_d, oc_d)])]
    for c in small:
        c.start()
    slots = 8
    size = dims[0][0] * dims[0][1] // 128
    where = ((held, 0, w_g), (held, 1, w_u), (late, 0, w_d))
    pending = {}
    step = 0
    for q, a, b, o, buf in ((2, a_d, b_d, o_d, tall), (1, a_u, b_u, o_u, wide), (0, a_g, b_g, o_g, wide)):
        rows = buf.shape[1]
        src, k, w = where[q]
        for t in range(dims[q][0] // rows):
            slot = step % slots
            if slot in pending:
                pending.pop(slot).wait()
            rr = pl.ds(t * rows, rows)
            scale = a[rr, :]
            for c in range(dims[q][1] // 128):
                cc = pl.ds(c * 128, 128)
                off = c * dims[q][0] + t * rows
                g = src[pl.ds(k * size + off, rows), :]
                buf[slot, :, cc] = w[rr, cc] - (g * scale) * b[:, cc]
            cp = pltpu.make_async_copy(buf.at[slot], o.at[rr, :], o_sem.at[slot])
            cp.start()
            pending[slot] = cp
            step += 1
    for cp in pending.values():
        cp.wait()
    for c in small:
        c.wait()


def solution(mesh):
    def local_program(x_in, h_act, d_gate, d_up, d_out, w_gate, w_up, w_down, r_gate, c_gate, r_up, c_up, r_down, c_down, beta_two, rel_step, clip_thr):
        (mg, ng), (md, nd) = w_gate.shape, w_down.shape
        tokens = x_in.shape[0]
        nk = tokens // KB
        def hbm(*arrays):
            return tuple(pltpu.with_memory_space_constraint(v, HB) for v in arrays)

        def vmem(*arrays):
            return tuple(pltpu.with_memory_space_constraint(v, VM) for v in arrays)

        one = tuple(v.reshape(1, 1) for v in (beta_two, rel_step, clip_thr))
        dims = [(mg, ng), (mg, ng), (md, nd)]
        mm, nn = max(mg, md), max(ng, nd)
        dma = pltpu.SemaphoreType.DMA

        def call(kernel, outs, args, in_spaces, out_space, scratch, **params):
            return pl.pallas_call(
                functools.partial(kernel, dims),
                out_shape=outs,
                in_specs=[pl.BlockSpec(memory_space=v) for v in in_spaces],
                out_specs=tuple(pl.BlockSpec(memory_space=out_space) for _ in outs),
                scratch_shapes=scratch,
                compiler_params=pltpu.CompilerParams(vmem_limit_bytes=GRANT * 2**20, **params),
                name=kernel.__name__,
            )(*args)

        def vm(shapes):
            return tuple(VM(s, F32) for s in shapes)

        def vm(shapes):
            return tuple(VM(s, F32) for s in shapes)

        size = mg * ng // 128
        lanes = [(m, 128) for m, _ in dims]
        stats = [s for m, n in dims for s in ((1, m), (1, n))]
        first = call(
            dot_kernel,
            vm([(2 * size, 128)]) + (VM((md, tokens), BF16), VM((tokens, nd), BF16))
            + vm(dims[:1] + lanes[:2] + [(8, ng), (8, ng), (8, 128), (3, 1, mm), (3, 1, nn)]),
            hbm(x_in, h_act, d_gate, d_up, d_out, w_gate, r_gate, c_gate, r_up, c_up, r_down, c_down), [HB] * 12, VM,
            [
                VM((nk, KB, mg), BF16), VM((2, HB_ROWS, md), BF16), VM((mg, tokens), BF16), VM((RING, tokens, WIDE), BF16),
                dma((nk,)), dma((2,)), dma((RING,)), dma((nk,)), dma((2,)), dma((6,)),
            ])
        second = call(
            exchange_kernel,
            vm([(size, 128)] + dims[1:] + lanes + [(1, n) for _, n in dims] + stats),
            vmem(*first) + hbm(w_up, w_down) + one, [VM] * len(first) + [HB] * 2 + [pltpu.SMEM] * 3, VM,
            [
                dma((2,)),
                VM((md, 128), F32), VM((8, nd), F32), VM((8, 128), F32),
                VM((3, 1, mm), F32), VM((3, 1, mm), F32), VM((3, 1, nn), F32), VM((3, 3, 1, nn), F32),
                VM((8, 128), F32), VM((7, 8, 128), F32), VM((8, 128), F32), VM((7, 8, 128), F32),
                dma((3,)), dma((3,)), dma((3, 3)), dma((3, 3)), dma((7,)), dma((7,)), dma((7,)), dma((7,)),
            ], collective_id=0, has_side_effects=True)
        outs = call(
            write_kernel,
            tuple(jax.ShapeDtypeStruct(s, F32) for s in dims + [(k,) for mn in dims for k in mn]),
            vmem(*first, *second), [VM] * (len(first) + len(second)), HB,
            [VM((8, mg // 8, ng), F32), VM((8, md // 8, nd), F32), dma((8,)), dma((6,))])
        return tuple(outs)

    act_spec = P(None, "row")
    cot_spec = P(None, "col")
    w_spec = P("row", "col")
    r_spec = P("row")
    c_spec = P("col")
    s_spec = P()
    return jax.shard_map(local_program, mesh=mesh, in_specs=(act_spec, act_spec, cot_spec, cot_spec, cot_spec, w_spec, w_spec, w_spec, r_spec, c_spec, r_spec, c_spec, r_spec, c_spec, s_spec, s_spec, s_spec), out_specs=(w_spec, w_spec, w_spec, r_spec, c_spec, r_spec, c_spec, r_spec, c_spec), check_vma=False)
```

```python
import functools

import jax
import jax.numpy as jnp
from jax import lax
from jax.experimental import pallas as pl
from jax.experimental.pallas import tpu as pltpu
from jax.sharding import PartitionSpec as P

EPS_SQ = 1e-30
EPS_SCALE = 1e-3
F32 = jnp.float32
BF16 = jnp.bfloat16
MESH = pl.DeviceIdType.MESH
VM = pltpu.VMEM
HB = pltpu.HBM
KB = 256
NT = 256
WIDE = 2 * NT
HB_ROWS = 512
RING = 5
PIECES = (128, 128)
GRANT = 18
CHUNKS = 4


def fold(v):
    slabs = v.reshape(-1, 8, v.shape[1])
    n = slabs.shape[0] // 4 * 4
    s = jnp.sum(slabs[:n].reshape(-1, 4, 8, v.shape[1]), axis=0)
    s = (s[0] + s[1]) + (s[2] + s[3])
    for i in range(n, slabs.shape[0]):
        s = s + slabs[i]
    return s


def dot_kernel(
    dims,
    x, h, dg, du, dd, wgh, rg, cg, ru, cu, rd, cd,
    held, ht, dt, wg, rs_g, rs_u, cs_g, cs_u, sw, ro, co,
    xs, hs, xt, ring, x_sem, h_sem, d_sem, first_sem, big_sem, s_sem,
):
    m, n = dims[0]
    nk = x.shape[0] // KB
    up = n // NT
    cots, rss, css = (dg, du), (rs_g, rs_u), (cs_g, cs_u)
    n_units = 2 * up
    tiles, unit_tile = [], []
    for q in range(2):
        odd = n % WIDE
        for c0, cols in ([(0, odd)] if odd and not q else []) + [(c, min(WIDE, n - c)) for c in range(0 if q else odd, n, WIDE)]:
            for off in range(0, cols, NT):
                unit_tile.append((len(tiles), off))
            tiles.append((q, c0, cols))

    wide0 = tiles[0][2]

    def x_copy(k):
        return pltpu.make_async_copy(x.at[pl.ds(k * KB, KB), :], xs.at[k], x_sem.at[k])

    def first_copy(k):
        return pltpu.make_async_copy(dg.at[pl.ds(k * KB, KB), pl.ds(0, wide0)], ring.at[0, pl.ds(k * KB, KB), pl.ds(0, wide0)], first_sem.at[k])

    def d_copy(t):
        q, c0, cols = tiles[t]
        return pltpu.make_async_copy(cots[q].at[:, pl.ds(c0, cols)], ring.at[t % RING, :, pl.ds(0, cols)], d_sem.at[t % RING])

    def h_copy(k):
        return pltpu.make_async_copy(h.at[pl.ds(k * HB_ROWS, HB_ROWS), :], hs.at[k % 2], h_sem.at[k % 2])

    bigs = [pltpu.make_async_copy(a, b, big_sem.at[i]) for i, (a, b) in enumerate(((wgh, wg), (dd, dt)))]
    small = [
        pltpu.make_async_copy(src, dst.at[q, 0, pl.ds(0, src.shape[0])], s_sem.at[i])
        for i, (src, dst, q) in enumerate(
            [(rg, ro, 0), (ru, ro, 1), (rd, ro, 2), (cg, co, 0), (cu, co, 1), (cd, co, 2)])
    ]
    for k in range(nk):
        x_copy(k).start()
        first_copy(k).start()

    blocks = ht.shape[0] // 128

    def h_turn(k, part):
        for c in range(part * (blocks // 2), blocks if part else blocks // 2):
            ht[pl.ds(c * 128, 128), pl.ds(k * HB_ROWS, HB_ROWS)] = hs[k % 2, :, pl.ds(c * 128, 128)].T

    def w_square(c):
        w = wg[:, pl.ds(c * 128, 128)]
        s = fold(w * w)
        if c == 0:
            sw[...] = s
        else:
            sw[...] += s

    before = {u: [] for u in range(n_units)}
    beside = [[] for _ in range(n_units)]
    heads = [u for u in range(n_units - 1) if unit_tile[u][0] != unit_tile[u + 1][0]]

    def head(u):
        return max(v for v in heads if v <= u)

    wait_h = (head(7), head(9), head(15), head(17))
    for u, k in zip((head(2), head(2), wait_h[1], head(wait_h[1] + 3)), range(4)):
        before[u].append(h_copy(k).start)
    for u, k in zip(wait_h, range(4)):
        before[u].append(h_copy(k).wait)
        for part in range(2):
            beside[u + part].append(lambda k=k, part=part: h_turn(k, part))
    before[head(13)].append(bigs[0].start)
    before[head(15)].append(bigs[1].start)
    w0 = head(20)
    before[w0].append(bigs[0].wait)
    span = n_units - w0
    for c in range(n // 128):
        beside[w0 + c * span // (n // 128)].append(lambda c=c: w_square(c))

    def run(*accs):
        def acc(z, par, p):
            return accs[(z * 2 + par) * 2 + p]

        def rhs(u, k):
            t, off = unit_tile[u]
            return ring[t % RING, pl.ds(k * KB, KB), pl.ds(off, NT)]

        def drain(u):
            q, j = divmod(u, up)
            cc = None
            for z in range(2):
                for p, size in enumerate(PIECES):
                    r0 = z * sum(PIECES) + sum(PIECES[:p])
                    g = pltpu.matmul_pop(acc(z, u % 2, p))
                    for half in range(2):
                        held[pl.ds((q * (n // 128) + 2 * j + half) * m + r0, size), :] = g[:, half * 128:half * 128 + 128]
                    s = g * g
                    lanes = s[:, :128] + s[:, 128:]
                    if j == 0:
                        rss[q][pl.ds(r0, size), :] = lanes
                    else:
                        rss[q][pl.ds(r0, size), :] += lanes
                    s = fold(s)
                    cc = s if cc is None else cc + s
            css[q][:, pl.ds(j * NT, NT)] = cc

        for z in range(2):
            for par in range(2):
                for p in range(2):
                    pltpu.matmul_pop(acc(z, par, p))

        for u in range(n_units):
            last = u == n_units - 1
            t = unit_tile[u][0]
            if not last and unit_tile[u + 1][0] != t:
                if u:
                    d_copy(t + 1).wait()
                if t and t - 1 + RING < len(tiles):
                    d_copy(t - 1 + RING).start()
                for f in before.pop(u):
                    f()
            for k in range(nk):
                if u == 0:
                    x_copy(k).wait()
                    first_copy(k).wait()
                    for z in range(2):
                        xt[pl.ds(z * 256, 256), pl.ds(k * KB, KB)] = xs[k, :, pl.ds(z * 256, 256)].T
                        pltpu.matmul_push_rhs(rhs(0, k), staging_register=k % 2, mxu_index=z)
                    if k % 2 and k // 2 + 1 < RING:
                        d_copy(k // 2 + 1).start()
                    if k == nk - 1 and unit_tile[1][0] == 1:
                        d_copy(1).wait()
                for z in range(2):
                    for p, size in enumerate(PIECES):
                        r0 = z * sum(PIECES) + sum(PIECES[:p])
                        pltpu.matmul_acc_lhs(acc(z, u % 2, p), xt[pl.ds(r0, size), pl.ds(k * KB, KB)],
                                             load_staged_rhs=(k % 2 if p == 0 else None))
                    if k < nk - 1:
                        if u:
                            pltpu.matmul_push_rhs(rhs(u, k + 1), staging_register=(k + 1) % 2, mxu_index=z)
                    elif not last:
                        pltpu.matmul_push_rhs(rhs(u + 1, 0), staging_register=0, mxu_index=z)
                if k == 1 and u:
                    drain(u - 1)
                if k == 2:
                    for f in beside[u]:
                        f()
        drain(n_units - 1)
        assert not any(before.values())

    for c in small:
        c.start()
    pl.run_scoped(run, *[pltpu.ACC(z)((size, NT), F32) for z in range(2) for par in range(2) for size in PIECES])
    for c in bigs[1:] + small:
        c.wait()


def exchange_kernel(
    dims,
    held, ht, dt, wg, rs_g, rs_u, cs_g, cs_u, sw_g, ro, co,
    wuh, wdh,
    b2, rel, clip,
    late, wu, wd, a_g, a_u, a_d, b_g, b_u, b_d, r_g, c_g, r_u, c_u, r_d, c_d,
    w_sem, rs_d, cs_d, rsend, rrecv, csend, crecv, pay, got, pay2, got2, r1s, r1r, c1s, c1r, p_s, p_r, p2_s, p2_r,
):
    col = lax.axis_index("col")
    row = lax.axis_index("row")
    row_peer = (row + 1 - 2 * (row % 2), (row + 2) % 4, 3 - row)
    mats = (
        dict(rs=rs_g, cs=cs_g, a=a_g, b=b_g, r=r_g, c=c_g),
        dict(rs=rs_u, cs=cs_u, a=a_u, b=b_u, r=r_u, c=c_u),
        dict(rs=rs_d, cs=cs_d, a=a_d, b=b_d, r=r_d, c=c_d),
    )
    for mat, (m, n) in zip(mats, dims):
        mat["m"], mat["n"] = m, n
        mat["mt"], mat["nt"] = m * 4, n * 2
    (mg, ng), (md, nd) = dims[0], dims[2]
    size = mg * ng // 128

    barrier = pltpu.get_barrier_semaphore()
    plane = [{"row": p, "col": cc} for cc in (col, 1 - col) for p in (row,) + row_peer][1:]
    for dev in plane:
        pl.semaphore_signal(barrier, inc=1, device_id=dev, device_id_type=MESH)

    loads = [pltpu.make_async_copy(a, b, w_sem.at[i]) for i, (a, b) in enumerate(((wuh, wu), (wdh, wd)))]
    for c in loads:
        c.start()
    pay[...] = jnp.zeros_like(pay)
    pay2[...] = jnp.zeros_like(pay2)

    def w_square(q, w, rows):
        m, n = dims[q]

        def chunk(r, sums):
            rr = pl.ds(pl.multiple_of(r * rows, 8), rows)
            new = []
            for c in range(n // 128):
                v = w[rr, c * 128:(c + 1) * 128]
                new.append(sums[c] + fold(v * v))
            return tuple(new)

        sums = lax.fori_loop(0, m // rows, chunk, (jnp.zeros((8, 128), F32),) * (n // 128))
        total = sums[0]
        for v in sums[1:]:
            total = total + v
        pay[pl.ds(q, 1), :] = jnp.sum(total, axis=0, keepdims=True)

    def first_sends(q):
        mat = mats[q]
        m, n = mat["m"], mat["n"]
        copies = [pltpu.make_async_remote_copy(
            rsend.at[q, :, pl.ds(0, m)], rrecv.at[q, :, pl.ds(0, m)], r1s.at[q], r1r.at[q],
            device_id={"col": 1 - col}, device_id_type=MESH)]
        for d in range(3):
            copies.append(pltpu.make_async_remote_copy(
                csend.at[q, :, pl.ds(0, n)], crecv.at[q, d, :, pl.ds(0, n)], c1s.at[q, d], c1r.at[q, d],
                device_id={"row": row_peer[d]}, device_id_type=MESH))
        return copies

    def first_reduce(q):
        mat = mats[q]
        csend[q, :, pl.ds(0, mat["n"])] = jnp.sum(mat["cs"][...], axis=0, keepdims=True)
        for b in range(mat["m"] // 128):
            t = mat["rs"][pl.ds(b * 128, 128), :].T
            rsend[q, :, pl.ds(b * 128, 128)] = jnp.sum(t, axis=0, keepdims=True)

    def new_stats(q):
        mat = mats[q]
        m, n = mat["m"], mat["n"]
        beta = b2[0, 0]
        rsum = rsend[q, :, pl.ds(0, m)] + rrecv[q, :, pl.ds(0, m)]
        r_new = beta * ro[q, :, pl.ds(0, m)] + (1.0 - beta) * (rsum * (1.0 / mat["nt"]) + EPS_SQ)
        mat["r"][...] = r_new
        csum = (csend[q, :, pl.ds(0, n)] + crecv[q, 0, :, pl.ds(0, n)]) + (
            crecv[q, 1, :, pl.ds(0, n)] + crecv[q, 2, :, pl.ds(0, n)])
        c_new = beta * co[q, :, pl.ds(0, n)] + (1.0 - beta) * (csum * (1.0 / mat["mt"]) + EPS_SQ)
        mat["c"][...] = c_new
        mat["b"][...] = lax.rsqrt(c_new)
        alpha = lax.rsqrt(r_new)
        rp = r_new[:, :128]
        for b in range(m // 128):
            blk = jnp.broadcast_to(alpha[:, b * 128:(b + 1) * 128], (128, 128))
            mat["a"][pl.ds(b * 128, 128), :] = blk.T
            if b:
                rp = rp + r_new[:, b * 128:(b + 1) * 128]
        if q == 2:
            pay2[pl.ds(3, 1), :] = rp
        else:
            pay[pl.ds(3 + q, 1), :] = rp

    def u_square(q, rows):
        mat = mats[q]
        m, n = mat["m"], mat["n"]
        src, first = (late, 0) if q == 2 else (held, q * size)
        blocks = n // 128

        def chunk(r, sums):
            r0 = pl.multiple_of(r * rows, 8)
            a = mat["a"][pl.ds(r0, rows), :]
            new = []
            for c in range(blocks):
                t = src[pl.ds(pl.multiple_of(first + c * m + r0, 8), rows), :] * a
                new.append(sums[c] + fold(t * t))
            return tuple(new)

        sums = lax.fori_loop(0, m // rows, chunk, (jnp.zeros((8, 128), F32),) * blocks)
        total = None
        for c in range(blocks):
            bb = mat["b"][:, c * 128:(c + 1) * 128]
            s = sums[c] * (bb * bb)
            total = s if total is None else total + s
        pay2[pl.ds(q, 1), :] = jnp.sum(total, axis=0, keepdims=True)

    rows = md // CHUNKS
    steps = nd // NT * CHUNKS

    def product(i):
        j, c = divmod(i, CHUNKS)
        rr = pl.ds(c * rows, rows)
        g = jnp.dot(ht[rr, :], dt[:, pl.ds(j * NT, NT)], preferred_element_type=F32)
        for half in range(2):
            late[pl.ds((2 * j + half) * md + c * rows, rows), :] = g[:, half * 128:half * 128 + 128]
        s = g * g
        lanes = s[:, :128] + s[:, 128:]
        if j == 0:
            rs_d[rr, :] = lanes
        else:
            rs_d[rr, :] += lanes
        cc = pl.ds(j * NT, NT)
        if c == 0:
            cs_d[:, cc] = fold(s)
        else:
            cs_d[:, cc] += fold(s)

    def plane_sends(src, dst, rows, s_sem, r_sem):
        rr = pl.ds(0, rows)
        return [pltpu.make_async_remote_copy(src.at[rr], dst.at[i, rr], s_sem.at[i], r_sem.at[i], device_id=dev, device_id_type=MESH)
                for i, dev in enumerate(plane)]

    def plane_sum(src, dst, rows):
        a = [src[pl.ds(0, rows), :]] + [dst[i, pl.ds(0, rows), :] for i in range(len(plane))]
        total = ((a[0] + a[1]) + (a[2] + a[3])) + ((a[4] + a[5]) + (a[6] + a[7]))
        return jnp.sum(total, axis=1, keepdims=True)

    early = [c for q in range(2) for c in first_sends(q)]
    for i in range(steps):
        if i == CHUNKS:
            first_reduce(0)
            first_reduce(1)
            pl.semaphore_wait(barrier, len(plane))
            for c in early:
                c.start()
        product(i)
    first_reduce(2)
    sends = first_sends(2)
    for c in sends:
        c.start()
    for c in early:
        c.wait()
    pay[pl.ds(0, 1), :] = jnp.sum(sw_g[...], axis=0, keepdims=True)
    for q in range(2):
        new_stats(q)
    for c in loads:
        c.wait()
    w_square(1, wu, 64)
    w_square(2, wd, md // 8)
    sums = plane_sends(pay, got, 5, p_s, p_r)
    for c in sums:
        c.start()
    for q in range(2):
        u_square(q, 64)
    for c in sends:
        c.wait()
    new_stats(2)
    u_square(2, md // 8)
    sums2 = plane_sends(pay2, got2, 4, p2_s, p2_r)
    for c in sums2:
        c.start()
    for c in sums + sums2:
        c.wait()
    norms = plane_sum(pay, got, 5)
    shapes = plane_sum(pay2, got2, 4)
    for q, mat in enumerate(mats):
        count = float(mat["mt"] * mat["nt"])
        r_sum = shapes[3:4] if q == 2 else norms[3 + q:4 + q]
        r_mean = r_sum * (0.5 / mat["mt"])
        u_rms = jnp.sqrt(r_mean * shapes[q:q + 1] / count)
        w_rms = jnp.sqrt(norms[q:q + 1] / count)
        step = rel[0, 0] * jnp.maximum(EPS_SCALE, w_rms)
        k = step * jnp.sqrt(r_mean) / jnp.maximum(1.0, u_rms / clip[0, 0])
        mat["b"][...] = mat["b"][...] * k


def write_kernel(
    dims,
    held, ht, dt, w_g, rs_g, rs_u, cs_g, cs_u, sw_g, ro, co,
    late, w_u, w_d, a_g, a_u, a_d, b_g, b_u, b_d, r_g, c_g, r_u, c_u, r_d, c_d,
    o_g, o_u, o_d, or_g, oc_g, or_u, oc_u, or_d, oc_d,
    wide, tall, o_sem, s_sem,
):
    small = [pltpu.make_async_copy(s.at[0], d, s_sem.at[i]) for i, (s, d) in enumerate(
        [(r_g, or_g), (c_g, oc_g), (r_u, or_u), (c_u, oc_u), (r_d, or_d), (c_d, oc_d)])]
    for c in small:
        c.start()
    slots = 8
    size = dims[0][0] * dims[0][1] // 128
    where = ((held, 0, w_g), (held, 1, w_u), (late, 0, w_d))
    pending = {}
    step = 0
    for q, a, b, o, buf in ((2, a_d, b_d, o_d, tall), (1, a_u, b_u, o_u, wide), (0, a_g, b_g, o_g, wide)):
        rows = buf.shape[1]
        src, k, w = where[q]
        for t in range(dims[q][0] // rows):
            slot = step % slots
            if slot in pending:
                pending.pop(slot).wait()
            rr = pl.ds(t * rows, rows)
            scale = a[rr, :]
            for c in range(dims[q][1] // 128):
                cc = pl.ds(c * 128, 128)
                off = c * dims[q][0] + t * rows
                g = src[pl.ds(k * size + off, rows), :]
                buf[slot, :, cc] = w[rr, cc] - (g * scale) * b[:, cc]
            cp = pltpu.make_async_copy(buf.at[slot], o.at[rr, :], o_sem.at[slot])
            cp.start()
            pending[slot] = cp
            step += 1
    for cp in pending.values():
        cp.wait()
    for c in small:
        c.wait()


def solution(mesh):
    def local_program(x_in, h_act, d_gate, d_up, d_out, w_gate, w_up, w_down, r_gate, c_gate, r_up, c_up, r_down, c_down, beta_two, rel_step, clip_thr):
        (mg, ng), (md, nd) = w_gate.shape, w_down.shape
        tokens = x_in.shape[0]
        nk = tokens // KB
        def hbm(*arrays):
            return tuple(pltpu.with_memory_space_constraint(v, HB) for v in arrays)

        def vmem(*arrays):
            return tuple(pltpu.with_memory_space_constraint(v, VM) for v in arrays)

        one = tuple(v.reshape(1, 1) for v in (beta_two, rel_step, clip_thr))
        dims = [(mg, ng), (mg, ng), (md, nd)]
        mm, nn = max(mg, md), max(ng, nd)
        dma = pltpu.SemaphoreType.DMA

        def call(kernel, outs, args, in_spaces, out_space, scratch, **params):
            return pl.pallas_call(
                functools.partial(kernel, dims),
                out_shape=outs,
                in_specs=[pl.BlockSpec(memory_space=v) for v in in_spaces],
                out_specs=tuple(pl.BlockSpec(memory_space=out_space) for _ in outs),
                scratch_shapes=scratch,
                compiler_params=pltpu.CompilerParams(vmem_limit_bytes=GRANT * 2**20, **params),
                name=kernel.__name__,
            )(*args)

        def vm(shapes):
            return tuple(VM(s, F32) for s in shapes)

        def vm(shapes):
            return tuple(VM(s, F32) for s in shapes)

        size = mg * ng // 128
        lanes = [(m, 128) for m, _ in dims]
        stats = [s for m, n in dims for s in ((1, m), (1, n))]
        first = call(
            dot_kernel,
            vm([(2 * size, 128)]) + (VM((md, tokens), BF16), VM((tokens, nd), BF16))
            + vm(dims[:1] + lanes[:2] + [(8, ng), (8, ng), (8, 128), (3, 1, mm), (3, 1, nn)]),
            hbm(x_in, h_act, d_gate, d_up, d_out, w_gate, r_gate, c_gate, r_up, c_up, r_down, c_down), [HB] * 12, VM,
            [
                VM((nk, KB, mg), BF16), VM((2, HB_ROWS, md), BF16), VM((mg, tokens), BF16), VM((RING, tokens, WIDE), BF16),
                dma((nk,)), dma((2,)), dma((RING,)), dma((nk,)), dma((2,)), dma((6,)),
            ])
        second = call(
            exchange_kernel,
            vm([(size, 128)] + dims[1:] + lanes + [(1, n) for _, n in dims] + stats),
            vmem(*first) + hbm(w_up, w_down) + one, [VM] * len(first) + [HB] * 2 + [pltpu.SMEM] * 3, VM,
            [
                dma((2,)),
                VM((md, 128), F32), VM((8, nd), F32),
                VM((3, 1, mm), F32), VM((3, 1, mm), F32), VM((3, 1, nn), F32), VM((3, 3, 1, nn), F32),
                VM((8, 128), F32), VM((7, 8, 128), F32), VM((8, 128), F32), VM((7, 8, 128), F32),
                dma((3,)), dma((3,)), dma((3, 3)), dma((3, 3)), dma((7,)), dma((7,)), dma((7,)), dma((7,)),
            ], collective_id=0, has_side_effects=True)
        outs = call(
            write_kernel,
            tuple(jax.ShapeDtypeStruct(s, F32) for s in dims + [(k,) for mn in dims for k in mn]),
            vmem(*first, *second), [VM] * (len(first) + len(second)), HB,
            [VM((8, mg // 8, ng), F32), VM((8, md // 8, nd), F32), dma((8,)), dma((6,))])
        return tuple(outs)

    act_spec = P(None, "row")
    cot_spec = P(None, "col")
    w_spec = P("row", "col")
    r_spec = P("row")
    c_spec = P("col")
    s_spec = P()
    return jax.shard_map(local_program, mesh=mesh, in_specs=(act_spec, act_spec, cot_spec, cot_spec, cot_spec, w_spec, w_spec, w_spec, r_spec, c_spec, r_spec, c_spec, r_spec, c_spec, s_spec, s_spec, s_spec), out_specs=(w_spec, w_spec, w_spec, r_spec, c_spec, r_spec, c_spec, r_spec, c_spec), check_vma=False)
```

```python
import functools

import jax
import jax.numpy as jnp
from jax import lax
from jax.experimental import pallas as pl
from jax.experimental.pallas import tpu as pltpu
from jax.sharding import PartitionSpec as P

EPS_SQ = 1e-30
EPS_SCALE = 1e-3
F32 = jnp.float32
BF16 = jnp.bfloat16
MESH = pl.DeviceIdType.MESH
VM = pltpu.VMEM
HB = pltpu.HBM
KB = 256
NT = 256
WIDE = 2 * NT
HB_ROWS = 512
RING = 5
PIECES = (128, 128)
GRANT = 18
CHUNKS = 4


def fold(v):
    slabs = v.reshape(-1, 8, v.shape[1])
    n = slabs.shape[0] // 4 * 4
    s = jnp.sum(slabs[:n].reshape(-1, 4, 8, v.shape[1]), axis=0)
    s = (s[0] + s[1]) + (s[2] + s[3])
    for i in range(n, slabs.shape[0]):
        s = s + slabs[i]
    return s


def dot_kernel(
    dims,
    x, h, dg, du, dd, wgh, rg, cg, ru, cu, rd, cd,
    held, ht, dt, wg, rs_g, rs_u, cs_g, cs_u, sw, ro, co,
    xs, hs, xt, ring, x_sem, h_sem, d_sem, first_sem, big_sem, s_sem,
):
    m, n = dims[0]
    nk = x.shape[0] // KB
    up = n // NT
    cots, rss, css = (dg, du), (rs_g, rs_u), (cs_g, cs_u)
    n_units = 2 * up
    tiles, unit_tile = [], []
    for q in range(2):
        odd = n % WIDE
        for c0, cols in ([(0, odd)] if odd and not q else []) + [(c, min(WIDE, n - c)) for c in range(0 if q else odd, n, WIDE)]:
            for off in range(0, cols, NT):
                unit_tile.append((len(tiles), off))
            tiles.append((q, c0, cols))

    wide0 = tiles[0][2]

    def x_copy(k):
        return pltpu.make_async_copy(x.at[pl.ds(k * KB, KB), :], xs.at[k], x_sem.at[k])

    def first_copy(k):
        return pltpu.make_async_copy(dg.at[pl.ds(k * KB, KB), pl.ds(0, wide0)], ring.at[0, pl.ds(k * KB, KB), pl.ds(0, wide0)], first_sem.at[k])

    def d_copy(t):
        q, c0, cols = tiles[t]
        return pltpu.make_async_copy(cots[q].at[:, pl.ds(c0, cols)], ring.at[t % RING, :, pl.ds(0, cols)], d_sem.at[t % RING])

    def h_copy(k):
        return pltpu.make_async_copy(h.at[pl.ds(k * HB_ROWS, HB_ROWS), :], hs.at[k % 2], h_sem.at[k % 2])

    bigs = [pltpu.make_async_copy(a, b, big_sem.at[i]) for i, (a, b) in enumerate(((wgh, wg), (dd, dt)))]
    small = [
        pltpu.make_async_copy(src, dst.at[q, 0, pl.ds(0, src.shape[0])], s_sem.at[i])
        for i, (src, dst, q) in enumerate(
            [(rg, ro, 0), (ru, ro, 1), (rd, ro, 2), (cg, co, 0), (cu, co, 1), (cd, co, 2)])
    ]
    for k in range(nk):
        x_copy(k).start()
        first_copy(k).start()

    blocks = ht.shape[0] // 128

    def h_turn(k, part):
        for c in range(part * (blocks // 2), blocks if part else blocks // 2):
            ht[pl.ds(c * 128, 128), pl.ds(k * HB_ROWS, HB_ROWS)] = hs[k % 2, :, pl.ds(c * 128, 128)].T

    def w_square(c):
        w = wg[:, pl.ds(c * 128, 128)]
        s = fold(w * w)
        if c == 0:
            sw[...] = s
        else:
            sw[...] += s

    before = {u: [] for u in range(n_units)}
    beside = [[] for _ in range(n_units)]
    heads = [u for u in range(n_units - 1) if unit_tile[u][0] != unit_tile[u + 1][0]]

    def head(u):
        return max(v for v in heads if v <= u)

    wait_h = (head(7), head(9), head(15), head(17))
    for u, k in zip((head(2), head(2), wait_h[1], head(wait_h[1] + 3)), range(4)):
        before[u].append(h_copy(k).start)
    for u, k in zip(wait_h, range(4)):
        before[u].append(h_copy(k).wait)
        for part in range(2):
            beside[u + part].append(lambda k=k, part=part: h_turn(k, part))
    before[head(13)].append(bigs[0].start)
    before[head(15)].append(bigs[1].start)
    w0 = head(20)
    before[w0].append(bigs[0].wait)
    span = n_units - w0
    for c in range(n // 128):
        beside[w0 + c * span // (n // 128)].append(lambda c=c: w_square(c))

    def run(*accs):
        def acc(z, par, p):
            return accs[(z * 2 + par) * 2 + p]

        def rhs(u, k):
            t, off = unit_tile[u]
            return ring[t % RING, pl.ds(k * KB, KB), pl.ds(off, NT)]

        def drain(u):
            q, j = divmod(u, up)
            cc = None
            for z in range(2):
                for p, size in enumerate(PIECES):
                    r0 = z * sum(PIECES) + sum(PIECES[:p])
                    g = pltpu.matmul_pop(acc(z, u % 2, p))
                    for half in range(2):
                        held[pl.ds((q * (n // 128) + 2 * j + half) * m + r0, size), :] = g[:, half * 128:half * 128 + 128]
                    s = g * g
                    lanes = s[:, :128] + s[:, 128:]
                    if j == 0:
                        rss[q][pl.ds(r0, size), :] = lanes
                    else:
                        rss[q][pl.ds(r0, size), :] += lanes
                    s = fold(s)
                    cc = s if cc is None else cc + s
            css[q][:, pl.ds(j * NT, NT)] = cc

        for z in range(2):
            for par in range(2):
                for p in range(2):
                    pltpu.matmul_pop(acc(z, par, p))

        for u in range(n_units):
            last = u == n_units - 1
            t = unit_tile[u][0]
            if not last and unit_tile[u + 1][0] != t:
                if u:
                    d_copy(t + 1).wait()
                if t and t - 1 + RING < len(tiles):
                    d_copy(t - 1 + RING).start()
                for f in before.pop(u):
                    f()
            for k in range(nk):
                if u == 0:
                    x_copy(k).wait()
                    first_copy(k).wait()
                    for z in range(2):
                        xt[pl.ds(z * 256, 256), pl.ds(k * KB, KB)] = xs[k, :, pl.ds(z * 256, 256)].T
                        pltpu.matmul_push_rhs(rhs(0, k), staging_register=k % 2, mxu_index=z)
                    if k % 2 == 0 and k // 2 + 1 < RING:
                        d_copy(k // 2 + 1).start()
                    if k == nk - 1 and unit_tile[1][0] == 1:
                        d_copy(1).wait()
                for z in range(2):
                    for p, size in enumerate(PIECES):
                        r0 = z * sum(PIECES) + sum(PIECES[:p])
                        pltpu.matmul_acc_lhs(acc(z, u % 2, p), xt[pl.ds(r0, size), pl.ds(k * KB, KB)],
                                             load_staged_rhs=(k % 2 if p == 0 else None))
                    if k < nk - 1:
                        if u:
                            pltpu.matmul_push_rhs(rhs(u, k + 1), staging_register=(k + 1) % 2, mxu_index=z)
                    elif not last:
                        pltpu.matmul_push_rhs(rhs(u + 1, 0), staging_register=0, mxu_index=z)
                if k == 1 and u:
                    drain(u - 1)
                if k == 2:
                    for f in beside[u]:
                        f()
        drain(n_units - 1)
        assert not any(before.values())

    for c in small:
        c.start()
    pl.run_scoped(run, *[pltpu.ACC(z)((size, NT), F32) for z in range(2) for par in range(2) for size in PIECES])
    for c in bigs[1:] + small:
        c.wait()


def exchange_kernel(
    dims,
    held, ht, dt, wg, rs_g, rs_u, cs_g, cs_u, sw_g, ro, co,
    wuh, wdh,
    b2, rel, clip,
    late, wu, wd, a_g, a_u, a_d, b_g, b_u, b_d, r_g, c_g, r_u, c_u, r_d, c_d,
    w_sem, rs_d, cs_d, rsend, rrecv, csend, crecv, pay, got, pay2, got2, r1s, r1r, c1s, c1r, p_s, p_r, p2_s, p2_r,
):
    col = lax.axis_index("col")
    row = lax.axis_index("row")
    row_peer = (row + 1 - 2 * (row % 2), (row + 2) % 4, 3 - row)
    mats = (
        dict(rs=rs_g, cs=cs_g, a=a_g, b=b_g, r=r_g, c=c_g),
        dict(rs=rs_u, cs=cs_u, a=a_u, b=b_u, r=r_u, c=c_u),
        dict(rs=rs_d, cs=cs_d, a=a_d, b=b_d, r=r_d, c=c_d),
    )
    for mat, (m, n) in zip(mats, dims):
        mat["m"], mat["n"] = m, n
        mat["mt"], mat["nt"] = m * 4, n * 2
    (mg, ng), (md, nd) = dims[0], dims[2]
    size = mg * ng // 128

    barrier = pltpu.get_barrier_semaphore()
    plane = [{"row": p, "col": cc} for cc in (col, 1 - col) for p in (row,) + row_peer][1:]
    for dev in plane:
        pl.semaphore_signal(barrier, inc=1, device_id=dev, device_id_type=MESH)

    loads = [pltpu.make_async_copy(a, b, w_sem.at[i]) for i, (a, b) in enumerate(((wuh, wu), (wdh, wd)))]
    for c in loads:
        c.start()
    pay[...] = jnp.zeros_like(pay)
    pay2[...] = jnp.zeros_like(pay2)

    def w_square(q, w, rows):
        m, n = dims[q]

        def chunk(r, sums):
            rr = pl.ds(pl.multiple_of(r * rows, 8), rows)
            new = []
            for c in range(n // 128):
                v = w[rr, c * 128:(c + 1) * 128]
                new.append(sums[c] + fold(v * v))
            return tuple(new)

        sums = lax.fori_loop(0, m // rows, chunk, (jnp.zeros((8, 128), F32),) * (n // 128))
        total = sums[0]
        for v in sums[1:]:
            total = total + v
        pay[pl.ds(q, 1), :] = jnp.sum(total, axis=0, keepdims=True)

    def first_sends(q):
        mat = mats[q]
        m, n = mat["m"], mat["n"]
        copies = [pltpu.make_async_remote_copy(
            rsend.at[q, :, pl.ds(0, m)], rrecv.at[q, :, pl.ds(0, m)], r1s.at[q], r1r.at[q],
            device_id={"col": 1 - col}, device_id_type=MESH)]
        for d in range(3):
            copies.append(pltpu.make_async_remote_copy(
                csend.at[q, :, pl.ds(0, n)], crecv.at[q, d, :, pl.ds(0, n)], c1s.at[q, d], c1r.at[q, d],
                device_id={"row": row_peer[d]}, device_id_type=MESH))
        return copies

    def first_reduce(q):
        mat = mats[q]
        csend[q, :, pl.ds(0, mat["n"])] = jnp.sum(mat["cs"][...], axis=0, keepdims=True)
        for b in range(mat["m"] // 128):
            t = mat["rs"][pl.ds(b * 128, 128), :].T
            rsend[q, :, pl.ds(b * 128, 128)] = jnp.sum(t, axis=0, keepdims=True)

    def new_stats(q):
        mat = mats[q]
        m, n = mat["m"], mat["n"]
        beta = b2[0, 0]
        rsum = rsend[q, :, pl.ds(0, m)] + rrecv[q, :, pl.ds(0, m)]
        r_new = beta * ro[q, :, pl.ds(0, m)] + (1.0 - beta) * (rsum * (1.0 / mat["nt"]) + EPS_SQ)
        mat["r"][...] = r_new
        csum = (csend[q, :, pl.ds(0, n)] + crecv[q, 0, :, pl.ds(0, n)]) + (
            crecv[q, 1, :, pl.ds(0, n)] + crecv[q, 2, :, pl.ds(0, n)])
        c_new = beta * co[q, :, pl.ds(0, n)] + (1.0 - beta) * (csum * (1.0 / mat["mt"]) + EPS_SQ)
        mat["c"][...] = c_new
        mat["b"][...] = lax.rsqrt(c_new)
        alpha = lax.rsqrt(r_new)
        rp = r_new[:, :128]
        for b in range(m // 128):
            blk = jnp.broadcast_to(alpha[:, b * 128:(b + 1) * 128], (128, 128))
            mat["a"][pl.ds(b * 128, 128), :] = blk.T
            if b:
                rp = rp + r_new[:, b * 128:(b + 1) * 128]
        if q == 2:
            pay2[pl.ds(3, 1), :] = rp
        else:
            pay[pl.ds(3 + q, 1), :] = rp

    def u_square(q, rows):
        mat = mats[q]
        m, n = mat["m"], mat["n"]
        src, first = (late, 0) if q == 2 else (held, q * size)
        blocks = n // 128

        def chunk(r, sums):
            r0 = pl.multiple_of(r * rows, 8)
            a = mat["a"][pl.ds(r0, rows), :]
            new = []
            for c in range(blocks):
                t = src[pl.ds(pl.multiple_of(first + c * m + r0, 8), rows), :] * a
                new.append(sums[c] + fold(t * t))
            return tuple(new)

        sums = lax.fori_loop(0, m // rows, chunk, (jnp.zeros((8, 128), F32),) * blocks)
        total = None
        for c in range(blocks):
            bb = mat["b"][:, c * 128:(c + 1) * 128]
            s = sums[c] * (bb * bb)
            total = s if total is None else total + s
        pay2[pl.ds(q, 1), :] = jnp.sum(total, axis=0, keepdims=True)

    rows = md // CHUNKS
    steps = nd // NT * CHUNKS

    def product(i):
        j, c = divmod(i, CHUNKS)
        rr = pl.ds(c * rows, rows)
        g = jnp.dot(ht[rr, :], dt[:, pl.ds(j * NT, NT)], preferred_element_type=F32)
        for half in range(2):
            late[pl.ds((2 * j + half) * md + c * rows, rows), :] = g[:, half * 128:half * 128 + 128]
        s = g * g
        lanes = s[:, :128] + s[:, 128:]
        if j == 0:
            rs_d[rr, :] = lanes
        else:
            rs_d[rr, :] += lanes
        cc = pl.ds(j * NT, NT)
        if c == 0:
            cs_d[:, cc] = fold(s)
        else:
            cs_d[:, cc] += fold(s)

    def plane_sends(src, dst, rows, s_sem, r_sem):
        rr = pl.ds(0, rows)
        return [pltpu.make_async_remote_copy(src.at[rr], dst.at[i, rr], s_sem.at[i], r_sem.at[i], device_id=dev, device_id_type=MESH)
                for i, dev in enumerate(plane)]

    def plane_sum(src, dst, rows):
        a = [src[pl.ds(0, rows), :]] + [dst[i, pl.ds(0, rows), :] for i in range(len(plane))]
        total = ((a[0] + a[1]) + (a[2] + a[3])) + ((a[4] + a[5]) + (a[6] + a[7]))
        return jnp.sum(total, axis=1, keepdims=True)

    early = [c for q in range(2) for c in first_sends(q)]
    for i in range(steps):
        if i == CHUNKS:
            first_reduce(0)
            first_reduce(1)
            pl.semaphore_wait(barrier, len(plane))
            for c in early:
                c.start()
        product(i)
    first_reduce(2)
    sends = first_sends(2)
    for c in sends:
        c.start()
    for c in early:
        c.wait()
    pay[pl.ds(0, 1), :] = jnp.sum(sw_g[...], axis=0, keepdims=True)
    for q in range(2):
        new_stats(q)
    for c in loads:
        c.wait()
    w_square(1, wu, 64)
    w_square(2, wd, md // 8)
    sums = plane_sends(pay, got, 5, p_s, p_r)
    for c in sums:
        c.start()
    for q in range(2):
        u_square(q, 64)
    for c in sends:
        c.wait()
    new_stats(2)
    u_square(2, md // 8)
    sums2 = plane_sends(pay2, got2, 4, p2_s, p2_r)
    for c in sums2:
        c.start()
    for c in sums + sums2:
        c.wait()
    norms = plane_sum(pay, got, 5)
    shapes = plane_sum(pay2, got2, 4)
    for q, mat in enumerate(mats):
        count = float(mat["mt"] * mat["nt"])
        r_sum = shapes[3:4] if q == 2 else norms[3 + q:4 + q]
        r_mean = r_sum * (0.5 / mat["mt"])
        u_rms = jnp.sqrt(r_mean * shapes[q:q + 1] / count)
        w_rms = jnp.sqrt(norms[q:q + 1] / count)
        step = rel[0, 0] * jnp.maximum(EPS_SCALE, w_rms)
        k = step * jnp.sqrt(r_mean) / jnp.maximum(1.0, u_rms / clip[0, 0])
        mat["b"][...] = mat["b"][...] * k


def write_kernel(
    dims,
    held, ht, dt, w_g, rs_g, rs_u, cs_g, cs_u, sw_g, ro, co,
    late, w_u, w_d, a_g, a_u, a_d, b_g, b_u, b_d, r_g, c_g, r_u, c_u, r_d, c_d,
    o_g, o_u, o_d, or_g, oc_g, or_u, oc_u, or_d, oc_d,
    wide, tall, o_sem, s_sem,
):
    small = [pltpu.make_async_copy(s.at[0], d, s_sem.at[i]) for i, (s, d) in enumerate(
        [(r_g, or_g), (c_g, oc_g), (r_u, or_u), (c_u, oc_u), (r_d, or_d), (c_d, oc_d)])]
    for c in small:
        c.start()
    slots = 8
    size = dims[0][0] * dims[0][1] // 128
    where = ((held, 0, w_g), (held, 1, w_u), (late, 0, w_d))
    pending = {}
    step = 0
    for q, a, b, o, buf in ((2, a_d, b_d, o_d, tall), (1, a_u, b_u, o_u, wide), (0, a_g, b_g, o_g, wide)):
        rows = buf.shape[1]
        src, k, w = where[q]
        for t in range(dims[q][0] // rows):
            slot = step % slots
            if slot in pending:
                pending.pop(slot).wait()
            rr = pl.ds(t * rows, rows)
            scale = a[rr, :]
            for c in range(dims[q][1] // 128):
                cc = pl.ds(c * 128, 128)
                off = c * dims[q][0] + t * rows
                g = src[pl.ds(k * size + off, rows), :]
                buf[slot, :, cc] = w[rr, cc] - (g * scale) * b[:, cc]
            cp = pltpu.make_async_copy(buf.at[slot], o.at[rr, :], o_sem.at[slot])
            cp.start()
            pending[slot] = cp
            step += 1
    for cp in pending.values():
        cp.wait()
    for c in small:
        c.wait()


def solution(mesh):
    def local_program(x_in, h_act, d_gate, d_up, d_out, w_gate, w_up, w_down, r_gate, c_gate, r_up, c_up, r_down, c_down, beta_two, rel_step, clip_thr):
        (mg, ng), (md, nd) = w_gate.shape, w_down.shape
        tokens = x_in.shape[0]
        nk = tokens // KB
        def hbm(*arrays):
            return tuple(pltpu.with_memory_space_constraint(v, HB) for v in arrays)

        def vmem(*arrays):
            return tuple(pltpu.with_memory_space_constraint(v, VM) for v in arrays)

        one = tuple(v.reshape(1, 1) for v in (beta_two, rel_step, clip_thr))
        dims = [(mg, ng), (mg, ng), (md, nd)]
        mm, nn = max(mg, md), max(ng, nd)
        dma = pltpu.SemaphoreType.DMA

        def call(kernel, outs, args, in_spaces, out_space, scratch, **params):
            return pl.pallas_call(
                functools.partial(kernel, dims),
                out_shape=outs,
                in_specs=[pl.BlockSpec(memory_space=v) for v in in_spaces],
                out_specs=tuple(pl.BlockSpec(memory_space=out_space) for _ in outs),
                scratch_shapes=scratch,
                compiler_params=pltpu.CompilerParams(vmem_limit_bytes=GRANT * 2**20, **params),
                name=kernel.__name__,
            )(*args)

        def vm(shapes):
            return tuple(VM(s, F32) for s in shapes)

        def vm(shapes):
            return tuple(VM(s, F32) for s in shapes)

        size = mg * ng // 128
        lanes = [(m, 128) for m, _ in dims]
        stats = [s for m, n in dims for s in ((1, m), (1, n))]
        first = call(
            dot_kernel,
            vm([(2 * size, 128)]) + (VM((md, tokens), BF16), VM((tokens, nd), BF16))
            + vm(dims[:1] + lanes[:2] + [(8, ng), (8, ng), (8, 128), (3, 1, mm), (3, 1, nn)]),
            hbm(x_in, h_act, d_gate, d_up, d_out, w_gate, r_gate, c_gate, r_up, c_up, r_down, c_down), [HB] * 12, VM,
            [
                VM((nk, KB, mg), BF16), VM((2, HB_ROWS, md), BF16), VM((mg, tokens), BF16), VM((RING, tokens, WIDE), BF16),
                dma((nk,)), dma((2,)), dma((RING,)), dma((nk,)), dma((2,)), dma((6,)),
            ])
        second = call(
            exchange_kernel,
            vm([(size, 128)] + dims[1:] + lanes + [(1, n) for _, n in dims] + stats),
            vmem(*first) + hbm(w_up, w_down) + one, [VM] * len(first) + [HB] * 2 + [pltpu.SMEM] * 3, VM,
            [
                dma((2,)),
                VM((md, 128), F32), VM((8, nd), F32),
                VM((3, 1, mm), F32), VM((3, 1, mm), F32), VM((3, 1, nn), F32), VM((3, 3, 1, nn), F32),
                VM((8, 128), F32), VM((7, 8, 128), F32), VM((8, 128), F32), VM((7, 8, 128), F32),
                dma((3,)), dma((3,)), dma((3, 3)), dma((3, 3)), dma((7,)), dma((7,)), dma((7,)), dma((7,)),
            ], collective_id=0, has_side_effects=True)
        outs = call(
            write_kernel,
            tuple(jax.ShapeDtypeStruct(s, F32) for s in dims + [(k,) for mn in dims for k in mn]),
            vmem(*first, *second), [VM] * (len(first) + len(second)), HB,
            [VM((8, mg // 8, ng), F32), VM((8, md // 8, nd), F32), dma((8,)), dma((6,))])
        return tuple(outs)

    act_spec = P(None, "row")
    cot_spec = P(None, "col")
    w_spec = P("row", "col")
    r_spec = P("row")
    c_spec = P("col")
    s_spec = P()
    return jax.shard_map(local_program, mesh=mesh, in_specs=(act_spec, act_spec, cot_spec, cot_spec, cot_spec, w_spec, w_spec, w_spec, r_spec, c_spec, r_spec, c_spec, r_spec, c_spec, s_spec, s_spec, s_spec), out_specs=(w_spec, w_spec, w_spec, r_spec, c_spec, r_spec, c_spec, r_spec, c_spec), check_vma=False)
```

```python
import functools

import jax
import jax.numpy as jnp
from jax import lax
from jax.experimental import pallas as pl
from jax.experimental.pallas import tpu as pltpu
from jax.sharding import PartitionSpec as P

EPS_SQ = 1e-30
EPS_SCALE = 1e-3
F32 = jnp.float32
BF16 = jnp.bfloat16
MESH = pl.DeviceIdType.MESH
VM = pltpu.VMEM
HB = pltpu.HBM
KB = 256
NT = 256
WIDE = 2 * NT
HB_ROWS = 512
RING = 5
PIECES = (128, 128)
GRANT = 18
CHUNKS = 4


def fold(v):
    slabs = v.reshape(-1, 8, v.shape[1])
    n = slabs.shape[0] // 4 * 4
    s = jnp.sum(slabs[:n].reshape(-1, 4, 8, v.shape[1]), axis=0)
    s = (s[0] + s[1]) + (s[2] + s[3])
    for i in range(n, slabs.shape[0]):
        s = s + slabs[i]
    return s


def dot_kernel(
    dims,
    x, h, dg, du, dd, wgh, rg, cg, ru, cu, rd, cd,
    held, ht, dt, wg, rs_g, rs_u, cs_g, cs_u, sw, ro, co,
    xs, hs, xt, ring, x_sem, h_sem, d_sem, first_sem, big_sem, s_sem,
):
    m, n = dims[0]
    nk = x.shape[0] // KB
    up = n // NT
    cots, rss, css = (dg, du), (rs_g, rs_u), (cs_g, cs_u)
    n_units = 2 * up
    tiles, unit_tile = [], []
    for q in range(2):
        odd = n % WIDE
        for c0, cols in ([(0, odd)] if odd and not q else []) + [(c, min(WIDE, n - c)) for c in range(0 if q else odd, n, WIDE)]:
            for off in range(0, cols, NT):
                unit_tile.append((len(tiles), off))
            tiles.append((q, c0, cols))

    wide0 = tiles[0][2]

    def x_copy(k):
        return pltpu.make_async_copy(x.at[pl.ds(k * KB, KB), :], xs.at[k], x_sem.at[k])

    def first_copy(k):
        return pltpu.make_async_copy(dg.at[pl.ds(k * KB, KB), pl.ds(0, wide0)], ring.at[0, pl.ds(k * KB, KB), pl.ds(0, wide0)], first_sem.at[k])

    def d_copy(t):
        q, c0, cols = tiles[t]
        return pltpu.make_async_copy(cots[q].at[:, pl.ds(c0, cols)], ring.at[t % RING, :, pl.ds(0, cols)], d_sem.at[t % RING])

    def h_copy(k):
        return pltpu.make_async_copy(h.at[pl.ds(k * HB_ROWS, HB_ROWS), :], hs.at[k % 2], h_sem.at[k % 2])

    bigs = [pltpu.make_async_copy(a, b, big_sem.at[i]) for i, (a, b) in enumerate(((wgh, wg), (dd, dt)))]
    small = [
        pltpu.make_async_copy(src, dst.at[q, 0, pl.ds(0, src.shape[0])], s_sem.at[i])
        for i, (src, dst, q) in enumerate(
            [(rg, ro, 0), (ru, ro, 1), (rd, ro, 2), (cg, co, 0), (cu, co, 1), (cd, co, 2)])
    ]
    for k in range(nk):
        x_copy(k).start()
        first_copy(k).start()

    blocks = ht.shape[0] // 128

    def h_turn(k, part):
        for c in range(part * (blocks // 2), blocks if part else blocks // 2):
            ht[pl.ds(c * 128, 128), pl.ds(k * HB_ROWS, HB_ROWS)] = hs[k % 2, :, pl.ds(c * 128, 128)].T

    def w_square(c):
        w = wg[:, pl.ds(c * 128, 128)]
        s = fold(w * w)
        if c == 0:
            sw[...] = s
        else:
            sw[...] += s

    before = {u: [] for u in range(n_units)}
    beside = [[] for _ in range(n_units)]
    heads = [u for u in range(n_units - 1) if unit_tile[u][0] != unit_tile[u + 1][0]]

    def head(u):
        return max(v for v in heads if v <= u)

    wait_h = (head(7), head(9), head(15), head(17))
    for u, k in zip((head(2), head(2), wait_h[1], head(wait_h[1] + 3)), range(4)):
        before[u].append(h_copy(k).start)
    for u, k in zip(wait_h, range(4)):
        before[u].append(h_copy(k).wait)
        for part in range(2):
            beside[u + part].append(lambda k=k, part=part: h_turn(k, part))
    before[head(13)].append(bigs[0].start)
    before[head(15)].append(bigs[1].start)
    w0 = head(20)
    before[w0].append(bigs[0].wait)
    span = n_units - w0
    for c in range(n // 128):
        beside[w0 + c * span // (n // 128)].append(lambda c=c: w_square(c))

    def run(*accs):
        def acc(z, par, p):
            return accs[(z * 2 + par) * 2 + p]

        def rhs(u, k):
            t, off = unit_tile[u]
            return ring[t % RING, pl.ds(k * KB, KB), pl.ds(off, NT)]

        def drain(u):
            q, j = divmod(u, up)
            cc = None
            for z in range(2):
                for p, size in enumerate(PIECES):
                    r0 = z * sum(PIECES) + sum(PIECES[:p])
                    g = pltpu.matmul_pop(acc(z, u % 2, p))
                    for half in range(2):
                        held[pl.ds((q * (n // 128) + 2 * j + half) * m + r0, size), :] = g[:, half * 128:half * 128 + 128]
                    s = g * g
                    lanes = s[:, :128] + s[:, 128:]
                    if j == 0:
                        rss[q][pl.ds(r0, size), :] = lanes
                    else:
                        rss[q][pl.ds(r0, size), :] += lanes
                    s = fold(s)
                    cc = s if cc is None else cc + s
            css[q][:, pl.ds(j * NT, NT)] = cc

        for z in range(2):
            for par in range(2):
                for p in range(2):
                    pltpu.matmul_pop(acc(z, par, p))

        for u in range(n_units):
            last = u == n_units - 1
            t = unit_tile[u][0]
            if not last and unit_tile[u + 1][0] != t:
                if u:
                    d_copy(t + 1).wait()
                if t and t - 1 + RING < len(tiles):
                    d_copy(t - 1 + RING).start()
                for f in before.pop(u):
                    f()
            for k in range(nk):
                if u == 0:
                    x_copy(k).wait()
                    first_copy(k).wait()
                    for z in range(2):
                        xt[pl.ds(z * 256, 256), pl.ds(k * KB, KB)] = xs[k, :, pl.ds(z * 256, 256)].T
                        pltpu.matmul_push_rhs(rhs(0, k), staging_register=k % 2, mxu_index=z)
                    if k % 2 == 0 and k // 2 + 1 < RING:
                        d_copy(k // 2 + 1).start()
                    if k == nk - 1 and unit_tile[1][0] == 1:
                        d_copy(1).wait()
                for z in range(2):
                    for p, size in enumerate(PIECES):
                        r0 = z * sum(PIECES) + sum(PIECES[:p])
                        pltpu.matmul_acc_lhs(acc(z, u % 2, p), xt[pl.ds(r0, size), pl.ds(k * KB, KB)],
                                             load_staged_rhs=(k % 2 if p == 0 else None))
                    if k < nk - 1:
                        if u:
                            pltpu.matmul_push_rhs(rhs(u, k + 1), staging_register=(k + 1) % 2, mxu_index=z)
                    elif not last:
                        pltpu.matmul_push_rhs(rhs(u + 1, 0), staging_register=0, mxu_index=z)
                if k == 1 and u:
                    drain(u - 1)
                if k == 2:
                    for f in beside[u]:
                        f()
        drain(n_units - 1)
        assert not any(before.values())

    for c in small:
        c.start()
    pl.run_scoped(run, *[pltpu.ACC(z)((size, NT), F32) for z in range(2) for par in range(2) for size in PIECES])
    for c in bigs[1:] + small:
        c.wait()


def exchange_kernel(
    dims,
    held, ht, dt, wg, rs_g, rs_u, cs_g, cs_u, sw_g, ro, co,
    wuh, wdh,
    b2, rel, clip,
    late, wu, wd, a_g, a_u, a_d, b_g, b_u, b_d, r_g, c_g, r_u, c_u, r_d, c_d,
    w_sem, rs_d, cs_d, rsend, rrecv, csend, crecv, pay, got, pay2, got2, r1s, r1r, c1s, c1r, p_s, p_r, p2_s, p2_r,
):
    col = lax.axis_index("col")
    row = lax.axis_index("row")
    row_peer = (row + 1 - 2 * (row % 2), (row + 2) % 4, 3 - row)
    mats = (
        dict(rs=rs_g, cs=cs_g, a=a_g, b=b_g, r=r_g, c=c_g),
        dict(rs=rs_u, cs=cs_u, a=a_u, b=b_u, r=r_u, c=c_u),
        dict(rs=rs_d, cs=cs_d, a=a_d, b=b_d, r=r_d, c=c_d),
    )
    for mat, (m, n) in zip(mats, dims):
        mat["m"], mat["n"] = m, n
        mat["mt"], mat["nt"] = m * 4, n * 2
    (mg, ng), (md, nd) = dims[0], dims[2]
    size = mg * ng // 128

    barrier = pltpu.get_barrier_semaphore()
    plane = [{"row": p, "col": cc} for cc in (col, 1 - col) for p in (row,) + row_peer][1:]
    for dev in plane:
        pl.semaphore_signal(barrier, inc=1, device_id=dev, device_id_type=MESH)

    loads = [pltpu.make_async_copy(a, b, w_sem.at[i]) for i, (a, b) in enumerate(((wuh, wu), (wdh, wd)))]
    for c in loads:
        c.start()
    pay[...] = jnp.zeros_like(pay)
    pay2[...] = jnp.zeros_like(pay2)

    def w_square(q, w, rows):
        m, n = dims[q]

        def chunk(r, sums):
            rr = pl.ds(pl.multiple_of(r * rows, 8), rows)
            new = []
            for c in range(n // 128):
                v = w[rr, c * 128:(c + 1) * 128]
                new.append(sums[c] + fold(v * v))
            return tuple(new)

        sums = lax.fori_loop(0, m // rows, chunk, (jnp.zeros((8, 128), F32),) * (n // 128))
        total = sums[0]
        for v in sums[1:]:
            total = total + v
        pay[pl.ds(q, 1), :] = jnp.sum(total, axis=0, keepdims=True)

    def first_sends(q):
        mat = mats[q]
        m, n = mat["m"], mat["n"]
        copies = [pltpu.make_async_remote_copy(
            rsend.at[q, :, pl.ds(0, m)], rrecv.at[q, :, pl.ds(0, m)], r1s.at[q], r1r.at[q],
            device_id={"col": 1 - col}, device_id_type=MESH)]
        for d in range(3):
            copies.append(pltpu.make_async_remote_copy(
                csend.at[q, :, pl.ds(0, n)], crecv.at[q, d, :, pl.ds(0, n)], c1s.at[q, d], c1r.at[q, d],
                device_id={"row": row_peer[d]}, device_id_type=MESH))
        return copies

    def first_reduce(q):
        mat = mats[q]
        for b in range(mat["m"] // 128):
            t = mat["rs"][pl.ds(b * 128, 128), :].T
            rsend[q, :, pl.ds(b * 128, 128)] = jnp.sum(t, axis=0, keepdims=True)
        csend[q, :, pl.ds(0, mat["n"])] = jnp.sum(mat["cs"][...], axis=0, keepdims=True)

    def new_rows(q):
        mat = mats[q]
        m = mat["m"]
        beta = b2[0, 0]
        rsum = rsend[q, :, pl.ds(0, m)] + rrecv[q, :, pl.ds(0, m)]
        r_new = beta * ro[q, :, pl.ds(0, m)] + (1.0 - beta) * (rsum * (1.0 / mat["nt"]) + EPS_SQ)
        mat["r"][...] = r_new
        alpha = lax.rsqrt(r_new)
        rp = r_new[:, :128]
        for b in range(m // 128):
            blk = jnp.broadcast_to(alpha[:, b * 128:(b + 1) * 128], (128, 128))
            mat["a"][pl.ds(b * 128, 128), :] = blk.T
            if b:
                rp = rp + r_new[:, b * 128:(b + 1) * 128]
        if q == 2:
            pay2[pl.ds(3, 1), :] = rp
        else:
            pay[pl.ds(3 + q, 1), :] = rp

    def new_cols(q):
        mat = mats[q]
        n = mat["n"]
        beta = b2[0, 0]
        csum = (csend[q, :, pl.ds(0, n)] + crecv[q, 0, :, pl.ds(0, n)]) + (
            crecv[q, 1, :, pl.ds(0, n)] + crecv[q, 2, :, pl.ds(0, n)])
        c_new = beta * co[q, :, pl.ds(0, n)] + (1.0 - beta) * (csum * (1.0 / mat["mt"]) + EPS_SQ)
        mat["c"][...] = c_new
        mat["b"][...] = lax.rsqrt(c_new)

    def u_square(q, rows, waits=()):
        mat = mats[q]
        m, n = mat["m"], mat["n"]
        src, first = (late, 0) if q == 2 else (held, q * size)
        blocks = n // 128

        def chunk(r, sums):
            r0 = pl.multiple_of(r * rows, 8)
            a = mat["a"][pl.ds(r0, rows), :]
            new = []
            for c in range(blocks):
                t = src[pl.ds(pl.multiple_of(first + c * m + r0, 8), rows), :] * a
                new.append(sums[c] + fold(t * t))
            return tuple(new)

        sums = lax.fori_loop(0, m // rows, chunk, (jnp.zeros((8, 128), F32),) * blocks)
        for c in waits:
            c.wait()
        new_cols(q)
        total = None
        for c in range(blocks):
            bb = mat["b"][:, c * 128:(c + 1) * 128]
            s = sums[c] * (bb * bb)
            total = s if total is None else total + s
        pay2[pl.ds(q, 1), :] = jnp.sum(total, axis=0, keepdims=True)

    rows = md // CHUNKS
    steps = nd // NT * CHUNKS

    def product(i):
        j, c = divmod(i, CHUNKS)
        rr = pl.ds(c * rows, rows)
        g = jnp.dot(ht[rr, :], dt[:, pl.ds(j * NT, NT)], preferred_element_type=F32)
        for half in range(2):
            late[pl.ds((2 * j + half) * md + c * rows, rows), :] = g[:, half * 128:half * 128 + 128]
        s = g * g
        lanes = s[:, :128] + s[:, 128:]
        if j == 0:
            rs_d[rr, :] = lanes
        else:
            rs_d[rr, :] += lanes
        cc = pl.ds(j * NT, NT)
        if c == 0:
            cs_d[:, cc] = fold(s)
        else:
            cs_d[:, cc] += fold(s)

    def plane_sends(src, dst, rows, s_sem, r_sem):
        rr = pl.ds(0, rows)
        return [pltpu.make_async_remote_copy(src.at[rr], dst.at[i, rr], s_sem.at[i], r_sem.at[i], device_id=dev, device_id_type=MESH)
                for i, dev in enumerate(plane)]

    def plane_sum(src, dst, rows):
        a = [src[pl.ds(0, rows), :]] + [dst[i, pl.ds(0, rows), :] for i in range(len(plane))]
        total = ((a[0] + a[1]) + (a[2] + a[3])) + ((a[4] + a[5]) + (a[6] + a[7]))
        return jnp.sum(total, axis=1, keepdims=True)

    early = [c for q in range(2) for c in first_sends(q)]
    for i in range(steps):
        if i == CHUNKS:
            first_reduce(0)
            first_reduce(1)
            pl.semaphore_wait(barrier, len(plane))
            for c in early:
                c.start()
        product(i)
    first_reduce(2)
    sends = first_sends(2)
    for c in sends:
        c.start()
    for c in early:
        c.wait()
    pay[pl.ds(0, 1), :] = jnp.sum(sw_g[...], axis=0, keepdims=True)
    for q in range(2):
        new_rows(q)
    for c in loads:
        c.wait()
    w_square(1, wu, 64)
    w_square(2, wd, md // 8)
    sums = plane_sends(pay, got, 5, p_s, p_r)
    for c in sums:
        c.start()
    for q in range(2):
        u_square(q, 64)
    sends[0].wait()
    new_rows(2)
    u_square(2, md // 8, sends[1:])
    sums2 = plane_sends(pay2, got2, 4, p2_s, p2_r)
    for c in sums2:
        c.start()
    for c in sums + sums2:
        c.wait()
    norms = plane_sum(pay, got, 5)
    shapes = plane_sum(pay2, got2, 4)
    for q, mat in enumerate(mats):
        count = float(mat["mt"] * mat["nt"])
        r_sum = shapes[3:4] if q == 2 else norms[3 + q:4 + q]
        r_mean = r_sum * (0.5 / mat["mt"])
        u_rms = jnp.sqrt(r_mean * shapes[q:q + 1] / count)
        w_rms = jnp.sqrt(norms[q:q + 1] / count)
        step = rel[0, 0] * jnp.maximum(EPS_SCALE, w_rms)
        k = step * jnp.sqrt(r_mean) / jnp.maximum(1.0, u_rms / clip[0, 0])
        mat["b"][...] = mat["b"][...] * k


def write_kernel(
    dims,
    held, ht, dt, w_g, rs_g, rs_u, cs_g, cs_u, sw_g, ro, co,
    late, w_u, w_d, a_g, a_u, a_d, b_g, b_u, b_d, r_g, c_g, r_u, c_u, r_d, c_d,
    o_g, o_u, o_d, or_g, oc_g, or_u, oc_u, or_d, oc_d,
    wide, tall, o_sem, s_sem,
):
    small = [pltpu.make_async_copy(s.at[0], d, s_sem.at[i]) for i, (s, d) in enumerate(
        [(r_g, or_g), (c_g, oc_g), (r_u, or_u), (c_u, oc_u), (r_d, or_d), (c_d, oc_d)])]
    for c in small:
        c.start()
    slots = 8
    size = dims[0][0] * dims[0][1] // 128
    where = ((held, 0, w_g), (held, 1, w_u), (late, 0, w_d))
    pending = {}
    step = 0
    for q, a, b, o, buf in ((2, a_d, b_d, o_d, tall), (1, a_u, b_u, o_u, wide), (0, a_g, b_g, o_g, wide)):
        rows = buf.shape[1]
        src, k, w = where[q]
        for t in range(dims[q][0] // rows):
            slot = step % slots
            if slot in pending:
                pending.pop(slot).wait()
            rr = pl.ds(t * rows, rows)
            scale = a[rr, :]
            for c in range(dims[q][1] // 128):
                cc = pl.ds(c * 128, 128)
                off = c * dims[q][0] + t * rows
                g = src[pl.ds(k * size + off, rows), :]
                buf[slot, :, cc] = w[rr, cc] - (g * scale) * b[:, cc]
            cp = pltpu.make_async_copy(buf.at[slot], o.at[rr, :], o_sem.at[slot])
            cp.start()
            pending[slot] = cp
            step += 1
    for cp in pending.values():
        cp.wait()
    for c in small:
        c.wait()


def solution(mesh):
    def local_program(x_in, h_act, d_gate, d_up, d_out, w_gate, w_up, w_down, r_gate, c_gate, r_up, c_up, r_down, c_down, beta_two, rel_step, clip_thr):
        (mg, ng), (md, nd) = w_gate.shape, w_down.shape
        tokens = x_in.shape[0]
        nk = tokens // KB
        def hbm(*arrays):
            return tuple(pltpu.with_memory_space_constraint(v, HB) for v in arrays)

        def vmem(*arrays):
            return tuple(pltpu.with_memory_space_constraint(v, VM) for v in arrays)

        one = tuple(v.reshape(1, 1) for v in (beta_two, rel_step, clip_thr))
        dims = [(mg, ng), (mg, ng), (md, nd)]
        mm, nn = max(mg, md), max(ng, nd)
        dma = pltpu.SemaphoreType.DMA

        def call(kernel, outs, args, in_spaces, out_space, scratch, **params):
            return pl.pallas_call(
                functools.partial(kernel, dims),
                out_shape=outs,
                in_specs=[pl.BlockSpec(memory_space=v) for v in in_spaces],
                out_specs=tuple(pl.BlockSpec(memory_space=out_space) for _ in outs),
                scratch_shapes=scratch,
                compiler_params=pltpu.CompilerParams(vmem_limit_bytes=GRANT * 2**20, **params),
                name=kernel.__name__,
            )(*args)

        def vm(shapes):
            return tuple(VM(s, F32) for s in shapes)

        def vm(shapes):
            return tuple(VM(s, F32) for s in shapes)

        size = mg * ng // 128
        lanes = [(m, 128) for m, _ in dims]
        stats = [s for m, n in dims for s in ((1, m), (1, n))]
        first = call(
            dot_kernel,
            vm([(2 * size, 128)]) + (VM((md, tokens), BF16), VM((tokens, nd), BF16))
            + vm(dims[:1] + lanes[:2] + [(8, ng), (8, ng), (8, 128), (3, 1, mm), (3, 1, nn)]),
            hbm(x_in, h_act, d_gate, d_up, d_out, w_gate, r_gate, c_gate, r_up, c_up, r_down, c_down), [HB] * 12, VM,
            [
                VM((nk, KB, mg), BF16), VM((2, HB_ROWS, md), BF16), VM((mg, tokens), BF16), VM((RING, tokens, WIDE), BF16),
                dma((nk,)), dma((2,)), dma((RING,)), dma((nk,)), dma((2,)), dma((6,)),
            ])
        second = call(
            exchange_kernel,
            vm([(size, 128)] + dims[1:] + lanes + [(1, n) for _, n in dims] + stats),
            vmem(*first) + hbm(w_up, w_down) + one, [VM] * len(first) + [HB] * 2 + [pltpu.SMEM] * 3, VM,
            [
                dma((2,)),
                VM((md, 128), F32), VM((8, nd), F32),
                VM((3, 1, mm), F32), VM((3, 1, mm), F32), VM((3, 1, nn), F32), VM((3, 3, 1, nn), F32),
                VM((8, 128), F32), VM((7, 8, 128), F32), VM((8, 128), F32), VM((7, 8, 128), F32),
                dma((3,)), dma((3,)), dma((3, 3)), dma((3, 3)), dma((7,)), dma((7,)), dma((7,)), dma((7,)),
            ], collective_id=0, has_side_effects=True)
        outs = call(
            write_kernel,
            tuple(jax.ShapeDtypeStruct(s, F32) for s in dims + [(k,) for mn in dims for k in mn]),
            vmem(*first, *second), [VM] * (len(first) + len(second)), HB,
            [VM((8, mg // 8, ng), F32), VM((8, md // 8, nd), F32), dma((8,)), dma((6,))])
        return tuple(outs)

    act_spec = P(None, "row")
    cot_spec = P(None, "col")
    w_spec = P("row", "col")
    r_spec = P("row")
    c_spec = P("col")
    s_spec = P()
    return jax.shard_map(local_program, mesh=mesh, in_specs=(act_spec, act_spec, cot_spec, cot_spec, cot_spec, w_spec, w_spec, w_spec, r_spec, c_spec, r_spec, c_spec, r_spec, c_spec, s_spec, s_spec, s_spec), out_specs=(w_spec, w_spec, w_spec, r_spec, c_spec, r_spec, c_spec, r_spec, c_spec), check_vma=False)
```
